256 devices in a mesh: rows: 32 (over y, z), cols: 8 (over x, core).
Axes of the slice: x: 4, y: 4, z: 8, core: 2. Of those that a mesh axis runs over, the one named last changes fastest.
Arguments:
- orthophoto: float32 [3, 4096, 4096], P(None, 'rows', 'cols'), may hold values from 0 to 1
Outputs:
- detail_zero: float32 [3, 4096, 4096], P(None, 'rows', 'cols')
- detail_one: float32 [3, 2048, 2048], P(None, 'rows', 'cols')
- detail_two: float32 [3, 1024, 1024], P(None, 'rows', 'cols')
- detail_three: float32 [3, 512, 512], P(None, 'rows', 'cols')
- detail_four: float32 [3, 256, 256], P(None, 'rows', 'cols')
- coarsest: float32 [3, 128, 128], P(None, 'rows', 'cols')
The draws below stay inside these ranges and needn't reach their ends.
All inputs are finite; a program needn't handle non-finite values.
Results may differ from the reference program's by a relative error of at most 0.00015.
Values sent between devices are 32-bit elements; how exact they have to be, the bound alone decides.
A program may use at most 64 MiB of HBM per device.

```python
import jax
import jax.numpy as jnp
from jax import lax

CHANNELS = 3
LEVELS = 5
NROWS = 4096
NCOLS = 4096


def steps_of(rng, dims, pieces, least, top_value):
    def one(position, shards_of):
        heights = jax.random.uniform(jax.random.fold_in(jax.random.fold_in(rng, 6), position), (shards_of,), jnp.float32, least / len(pieces), top_value / len(pieces))
        return jnp.repeat(jnp.exp(heights), dims[position] // shards_of).reshape((-1,) + (1,) * (len(dims) - position - 1))

    gain = one(*pieces[0])
    for cut in pieces[1:]:
        gain = gain * one(*cut)
    return gain


def setup_inputs(seed: int = 0) -> dict:
    key_list = jax.random.split(jax.random.key(seed), 2)
    return {
        "orthophoto": jnp.clip(1.0 * jax.random.uniform(key_list[0], (CHANNELS, NROWS, NCOLS), jnp.float32) ** steps_of(key_list[0], (CHANNELS, NROWS, NCOLS), ((1, 32), (2, 8)), -0.2, 0.2), 0.0, 1.0),
    }


TAPS = (0.0625, 0.25, 0.375, 0.25, 0.0625)


def decimate(padded, axis_dim, out_count):
    summed = TAPS[0] * lax.slice_in_dim(padded, 0, 2 * out_count - 1, 2, axis_dim)
    for tap_index in range(1, 5):
        summed = summed + TAPS[tap_index] * lax.slice_in_dim(padded, tap_index, tap_index + 2 * out_count - 1, 2, axis_dim)
    return summed


def shrink(current):
    padded = jnp.pad(current, ((0, 0), (2, 2), (2, 2)), mode="reflect")
    vertical = decimate(padded, 1, current.shape[1] // 2)
    return decimate(vertical, 2, current.shape[2] // 2)


def alternate(even_part, odd_part, axis_dim):
    stacked = jnp.stack([even_part, odd_part], axis=axis_dim + 1)
    new_shape = list(even_part.shape)
    new_shape[axis_dim] = 2 * new_shape[axis_dim]
    return stacked.reshape(new_shape)


def upsample(bordered, axis_dim):
    inner_count = bordered.shape[axis_dim] - 2
    before = lax.slice_in_dim(bordered, 0, inner_count, 1, axis_dim)
    center = lax.slice_in_dim(bordered, 1, inner_count + 1, 1, axis_dim)
    after = lax.slice_in_dim(bordered, 2, inner_count + 2, 1, axis_dim)
    return alternate((before + 6.0 * center + after) * 0.125, (center + after) * 0.5, axis_dim)


def expand(bordered):
    return upsample(upsample(bordered, 1), 2)


def pad_coarse(coarse, axis_dim):
    inner_count = coarse.shape[axis_dim]
    head_cell = lax.slice_in_dim(coarse, 1, 2, 1, axis_dim)
    tail_cell = lax.slice_in_dim(coarse, inner_count - 1, inner_count, 1, axis_dim)
    return jnp.concatenate([head_cell, coarse, tail_cell], axis=axis_dim)


def encode_plane(plane):
    current = plane[None]
    details = []
    for layer_index in range(LEVELS):
        coarse = shrink(current)
        bordered = pad_coarse(pad_coarse(coarse, 1), 2)
        details.append(current - expand(bordered))
        current = coarse
    return (details[0][0], details[1][0], details[2][0], details[3][0], details[4][0], current[0])


def reference(orthophoto):
    results = lax.map(encode_plane, orthophoto)
    return (results[0], results[1], results[2], results[3], results[4], results[5])
```

```python
import functools

import jax
import jax.numpy as jnp
import numpy as np
from jax import lax
from jax.experimental import pallas as pl
from jax.experimental.pallas import tpu as pltpu
from jax.sharding import PartitionSpec as P

CH = 3
ROWS = 128
COLS = 512
LEVELS = 5
H = [ROWS >> k for k in range(6)]
W = [COLS >> k for k in range(6)]
R = [0, 72, 40, 24, 16, 8]
BASE = [0, 0, 216, 336, 408, 456]
POS = [0, 0, 0, 0, 64, 96]
F32 = jnp.float32
BF16 = jnp.bfloat16
MESH = pl.DeviceIdType.MESH
TAPS = (1.0, 4.0, 6.0, 4.0, 1.0)


def column_reductions(low, high):
    result = [None]
    total = None
    for k in range(1, LEVELS + 1):
        n = W[k - 1]
        step = np.zeros((n + 3, W[k] + 3))
        for j in range(0 if low else -1, W[k] if high else W[k] + 2):
            for tap in range(5):
                cell = 2 * j - 2 + tap
                if low and cell < 0:
                    cell = -cell
                if high and cell > n - 1:
                    cell = 2 * (n - 1) - cell
                if -1 <= cell <= n + 1:
                    step[cell + 1, j + 1] += TAPS[tap] / 16
        total = step[1 : n + 1] if k == 1 else total @ step
        result.append(total)
    return result


def reduction_table(low, high):
    t = column_reductions(low, high)

    def edge(k):
        cells = (W[k] - 1, W[k] - 1 if high else W[k], W[k] + 1, 1 if low else -1, 0)
        return t[k][:, [c + 1 for c in cells]]

    first = np.zeros((COLS, 512))
    first[:, 0:256] = t[1][:, 1:257]
    first[:, 384:512] = t[2][:, 1:129]
    for k in (1, 2):
        first[:, 256 + 8 * (k - 1) : 256 + 8 * (k - 1) + 5] = edge(k)
    last = np.zeros((COLS, 256))
    for k in (3, 4, 5):
        last[:, 8 * (k - 1) : 8 * (k - 1) + 5] = edge(k)
        last[:, 128 + POS[k] : 128 + POS[k] + W[k]] = t[k][:, 1 : W[k] + 1]
    top = np.asarray(last.astype(jnp.bfloat16), np.float64)
    rest = np.asarray((last - top).astype(jnp.bfloat16), np.float64)
    assert np.array_equal(top + rest, last)
    assert np.array_equal(np.asarray(first.astype(jnp.bfloat16), np.float64), first)
    return np.concatenate([first, top, rest], axis=1)


def expansion_row(k, cell):
    row = np.zeros(2 * W[k])
    for i in range(W[k]):
        row[2 * i] += {i - 1: 0.125, i: 0.75, i + 1: 0.125}.get(cell, 0.0)
        row[2 * i + 1] += {i: 0.5, i + 1: 0.5}.get(cell, 0.0)
    return row


def expansion_table(k, main_at, edge_at, lanes):
    spread = np.zeros((lanes, 2 * W[k]))
    keep = np.zeros((lanes, W[k]))
    for c in range(W[k]):
        spread[main_at + c] = expansion_row(k, c)
        keep[main_at + c, c] = 1
    own = edge_at + 8 * (k - 1)
    came = own + 64
    spread[own + 1] = expansion_row(k, W[k])
    spread[own + 3] = expansion_row(k, -1)
    for s, cell in enumerate((-1, 0, 1, W[k] - 1, W[k])):
        spread[came + s] = expansion_row(k, cell)
        if 0 <= cell < W[k]:
            keep[came + s, cell] = 1
    return spread, keep


def padded(a, cols):
    return np.pad(a, ((0, 0), (0, cols - a.shape[1])))


def tables():
    plain, low, high = (reduction_table(*e) for e in ((False, False), (True, False), (False, True)))
    assert np.array_equal(plain[128:], low[128:]) and np.array_equal(plain[:384], high[:384])
    t_low = np.stack([plain[:128], low[:128]])
    t_high = np.stack([plain[384:], high[384:]])
    v1, s1 = expansion_table(1, 0, 256, 384)
    w2 = np.concatenate(expansion_table(2, 128, 0, 256), axis=1)
    deep = []
    for k in (3, 4, 5):
        spread, keep = expansion_table(k, 128 + POS[k], 0, 256)
        deep.append(np.concatenate([padded(spread, 128), padded(keep, 128)], axis=1))
    return [a.astype(jnp.bfloat16) for a in (t_low, plain[128:384], t_high, v1, s1[256:], w2, np.stack(deep))]


def split3(a):
    top = a.astype(BF16)
    rest = a - top.astype(F32)
    mid = rest.astype(BF16)
    return top, mid, (rest - mid.astype(F32)).astype(BF16)


def dot3(parts, table):
    return sum(jnp.dot(p, table, preferred_element_type=F32) for p in parts)


def reduce_rows(k, src, dst, first, last):
    n, h = H[k - 1], H[k]

    def tap(o):
        return src[:, :, pl.ds(8 + o, h, stride=2), :]

    dst[:, :, 8 : 8 + h, :] = (tap(-2) + tap(2)) * 0.0625 + (tap(-1) + tap(1)) * 0.25 + tap(0) * 0.375

    def s(i):
        return src[:, :, 8 + i : 9 + i, :]

    def d(i):
        return dst[:, :, 8 + i : 9 + i, :]

    below = jnp.where(first, d(1), s(-1) * 0.25 + s(0) * 0.0625)
    zero = jnp.zeros_like(below)
    dst[:, :, 6:7, :] = jnp.where(first, d(2), zero)
    dst[:, :, 7:8, :] = below
    dst[:, :, 8 + h : 9 + h, :] = jnp.where(
        last, d(h - 2), s(n - 2) * 0.0625 + s(n - 1) * 0.25 + s(n) * 0.375 + s(n + 1) * 0.25
    )
    dst[:, :, 9 + h : 10 + h, :] = jnp.where(last, zero, s(n) * 0.0625 + s(n + 1) * 0.25)
    dst[:, :, 10 + h : 11 + h, :] = below
    left = R[k] - h - 3
    dst[:, :, 11 + h : 11 + h + left, :] = jnp.zeros((CH, 4, left, 128), F32)


def rows_of(k, y):
    return jnp.concatenate(
        [jnp.concatenate([y[c, t, 8 : 8 + R[k], :] for t in range(4)], axis=1) for c in range(CH)], axis=0
    )


def kernel(
    x_hbm, tlow_hbm, tmid_hbm, thigh_hbm, v1_hbm, s1_hbm, w2_hbm, w345_hbm,
    o0, o1, o2, o3, o4, o5,
    xs, y1, y2, y3, y4, y5, tv, v1, s1, w2, w345, p1, p2, p3,
    rh, rl, cb, rh_in, rl_in, cbm, cbp, chm, chp, clm, clp,
    g1, g2, g3, g4, g5, m1, m2, m3, m4, d0, d1, d2, d3w, d4w, d3, d4, d5,
    load_sem, out_sem, send_sem, recv_sem,
):
    r, c = lax.axis_index("rows"), lax.axis_index("cols")
    nr, nc = lax.axis_size("rows"), lax.axis_size("cols")
    first, last = r == 0, r == nr - 1
    left, right = c == 0, c == nc - 1
    up, down = jnp.logical_not(first), jnp.logical_not(last)
    west, east = jnp.logical_not(left), jnp.logical_not(right)

    loads = [pltpu.make_async_copy(x_hbm.at[:, :, pl.ds(128 * t, 128)], xs.at[:, t, pl.ds(8, ROWS), :], load_sem.at[t]) for t in range(4)]
    loads += [
        pltpu.make_async_copy(tlow_hbm.at[left.astype(jnp.int32)], tv.at[pl.ds(0, 128)], load_sem.at[4]),
        pltpu.make_async_copy(tmid_hbm, tv.at[pl.ds(128, 256)], load_sem.at[5]),
        pltpu.make_async_copy(thigh_hbm.at[right.astype(jnp.int32)], tv.at[pl.ds(384, 128)], load_sem.at[6]),
        pltpu.make_async_copy(v1_hbm, v1, load_sem.at[7]),
        pltpu.make_async_copy(s1_hbm, s1, load_sem.at[8]),
        pltpu.make_async_copy(w2_hbm, w2, load_sem.at[9]),
        pltpu.make_async_copy(w345_hbm, w345, load_sem.at[10]),
    ]
    for copy in loads:
        copy.start()

    def there(dr, dc):
        ok = jnp.bool_(True)
        if dr:
            ok = jnp.logical_and(ok, up if dr < 0 else down)
        if dc:
            ok = jnp.logical_and(ok, west if dc < 0 else east)
        return ok

    edge = pl.ds(256, 128)
    messages = [
        (rh, rh_in, 1, 0),
        (rl, rl_in, -1, 0),
        (cb, cbm, 0, 1),
        (cb, cbp, 0, -1),
        (rh.at[:, :, edge], chm, 1, 1),
        (rh.at[:, :, edge], chp, 1, -1),
        (rl.at[:, :, edge], clm, -1, 1),
        (rl.at[:, :, edge], clp, -1, -1),
    ]
    barrier = pltpu.get_barrier_semaphore()
    for _, dst, dr, dc in messages:

        @pl.when(there(dr, dc))
        def _(dr=dr, dc=dc):
            pl.semaphore_signal(barrier, inc=1, device_id=(r + dr, c + dc), device_id_type=MESH)

        @pl.when(jnp.logical_not(there(-dr, -dc)))
        def _(dst=dst):
            dst[...] = jnp.zeros_like(dst)

    for copy in loads[:4]:
        copy.wait()
    xs[:, :, 6:7, :] = jnp.where(first, xs[:, :, 10:11, :], 0.0)
    xs[:, :, 7:8, :] = jnp.where(first, xs[:, :, 9:10, :], 0.0)
    xs[:, :, 136:137, :] = jnp.where(last, xs[:, :, 134:135, :], 0.0)
    xs[:, :, 137:138, :] = jnp.zeros((CH, 4, 1, 128), F32)
    ys = (xs, y1, y2, y3, y4, y5)
    for k in range(1, LEVELS + 1):
        reduce_rows(k, ys[k - 1], ys[k], first, last)
    for copy in loads[4:7]:
        copy.wait()
    p1[...] = dot3(split3(rows_of(1, y1)), tv[:, 0:384])
    p2[...] = dot3(split3(rows_of(2, y2)), tv[:, 256:512])
    deep = split3(jnp.concatenate([rows_of(k, ys[k]) for k in (3, 4, 5)], axis=0))
    p3[...] = dot3(deep, tv[:, 512:768]) + dot3(deep, tv[:, 768:1024])

    edges = jnp.concatenate([p1[:, 256:384], p2[:, 0:128], p3[:, 0:128], jnp.zeros((32, 128), F32)], axis=0)
    turned = jnp.transpose(edges)
    place = lax.broadcasted_iota(jnp.int32, (8, 512), 1)

    def of_level(k, a):
        ok = place < (BASE[k + 1] if k < LEVELS else 480)
        return jnp.where(jnp.logical_and(ok, place >= BASE[k]), a, 0.0)

    cb[...] = sum(of_level(k, turned[8 * (k - 1) : 8 * k]) for k in range(1, LEVELS + 1))

    lane = lax.broadcasted_iota(jnp.int32, (1, 128), 1)

    def tiles(k, ch, slot):
        if k == 1:
            at = 72 * ch + slot
            return p1[at : at + 1, 0:256], p1[at : at + 1, 256:384]
        if k == 2:
            at = 40 * ch + slot
            return p2[at : at + 1, 128:256], p2[at : at + 1, 0:128]
        at = BASE[k] - BASE[3] + R[k] * ch + slot
        return p3[at : at + 1, 128:256], p3[at : at + 1, 0:128]

    def strip(ch, slot_of):
        both = [None] + [tiles(k, ch, slot_of(k)) for k in range(1, LEVELS + 1)]
        cells = both[5][1]
        for k in (4, 3, 2, 1):
            cells = jnp.where(lane < 8 * k, both[k][1], cells)
        small = jnp.where(lane < 64, both[3][0], jnp.where(lane < 96, both[4][0], both[5][0]))
        return jnp.concatenate([both[1][0], cells, both[2][0], small], axis=1)

    for ch in range(CH):
        for i in range(3):
            rh[ch, i : i + 1, :] = strip(ch, lambda k: H[k] - 1 + i)
        rl[ch, 0:1, :] = strip(ch, lambda k: H[k] + 2)
        rl[ch, 1:2, :] = strip(ch, lambda k: 0)
        rh[ch, 3:4, :] = jnp.zeros((1, 640), F32)

    neighbours = (up.astype(jnp.int32) + down.astype(jnp.int32) + 1) * (
        west.astype(jnp.int32) + east.astype(jnp.int32) + 1
    ) - 1
    pl.semaphore_wait(barrier, neighbours)
    copies = []
    for m, (src, dst, dr, dc) in enumerate(messages):
        copy = pltpu.make_async_remote_copy(
            src_ref=src, dst_ref=dst, send_sem=send_sem.at[m], recv_sem=recv_sem.at[m],
            device_id=(r + dr, c + dc), device_id_type=MESH,
        )
        copies.append(copy)
        pl.when(there(dr, dc))(copy.start)
    for copy in loads[7:]:
        copy.wait()
    for copy, (_, _, dr, dc) in zip(copies, messages):
        pl.when(there(-dr, -dc))(copy.wait_recv)

    sub = lax.broadcasted_iota(jnp.int32, (8, 512), 0)
    comb = jnp.where(sub < 3, cbm[...], cbp[...])
    came = jnp.transpose(
        jnp.concatenate(
            [jnp.zeros((64, 512), F32)] + [of_level(k, comb) for k in range(1, LEVELS + 1)] + [jnp.zeros((24, 512), F32)],
            axis=0,
        )
    )
    p1[:, 256:384] += came[0:216]
    p2[:, 0:128] += came[216:336]
    p3[:, 0:128] += came[336:480]
    is_left = jnp.bitwise_and(lane, 7) < 3

    def add_row(ch, slot_of, strip_in, corner):
        cells = strip_in[:, 256:384] + pltpu.roll(corner, 64, 1)
        at = 72 * ch + slot_of(1)
        p1[at : at + 1, 0:256] += strip_in[:, 0:256]
        p1[at : at + 1, 256:384] += cells
        at = 40 * ch + slot_of(2)
        p2[at : at + 1, 0:128] += cells
        p2[at : at + 1, 128:256] += strip_in[:, 384:512]
        for k in (3, 4, 5):
            at = BASE[k] - BASE[3] + R[k] * ch + slot_of(k)
            p3[at : at + 1, 0:128] += cells
            p3[at : at + 1, 128:256] += strip_in[:, 512:640]

    for ch in range(CH):
        for i in range(3):
            corner = jnp.where(is_left, chm[ch, i : i + 1, :], chp[ch, i : i + 1, :])
            add_row(ch, lambda k: H[k] + 2 if i == 0 else i - 1, rh_in[ch, i : i + 1, :], corner)
        for i in range(2):
            corner = jnp.where(is_left, clm[ch, i : i + 1, :], clp[ch, i : i + 1, :])
            add_row(ch, lambda k: H[k] - 1 + i, rl_in[ch, i : i + 1, :], corner)

    parts = split3(p1[...])
    wide1 = dot3(parts, v1[...])
    level1 = p1[:, 0:256] + dot3([p[:, 256:384] for p in parts], s1[...])
    both2 = dot3(split3(p2[...]), w2[...])
    deep = p3[...]
    both3 = dot3(split3(deep[0:72]), w345[0])
    both4 = dot3(split3(deep[72:120]), w345[1])
    both5 = dot3(split3(deep[120:144]), w345[2])

    def put(k, wide, g):
        h = H[k]
        for ch in range(CH):
            for t in range(g.shape[1]):
                a = wide[R[k] * ch : R[k] * (ch + 1), 128 * t : 128 * (t + 1)]
                g[ch, t, 8 : 8 + h, :] = a[0:h]
                g[ch, t, 7:8, :] = a[h + 2 : h + 3]
                g[ch, t, 8 + h : 9 + h, :] = jnp.where(last, a[h - 1 : h], a[h : h + 1])

    put(1, wide1, g1)
    put(2, both2[:, 0:256], g2)
    put(3, both3, g3)
    put(4, both4, g4)
    put(5, both5, g5)

    def keep(k, level, m):
        for ch in range(CH):
            for t in range(m.shape[1]):
                m[ch, t] = level[R[k] * ch : R[k] * ch + H[k], 128 * t : 128 * (t + 1)]

    keep(1, level1, m1)
    keep(2, both2[:, 256:384], m2)
    keep(3, both3[:, 128:256], m3)
    keep(4, both4[:, 128:256], m4)

    def detail(k, g, level, at, out):
        h = H[k]
        lo, mid, hi = (g[:, :, 7 + i : 7 + i + h, :] for i in range(3))
        even, odd = pl.ds(at, h, stride=2), pl.ds(at + 1, h, stride=2)
        out[:, :, pl.ds(0, h, stride=2), :] = level[:, :, even, :] - (lo + 6.0 * mid + hi) * 0.125
        out[:, :, pl.ds(1, h, stride=2), :] = level[:, :, odd, :] - (mid + hi) * 0.5

    outs = []

    def send_out(src, dst):
        copy = pltpu.make_async_copy(src, dst, out_sem.at[len(outs)])
        copy.start()
        outs.append(copy)

    detail(1, g1, xs, 8, d0)
    for t in range(4):
        send_out(d0.at[:, t], o0.at[:, :, pl.ds(128 * t, 128)])
    detail(2, g2, m1, 0, d1)
    for t in range(2):
        send_out(d1.at[:, t], o1.at[:, :, pl.ds(128 * t, 128)])
    detail(3, g3, m2, 0, d2)
    send_out(d2.at[:, 0], o2)
    detail(4, g4, m3, 0, d3w)
    d3[...] = d3w[:, 0, :, 0:64]
    send_out(d3, o3)
    detail(5, g5, m4, 0, d4w)
    d4[...] = d4w[:, 0, :, 0:32]
    send_out(d4, o4)
    for ch in range(CH):
        d5[ch] = both5[8 * ch : 8 * ch + 4, 128:144]
    send_out(d5, o5)

    for copy, (_, _, dr, dc) in zip(copies, messages):
        pl.when(there(dr, dc))(copy.wait_send)
    for copy in outs:
        copy.wait()


def body(orthophoto):
    def vmem(*shape, dtype=F32):
        return pltpu.VMEM(shape, dtype)

    scratch = [vmem(CH, 4, ROWS + 16, 128)]
    scratch += [vmem(CH, 4, H[k] + 16, 128) for k in range(1, 6)]
    scratch += [vmem(512, 1024, dtype=BF16), vmem(384, 512, dtype=BF16), vmem(128, 256, dtype=BF16)]
    scratch += [vmem(256, 384, dtype=BF16), vmem(3, 256, 256, dtype=BF16)]
    scratch += [vmem(216, 384), vmem(120, 256), vmem(144, 256)]
    scratch += [vmem(CH, 4, 640), vmem(CH, 2, 640), vmem(8, 512)]
    scratch += [vmem(CH, 4, 640), vmem(CH, 2, 640), vmem(8, 512), vmem(8, 512)]
    scratch += [vmem(CH, 4, 128), vmem(CH, 4, 128), vmem(CH, 2, 128), vmem(CH, 2, 128)]
    scratch += [vmem(CH, t, H[k] + 16, 128) for k, t in ((1, 4), (2, 2), (3, 1), (4, 1), (5, 1))]
    scratch += [vmem(CH, t, H[k], 128) for k, t in ((1, 2), (2, 1), (3, 1), (4, 1))]
    scratch += [vmem(CH, t, H[k], 128) for k, t in ((0, 4), (1, 2), (2, 1), (3, 1), (4, 1))]
    scratch += [vmem(CH, H[3], W[3]), vmem(CH, H[4], W[4]), vmem(CH, H[5], W[5])]
    scratch += [pltpu.SemaphoreType.DMA((n,)) for n in (11, 10, 8, 8)]
    anywhere = pl.BlockSpec(memory_space=pl.ANY)
    results = pl.pallas_call(
        kernel,
        out_shape=[jax.ShapeDtypeStruct((CH, H[k], W[k]), F32) for k in range(6)],
        in_specs=[anywhere] * 8,
        out_specs=[anywhere] * 6,
        scratch_shapes=scratch,
        compiler_params=pltpu.CompilerParams(collective_id=0, has_side_effects=True),
    )(orthophoto, *tables())
    return tuple(results)


def solution(mesh):
    placed = P(None, "rows", "cols")
    return jax.shard_map(body, mesh=mesh, in_specs=(placed,), out_specs=(placed,) * 6, check_vma=False)
```

```python
import functools

import jax
import jax.numpy as jnp
import numpy as np
from jax import lax
from jax.experimental import pallas as pl
from jax.experimental.pallas import tpu as pltpu
from jax.sharding import PartitionSpec as P

CH = 3
ROWS = 128
COLS = 512
LEVELS = 5
H = [ROWS >> k for k in range(6)]
W = [COLS >> k for k in range(6)]
R = [0, 72, 40, 24, 16, 8]
BASE = [0, 0, 216, 336, 408, 456]
POS = [0, 0, 0, 0, 64, 96]
F32 = jnp.float32
BF16 = jnp.bfloat16
MESH = pl.DeviceIdType.MESH
TAPS = (1.0, 4.0, 6.0, 4.0, 1.0)


def column_reductions(low, high):
    result = [None]
    total = None
    for k in range(1, LEVELS + 1):
        n = W[k - 1]
        step = np.zeros((n + 3, W[k] + 3))
        for j in range(0 if low else -1, W[k] if high else W[k] + 2):
            for tap in range(5):
                cell = 2 * j - 2 + tap
                if low and cell < 0:
                    cell = -cell
                if high and cell > n - 1:
                    cell = 2 * (n - 1) - cell
                if -1 <= cell <= n + 1:
                    step[cell + 1, j + 1] += TAPS[tap] / 16
        total = step[1 : n + 1] if k == 1 else total @ step
        result.append(total)
    return result


def reduction_table(low, high):
    t = column_reductions(low, high)

    def edge(k):
        cells = (W[k] - 1, W[k] - 1 if high else W[k], W[k] + 1, 1 if low else -1, 0)
        return t[k][:, [c + 1 for c in cells]]

    first = np.zeros((COLS, 512))
    first[:, 0:256] = t[1][:, 1:257]
    first[:, 384:512] = t[2][:, 1:129]
    for k in (1, 2):
        first[:, 256 + 8 * (k - 1) : 256 + 8 * (k - 1) + 5] = edge(k)
    last = np.zeros((COLS, 256))
    for k in (3, 4, 5):
        last[:, 8 * (k - 1) : 8 * (k - 1) + 5] = edge(k)
        last[:, 128 + POS[k] : 128 + POS[k] + W[k]] = t[k][:, 1 : W[k] + 1]
    top = np.asarray(last.astype(jnp.bfloat16), np.float64)
    rest = np.asarray((last - top).astype(jnp.bfloat16), np.float64)
    assert np.array_equal(top + rest, last)
    assert np.array_equal(np.asarray(first.astype(jnp.bfloat16), np.float64), first)
    return np.concatenate([first, top, rest], axis=1)


def expansion_row(k, cell):
    row = np.zeros(2 * W[k])
    for i in range(W[k]):
        row[2 * i] += {i - 1: 0.125, i: 0.75, i + 1: 0.125}.get(cell, 0.0)
        row[2 * i + 1] += {i: 0.5, i + 1: 0.5}.get(cell, 0.0)
    return row


def expansion_table(k, main_at, edge_at, lanes):
    spread = np.zeros((lanes, 2 * W[k]))
    keep = np.zeros((lanes, W[k]))
    for c in range(W[k]):
        spread[main_at + c] = expansion_row(k, c)
        keep[main_at + c, c] = 1
    own = edge_at + 8 * (k - 1)
    came = own + 64
    spread[own + 1] = expansion_row(k, W[k])
    spread[own + 3] = expansion_row(k, -1)
    for s, cell in enumerate((-1, 0, 1, W[k] - 1, W[k])):
        spread[came + s] = expansion_row(k, cell)
        if 0 <= cell < W[k]:
            keep[came + s, cell] = 1
    return spread, keep


def padded(a, cols):
    return np.pad(a, ((0, 0), (0, cols - a.shape[1])))


def tables():
    plain, low, high = (reduction_table(*e) for e in ((False, False), (True, False), (False, True)))
    assert np.array_equal(plain[128:], low[128:]) and np.array_equal(plain[:384], high[:384])
    t_low = np.stack([plain[:128], low[:128]])
    t_high = np.stack([plain[384:], high[384:]])
    v1, s1 = expansion_table(1, 0, 256, 384)
    w2 = np.concatenate(expansion_table(2, 128, 0, 256), axis=1)
    deep = []
    for k in (3, 4, 5):
        spread, keep = expansion_table(k, 128 + POS[k], 0, 256)
        deep.append(np.concatenate([padded(spread, 128), padded(keep, 128)], axis=1))
    return [a.astype(jnp.bfloat16) for a in (t_low, plain[128:384], t_high, v1, s1[256:], w2, np.stack(deep))]


def split3(a):
    top = a.astype(BF16)
    rest = a - top.astype(F32)
    mid = rest.astype(BF16)
    return top, mid, (rest - mid.astype(F32)).astype(BF16)


def dot3(parts, table):
    return sum(jnp.dot(p, table, preferred_element_type=F32) for p in parts)


def reduce_rows(k, src, dst, first, last):
    n, h = H[k - 1], H[k]

    def tap(o):
        return src[:, :, pl.ds(8 + o, h, stride=2), :]

    dst[:, :, 8 : 8 + h, :] = (tap(-2) + tap(2)) * 0.0625 + (tap(-1) + tap(1)) * 0.25 + tap(0) * 0.375

    def s(i):
        return src[:, :, 8 + i : 9 + i, :]

    def d(i):
        return dst[:, :, 8 + i : 9 + i, :]

    below = jnp.where(first, d(1), s(-1) * 0.25 + s(0) * 0.0625)
    zero = jnp.zeros_like(below)
    dst[:, :, 6:7, :] = jnp.where(first, d(2), zero)
    dst[:, :, 7:8, :] = below
    dst[:, :, 8 + h : 9 + h, :] = jnp.where(
        last, d(h - 2), s(n - 2) * 0.0625 + s(n - 1) * 0.25 + s(n) * 0.375 + s(n + 1) * 0.25
    )
    dst[:, :, 9 + h : 10 + h, :] = jnp.where(last, zero, s(n) * 0.0625 + s(n + 1) * 0.25)
    dst[:, :, 10 + h : 11 + h, :] = below
    left = R[k] - h - 3
    dst[:, :, 11 + h : 11 + h + left, :] = jnp.zeros((CH, 4, left, 128), F32)


def rows_of(k, y):
    return jnp.concatenate(
        [jnp.concatenate([y[c, t, 8 : 8 + R[k], :] for t in range(4)], axis=1) for c in range(CH)], axis=0
    )


def exchange_kernel(
    x_hbm, tlow_hbm, tmid_hbm, thigh_hbm, v1_hbm, s1_hbm, w2_hbm, w345_hbm,
    xs, g1, g2, g3, g4, g5, m1, m2, m3, m4, m5,
    y1, y2, y3, y4, y5, tv, v1, s1, w2, w345, p1, p2, p3,
    rh, rl, cb, rh_in, rl_in, cbm, cbp, chm, chp, clm, clp,
    load_sem, send_sem, recv_sem,
):
    r, c = lax.axis_index("rows"), lax.axis_index("cols")
    nr, nc = lax.axis_size("rows"), lax.axis_size("cols")
    first, last = r == 0, r == nr - 1
    left, right = c == 0, c == nc - 1
    up, down = jnp.logical_not(first), jnp.logical_not(last)
    west, east = jnp.logical_not(left), jnp.logical_not(right)

    loads = [pltpu.make_async_copy(x_hbm.at[:, :, pl.ds(128 * t, 128)], xs.at[:, t, pl.ds(8, ROWS), :], load_sem.at[t]) for t in range(4)]
    loads += [
        pltpu.make_async_copy(tlow_hbm.at[left.astype(jnp.int32)], tv.at[pl.ds(0, 128)], load_sem.at[4]),
        pltpu.make_async_copy(tmid_hbm, tv.at[pl.ds(128, 256)], load_sem.at[5]),
        pltpu.make_async_copy(thigh_hbm.at[right.astype(jnp.int32)], tv.at[pl.ds(384, 128)], load_sem.at[6]),
        pltpu.make_async_copy(v1_hbm, v1, load_sem.at[7]),
        pltpu.make_async_copy(s1_hbm, s1, load_sem.at[8]),
        pltpu.make_async_copy(w2_hbm, w2, load_sem.at[9]),
        pltpu.make_async_copy(w345_hbm, w345, load_sem.at[10]),
    ]
    for copy in loads:
        copy.start()

    def there(dr, dc):
        ok = jnp.bool_(True)
        if dr:
            ok = jnp.logical_and(ok, up if dr < 0 else down)
        if dc:
            ok = jnp.logical_and(ok, west if dc < 0 else east)
        return ok

    edge = pl.ds(256, 128)
    messages = [
        (rh, rh_in, 1, 0),
        (rl, rl_in, -1, 0),
        (cb, cbm, 0, 1),
        (cb, cbp, 0, -1),
        (rh.at[:, :, edge], chm, 1, 1),
        (rh.at[:, :, edge], chp, 1, -1),
        (rl.at[:, :, edge], clm, -1, 1),
        (rl.at[:, :, edge], clp, -1, -1),
    ]
    barrier = pltpu.get_barrier_semaphore()
    for _, dst, dr, dc in messages:

        @pl.when(there(dr, dc))
        def _(dr=dr, dc=dc):
            pl.semaphore_signal(barrier, inc=1, device_id=(r + dr, c + dc), device_id_type=MESH)

        @pl.when(jnp.logical_not(there(-dr, -dc)))
        def _(dst=dst):
            dst[...] = jnp.zeros_like(dst)

    for copy in loads[:4]:
        copy.wait()
    xs[:, :, 6:7, :] = jnp.where(first, xs[:, :, 10:11, :], 0.0)
    xs[:, :, 7:8, :] = jnp.where(first, xs[:, :, 9:10, :], 0.0)
    xs[:, :, 136:137, :] = jnp.where(last, xs[:, :, 134:135, :], 0.0)
    xs[:, :, 137:138, :] = jnp.zeros((CH, 4, 1, 128), F32)
    ys = (xs, y1, y2, y3, y4, y5)
    for k in range(1, LEVELS + 1):
        reduce_rows(k, ys[k - 1], ys[k], first, last)
    for copy in loads[4:7]:
        copy.wait()
    p1[...] = dot3(split3(rows_of(1, y1)), tv[:, 0:384])
    p2[...] = dot3(split3(rows_of(2, y2)), tv[:, 256:512])
    deep = split3(jnp.concatenate([rows_of(k, ys[k]) for k in (3, 4, 5)], axis=0))
    p3[...] = dot3(deep, tv[:, 512:768]) + dot3(deep, tv[:, 768:1024])

    edges = jnp.concatenate([p1[:, 256:384], p2[:, 0:128], p3[:, 0:128], jnp.zeros((32, 128), F32)], axis=0)
    turned = jnp.transpose(edges)
    place = lax.broadcasted_iota(jnp.int32, (8, 512), 1)

    def of_level(k, a):
        ok = place < (BASE[k + 1] if k < LEVELS else 480)
        return jnp.where(jnp.logical_and(ok, place >= BASE[k]), a, 0.0)

    cb[...] = sum(of_level(k, turned[8 * (k - 1) : 8 * k]) for k in range(1, LEVELS + 1))

    lane = lax.broadcasted_iota(jnp.int32, (1, 128), 1)

    def tiles(k, ch, slot):
        if k == 1:
            at = 72 * ch + slot
            return p1[at : at + 1, 0:256], p1[at : at + 1, 256:384]
        if k == 2:
            at = 40 * ch + slot
            return p2[at : at + 1, 128:256], p2[at : at + 1, 0:128]
        at = BASE[k] - BASE[3] + R[k] * ch + slot
        return p3[at : at + 1, 128:256], p3[at : at + 1, 0:128]

    def strip(ch, slot_of):
        both = [None] + [tiles(k, ch, slot_of(k)) for k in range(1, LEVELS + 1)]
        cells = both[5][1]
        for k in (4, 3, 2, 1):
            cells = jnp.where(lane < 8 * k, both[k][1], cells)
        small = jnp.where(lane < 64, both[3][0], jnp.where(lane < 96, both[4][0], both[5][0]))
        return jnp.concatenate([both[1][0], cells, both[2][0], small], axis=1)

    for ch in range(CH):
        for i in range(3):
            rh[ch, i : i + 1, :] = strip(ch, lambda k: H[k] - 1 + i)
        rl[ch, 0:1, :] = strip(ch, lambda k: H[k] + 2)
        rl[ch, 1:2, :] = strip(ch, lambda k: 0)
        rh[ch, 3:4, :] = jnp.zeros((1, 640), F32)

    neighbours = (up.astype(jnp.int32) + down.astype(jnp.int32) + 1) * (
        west.astype(jnp.int32) + east.astype(jnp.int32) + 1
    ) - 1
    pl.semaphore_wait(barrier, neighbours)
    copies = []
    for m, (src, dst, dr, dc) in enumerate(messages):
        copy = pltpu.make_async_remote_copy(
            src_ref=src, dst_ref=dst, send_sem=send_sem.at[m], recv_sem=recv_sem.at[m],
            device_id=(r + dr, c + dc), device_id_type=MESH,
        )
        copies.append(copy)
        pl.when(there(dr, dc))(copy.start)
    for copy in loads[7:]:
        copy.wait()
    for copy, (_, _, dr, dc) in zip(copies, messages):
        pl.when(there(-dr, -dc))(copy.wait_recv)

    sub = lax.broadcasted_iota(jnp.int32, (8, 512), 0)
    comb = jnp.where(sub < 3, cbm[...], cbp[...])
    came = jnp.transpose(
        jnp.concatenate(
            [jnp.zeros((64, 512), F32)] + [of_level(k, comb) for k in range(1, LEVELS + 1)] + [jnp.zeros((24, 512), F32)],
            axis=0,
        )
    )
    p1[:, 256:384] += came[0:216]
    p2[:, 0:128] += came[216:336]
    p3[:, 0:128] += came[336:480]
    is_left = jnp.bitwise_and(lane, 7) < 3

    def add_row(ch, slot_of, strip_in, corner):
        cells = strip_in[:, 256:384] + pltpu.roll(corner, 64, 1)
        at = 72 * ch + slot_of(1)
        p1[at : at + 1, 0:256] += strip_in[:, 0:256]
        p1[at : at + 1, 256:384] += cells
        at = 40 * ch + slot_of(2)
        p2[at : at + 1, 0:128] += cells
        p2[at : at + 1, 128:256] += strip_in[:, 384:512]
        for k in (3, 4, 5):
            at = BASE[k] - BASE[3] + R[k] * ch + slot_of(k)
            p3[at : at + 1, 0:128] += cells
            p3[at : at + 1, 128:256] += strip_in[:, 512:640]

    for ch in range(CH):
        for i in range(3):
            corner = jnp.where(is_left, chm[ch, i : i + 1, :], chp[ch, i : i + 1, :])
            add_row(ch, lambda k: H[k] + 2 if i == 0 else i - 1, rh_in[ch, i : i + 1, :], corner)
        for i in range(2):
            corner = jnp.where(is_left, clm[ch, i : i + 1, :], clp[ch, i : i + 1, :])
            add_row(ch, lambda k: H[k] - 1 + i, rl_in[ch, i : i + 1, :], corner)

    parts = split3(p1[...])
    wide1 = dot3(parts, v1[...])
    level1 = p1[:, 0:256] + dot3([p[:, 256:384] for p in parts], s1[...])
    both2 = dot3(split3(p2[...]), w2[...])
    deep = p3[...]
    both3 = dot3(split3(deep[0:72]), w345[0])
    both4 = dot3(split3(deep[72:120]), w345[1])
    both5 = dot3(split3(deep[120:144]), w345[2])

    def put(k, wide, g):
        h = H[k]
        for ch in range(CH):
            for t in range(g.shape[1]):
                a = wide[R[k] * ch : R[k] * (ch + 1), 128 * t : 128 * (t + 1)]
                g[ch, t, 8 : 8 + h, :] = a[0:h]
                g[ch, t, 7:8, :] = a[h + 2 : h + 3]
                g[ch, t, 8 + h : 9 + h, :] = jnp.where(last, a[h - 1 : h], a[h : h + 1])

    put(1, wide1, g1)
    put(2, both2[:, 0:256], g2)
    put(3, both3, g3)
    put(4, both4, g4)
    put(5, both5, g5)

    def keep(k, level, m):
        for ch in range(CH):
            for t in range(m.shape[1]):
                m[ch, t] = level[R[k] * ch : R[k] * ch + H[k], 128 * t : 128 * (t + 1)]

    keep(1, level1, m1)
    keep(2, both2[:, 256:384], m2)
    keep(3, both3[:, 128:256], m3)
    keep(4, both4[:, 128:256], m4)

    for ch in range(CH):
        m5[ch] = both5[8 * ch : 8 * ch + 8, 128:256]
    for copy, (_, _, dr, dc) in zip(copies, messages):
        pl.when(there(dr, dc))(copy.wait_send)


def detail_kernel(
    xs, g1, g2, g3, g4, g5, m1, m2, m3, m4, m5,
    o0, o1, o2, o3, o4, o5,
    d0, d1, d2, d3w, d4w, d3, d4, d5, out_sem,
):
    def detail(k, g, level, at, out):
        h = H[k]
        lo, mid, hi = (g[:, :, 7 + i : 7 + i + h, :] for i in range(3))
        even, odd = pl.ds(at, h, stride=2), pl.ds(at + 1, h, stride=2)
        out[:, :, pl.ds(0, h, stride=2), :] = level[:, :, even, :] - (lo + 6.0 * mid + hi) * 0.125
        out[:, :, pl.ds(1, h, stride=2), :] = level[:, :, odd, :] - (mid + hi) * 0.5

    outs = []

    def send_out(src, dst):
        copy = pltpu.make_async_copy(src, dst, out_sem.at[len(outs)])
        copy.start()
        outs.append(copy)

    detail(1, g1, xs, 8, d0)
    for t in range(4):
        send_out(d0.at[:, t], o0.at[:, :, pl.ds(128 * t, 128)])
    detail(2, g2, m1, 0, d1)
    for t in range(2):
        send_out(d1.at[:, t], o1.at[:, :, pl.ds(128 * t, 128)])
    detail(3, g3, m2, 0, d2)
    send_out(d2.at[:, 0], o2)
    detail(4, g4, m3, 0, d3w)
    d3[...] = d3w[:, 0, :, 0:64]
    send_out(d3, o3)
    detail(5, g5, m4, 0, d4w)
    d4[...] = d4w[:, 0, :, 0:32]
    send_out(d4, o4)
    d5[...] = m5[:, 0:4, 0:16]
    send_out(d5, o5)

    for copy in outs:
        copy.wait()


def body(orthophoto):
    def vmem(*shape, dtype=F32):
        return pltpu.VMEM(shape, dtype)

    held = [(CH, 4, ROWS + 16, 128)]
    held += [(CH, t, H[k] + 16, 128) for k, t in ((1, 4), (2, 2), (3, 1), (4, 1), (5, 1))]
    held += [(CH, t, H[k], 128) for k, t in ((1, 2), (2, 1), (3, 1), (4, 1))] + [(CH, 8, 128)]
    scratch = [vmem(CH, 4, H[k] + 16, 128) for k in range(1, 6)]
    scratch += [vmem(512, 1024, dtype=BF16), vmem(384, 512, dtype=BF16), vmem(128, 256, dtype=BF16)]
    scratch += [vmem(256, 384, dtype=BF16), vmem(3, 256, 256, dtype=BF16)]
    scratch += [vmem(216, 384), vmem(120, 256), vmem(144, 256)]
    scratch += [vmem(CH, 4, 640), vmem(CH, 2, 640), vmem(8, 512)]
    scratch += [vmem(CH, 4, 640), vmem(CH, 2, 640), vmem(8, 512), vmem(8, 512)]
    scratch += [vmem(CH, 4, 128), vmem(CH, 4, 128), vmem(CH, 2, 128), vmem(CH, 2, 128)]
    scratch += [pltpu.SemaphoreType.DMA((n,)) for n in (11, 8, 8)]
    anywhere = pl.BlockSpec(memory_space=pltpu.HBM)
    inside = pl.BlockSpec(memory_space=pltpu.VMEM)
    arrays = pl.pallas_call(
        exchange_kernel,
        out_shape=[jax.ShapeDtypeStruct(shape, F32) for shape in held],
        in_specs=[anywhere] * 8,
        out_specs=[inside] * len(held),
        scratch_shapes=scratch,
        compiler_params=pltpu.CompilerParams(collective_id=0, has_side_effects=True, vmem_limit_bytes=24 << 20),
    )(*[pltpu.with_memory_space_constraint(jnp.asarray(a), pltpu.HBM) for a in (orthophoto, *tables())])
    scratch = [vmem(CH, t, H[k], 128) for k, t in ((0, 4), (1, 2), (2, 1), (3, 1), (4, 1))]
    scratch += [vmem(CH, H[3], W[3]), vmem(CH, H[4], W[4]), vmem(CH, H[5], W[5])]
    results = pl.pallas_call(
        detail_kernel,
        out_shape=[jax.ShapeDtypeStruct((CH, H[k], W[k]), F32) for k in range(6)],
        in_specs=[inside] * len(held),
        out_specs=[anywhere] * 6,
        scratch_shapes=scratch + [pltpu.SemaphoreType.DMA((10,))],
        compiler_params=pltpu.CompilerParams(vmem_limit_bytes=8 << 20),
    )(*arrays)
    return tuple(results)


def solution(mesh):
    placed = P(None, "rows", "cols")
    return jax.shard_map(body, mesh=mesh, in_specs=(placed,), out_specs=(placed,) * 6, check_vma=False)
```

```python
import functools

import jax
import jax.numpy as jnp
import numpy as np
from jax import lax
from jax.experimental import pallas as pl
from jax.experimental.pallas import tpu as pltpu
from jax.sharding import PartitionSpec as P

CH = 3
ROWS = 128
COLS = 512
LEVELS = 5
H = [ROWS >> k for k in range(6)]
W = [COLS >> k for k in range(6)]
R = [0, 72, 40, 24, 16, 8]
BASE = [0, 0, 216, 336, 408, 456]
POS = [0, 0, 0, 0, 64, 96]
F32 = jnp.float32
BF16 = jnp.bfloat16
MESH = pl.DeviceIdType.MESH
TAPS = (1.0, 4.0, 6.0, 4.0, 1.0)


def column_reductions(low, high):
    result = [None]
    total = None
    for k in range(1, LEVELS + 1):
        n = W[k - 1]
        step = np.zeros((n + 3, W[k] + 3))
        for j in range(0 if low else -1, W[k] if high else W[k] + 2):
            for tap in range(5):
                cell = 2 * j - 2 + tap
                if low and cell < 0:
                    cell = -cell
                if high and cell > n - 1:
                    cell = 2 * (n - 1) - cell
                if -1 <= cell <= n + 1:
                    step[cell + 1, j + 1] += TAPS[tap] / 16
        total = step[1 : n + 1] if k == 1 else total @ step
        result.append(total / 16.0**k)
    return result


def reduction_table(low, high):
    t = column_reductions(low, high)

    def edge(k):
        cells = (W[k] - 1, W[k] - 1 if high else W[k], W[k] + 1, 1 if low else -1, 0)
        return t[k][:, [c + 1 for c in cells]]

    first = np.zeros((COLS, 512))
    first[:, 0:256] = t[1][:, 1:257]
    first[:, 384:512] = t[2][:, 1:129]
    last = np.zeros((COLS, 256))
    for k in (3, 4, 5):
        last[:, 8 * (k - 1) : 8 * (k - 1) + 5] = edge(k)
        last[:, 128 + POS[k] : 128 + POS[k] + W[k]] = t[k][:, 1 : W[k] + 1]
    for k in (1, 2):
        first[:, 256 + 8 * (k - 1) : 256 + 8 * (k - 1) + 5] = edge(k)
    top = np.asarray(last.astype(jnp.bfloat16), np.float64)
    rest = np.asarray((last - top).astype(jnp.bfloat16), np.float64)
    assert np.array_equal(top + rest, last)
    first[:, 272:296] = top[:, 16:40]
    assert np.array_equal(np.asarray(first.astype(jnp.bfloat16), np.float64), first)
    return np.concatenate([first, top, rest], axis=1)


def expansion_row(k, cell):
    row = np.zeros(2 * W[k])
    for i in range(W[k]):
        row[2 * i] += {i - 1: 0.125, i: 0.75, i + 1: 0.125}.get(cell, 0.0)
        row[2 * i + 1] += {i: 0.5, i + 1: 0.5}.get(cell, 0.0)
    return row


def expansion_table(k, main_at, edge_at, lanes):
    spread = np.zeros((lanes, 2 * W[k]))
    keep = np.zeros((lanes, W[k]))
    for c in range(W[k]):
        spread[main_at + c] = expansion_row(k, c)
        keep[main_at + c, c] = 1
    own = edge_at + 8 * (k - 1)
    came = own + 64
    spread[own + 1] = expansion_row(k, W[k])
    spread[own + 3] = expansion_row(k, -1)
    for s, cell in enumerate((-1, 0, 1, W[k] - 1, W[k])):
        spread[came + s] = expansion_row(k, cell)
        if 0 <= cell < W[k]:
            keep[came + s, cell] = 1
    return spread, keep


def arrival_table(k):
    spread = np.zeros((128, 2 * W[k]))
    keep = np.zeros((128, W[k]))
    for part in range(3):
        for s, cell in enumerate((-1, 0, 1, W[k] - 1, W[k])):
            lane = 24 * (k - 1) + 8 * part + s
            spread[lane] = expansion_row(k, cell)
            if 0 <= cell < W[k]:
                keep[lane, cell] = 1
    return spread, keep


def padded(a, cols):
    return np.pad(a, ((0, 0), (0, cols - a.shape[1])))


def tables():
    plain, low, high = (reduction_table(*e) for e in ((False, False), (True, False), (False, True)))
    assert np.array_equal(plain[128:], low[128:]) and np.array_equal(plain[:384], high[:384])
    t_low = np.stack([plain[:128], low[:128]])
    t_high = np.stack([plain[384:], high[384:]])
    v1, s1 = expansion_table(1, 0, 256, 384)
    w2 = np.concatenate(expansion_table(2, 128, 0, 256), axis=1)
    deep = []
    for k in (3, 4, 5):
        spread, keep = expansion_table(k, 128 + POS[k], 0, 256)
        deep.append(np.concatenate([padded(spread, 128), padded(keep, 128)], axis=1))
    spread, keep = arrival_table(1)
    assert not spread[:, 128:384].any()
    arrive = [spread[:, :128], spread[:, 384:], keep]
    arrive += arrival_table(2)
    for k in (3, 4, 5):
        arrive += [padded(a, 128) for a in arrival_table(k)]
    parts = (t_low, plain[128:384], t_high, v1, s1[256:], w2, np.stack(deep), np.concatenate(arrive, axis=1))
    return [a.astype(jnp.bfloat16) for a in parts]


def split3(a):
    top = a.astype(BF16)
    rest = a - top.astype(F32)
    mid = rest.astype(BF16)
    return top, mid, (rest - mid.astype(F32)).astype(BF16)


def dot3(a, table):
    m = a.shape[0]
    p = jnp.dot(jnp.concatenate(split3(a), axis=0), table, preferred_element_type=F32)
    return p[0:m] + p[m : 2 * m] + p[2 * m : 3 * m]


def reduce_rows(k, t, src, dst, first, last):
    h = H[k]
    count = R[k]

    def tap(o):
        return src[:, t, pl.ds(6 + o, count, stride=2), :]

    dst[:, t, 7 : 7 + count, :] = (tap(-2) + tap(2)) + (tap(-1) + tap(1)) * 4.0 + tap(0) * 6.0
    mirror(dst, t, h, first, last, k < LEVELS)


def mirror(a, t, h, first, last, outer):
    a[:, t, 7:8, :] = a[:, t, pl.ds(jnp.where(first, 9, 7), 1), :]
    if outer:
        a[:, t, 6:7, :] = a[:, t, pl.ds(jnp.where(first, 10, 6), 1), :]
        a[:, t, 8 + h : 9 + h, :] = a[:, t, pl.ds(jnp.where(last, 6 + h, 8 + h), 1), :]


def rows_of(k, y, tiles):
    return jnp.concatenate(
        [jnp.concatenate([y[c, t, 7 : 7 + R[k], :] for t in tiles], axis=1) for c in range(CH)], axis=0
    )


def detail(g, level, at, out, count):
    lo, mid, hi = (g[:, :, i : i + count, :] for i in range(3))
    even, odd = pl.ds(at, count, stride=2), pl.ds(at + 1, count, stride=2)
    out[:, :, pl.ds(0, count, stride=2), :] = level[:, :, even, :] - ((lo + hi) * 0.125 + mid * 0.75)
    out[:, :, pl.ds(1, count, stride=2), :] = level[:, :, odd, :] - (mid + hi) * 0.5


def exchange_kernel(
    x_hbm, tlow_hbm, tmid_hbm, thigh_hbm, v1_hbm, s1_hbm, w2_hbm, w345_hbm, arrive_hbm,
    d0, d1, d2, d3, d4, d5,
    xs, y1, y2, y3, y4, y5, tv, v1, s1, w2, w345, arrive, srs, ri, ci,
    rh, rl, cb, rh_in, rl_in, cbm, cbp, chm, chp, clm, clp,
    g1, g2, g3, g4, g5, m1, m2, m3, m4, m5, d3w, d4w,
    load_sem, send_sem, recv_sem,
):
    r, c = lax.axis_index("rows"), lax.axis_index("cols")
    nr, nc = lax.axis_size("rows"), lax.axis_size("cols")
    first, last = r == 0, r == nr - 1
    left, right = c == 0, c == nc - 1
    up, down = jnp.logical_not(first), jnp.logical_not(last)
    west, east = jnp.logical_not(left), jnp.logical_not(right)

    loads = [
        pltpu.make_async_copy(x_hbm.at[:, :, pl.ds(128 * t, 128)], xs.at[:, t, pl.ds(8, ROWS), :], load_sem.at[t])
        for t in range(4)
    ]
    loads += [
        pltpu.make_async_copy(tlow_hbm.at[left.astype(jnp.int32)], tv.at[pl.ds(0, 128)], load_sem.at[4]),
        pltpu.make_async_copy(tmid_hbm, tv.at[pl.ds(128, 256)], load_sem.at[5]),
        pltpu.make_async_copy(thigh_hbm.at[right.astype(jnp.int32)], tv.at[pl.ds(384, 128)], load_sem.at[6]),
        pltpu.make_async_copy(v1_hbm, v1, load_sem.at[7]),
        pltpu.make_async_copy(s1_hbm, s1, load_sem.at[8]),
        pltpu.make_async_copy(w2_hbm, w2, load_sem.at[9]),
        pltpu.make_async_copy(w345_hbm, w345, load_sem.at[10]),
        pltpu.make_async_copy(arrive_hbm, arrive, load_sem.at[11]),
    ]
    for copy in loads:
        copy.start()

    def there(dr, dc):
        ok = jnp.bool_(True)
        if dr:
            ok = jnp.logical_and(ok, up if dr < 0 else down)
        if dc:
            ok = jnp.logical_and(ok, west if dc < 0 else east)
        return ok

    edge = pl.ds(256, 128)
    messages = [
        (rh, rh_in, 1, 0),
        (rh.at[:, :, edge], chm, 1, 1),
        (rh.at[:, :, edge], chp, 1, -1),
        (rl, rl_in, -1, 0),
        (rl.at[:, :, edge], clm, -1, 1),
        (rl.at[:, :, edge], clp, -1, -1),
        (cb, cbm, 0, 1),
        (cb, cbp, 0, -1),
    ]
    barrier = pltpu.get_barrier_semaphore()
    for _, dst, dr, dc in messages:

        @pl.when(there(dr, dc))
        def _(dr=dr, dc=dc):
            pl.semaphore_signal(barrier, inc=1, device_id=(r + dr, c + dc), device_id_type=MESH)

        @pl.when(jnp.logical_not(there(-dr, -dc)))
        def _(dst=dst):
            dst[...] = jnp.zeros_like(dst)

    ys = (xs, y1, y2, y3, y4, y5)
    for k in range(LEVELS):
        ys[k][:, :, 0:8, :] = jnp.zeros((CH, 4, 8, 128), F32)
        ys[k][:, :, 8 + H[k] : 32 + H[k], :] = jnp.zeros((CH, 4, 24, 128), F32)
    srs[...] = jnp.zeros_like(srs)
    ri[...] = jnp.zeros_like(ri)
    ci[...] = jnp.zeros_like(ci)
    rh[...] = jnp.zeros_like(rh)

    for t in range(4):
        loads[t].wait()
        mirror(xs, t, ROWS, first, last, True)
        for k in range(1, LEVELS + 1):
            reduce_rows(k, t, ys[k - 1], ys[k], first, last)

    for k in range(1, LEVELS + 1):
        for ch in range(CH):
            at = 16 * (k - 1) + 3 * ch
            srs[:, at : at + 3, :] = ys[k][ch, :, 7 + H[k] : 10 + H[k], :]
            at = 16 * (k - 1) + 9 + 2 * ch
            srs[:, at : at + 2, :] = ys[k][ch, :, 7:9, :]
    for copy in loads[4:7]:
        copy.wait()
    strips = jnp.concatenate([srs[t] for t in range(4)], axis=1)
    near = dot3(strips[0:32], tv[:, 0:512])
    deep = dot3(strips[32:80], tv[:, 512:1024])
    deep = deep[:, 0:256] + deep[:, 256:512]
    lane = lax.broadcasted_iota(jnp.int32, (16, 128), 1)
    cells = jnp.where(lane < 32, deep[16:32, 0:128], deep[32:48, 0:128])
    cells = jnp.where(lane < 24, deep[0:16, 0:128], cells)
    cells = jnp.where(lane < 8, near[0:16, 256:384], jnp.where(lane < 16, near[16:32, 256:384], cells))
    small = jnp.where(lane < 64, deep[0:16, 128:256], jnp.where(lane < 96, deep[16:32, 128:256], deep[32:48, 128:256]))
    strips = jnp.concatenate([near[0:16, 0:256], cells, near[16:32, 384:512], small], axis=1)
    for ch in range(CH):
        rh[ch, 0:3, :] = strips[3 * ch : 3 * ch + 3]
        rl[ch, :, :] = strips[9 + 2 * ch : 11 + 2 * ch]

    neighbours = (up.astype(jnp.int32) + down.astype(jnp.int32) + 1) * (
        west.astype(jnp.int32) + east.astype(jnp.int32) + 1
    ) - 1
    pl.semaphore_wait(barrier, neighbours)
    copies = []
    for m, (src, dst, dr, dc) in enumerate(messages):
        copies.append(
            pltpu.make_async_remote_copy(
                src_ref=src, dst_ref=dst, send_sem=send_sem.at[m], recv_sem=recv_sem.at[m],
                device_id=(r + dr, c + dc), device_id_type=MESH,
            )
        )
        if m < 6:
            pl.when(there(dr, dc))(copies[m].start)

    outer = jnp.concatenate([rows_of(k, ys[k], (0, 3)) for k in range(1, LEVELS + 1)], axis=0)
    table = jnp.concatenate([tv[0:128], tv[384:512]], axis=0)
    turned = dot3(outer, jnp.concatenate([table[:, 256:384], table[:, 768:896]], axis=1))
    turned = jnp.concatenate([turned[:, 0:128] + turned[:, 128:256], jnp.zeros((32, 128), F32)], axis=0)
    turned = jnp.transpose(turned)
    place = lax.broadcasted_iota(jnp.int32, (8, 512), 1)

    def of_level(k, a):
        ok = place < (BASE[k + 1] if k < LEVELS else 480)
        return jnp.where(jnp.logical_and(ok, place >= BASE[k]), a, 0.0)

    cb[...] = sum(of_level(k, turned[8 * (k - 1) : 8 * k]) for k in range(1, LEVELS + 1))
    for m in (6, 7):
        pl.when(there(*messages[m][2:]))(copies[m].start)

    for copy in loads[7:]:
        copy.wait()
    p12 = dot3(jnp.concatenate([rows_of(k, ys[k], range(4)) for k in (1, 2)], axis=0), tv[:, 0:512])
    p345 = dot3(jnp.concatenate([rows_of(k, ys[k], range(4)) for k in (3, 4, 5)], axis=0), tv[:, 512:1024])
    p345 = p345[:, 0:256] + p345[:, 256:512]

    def put(k, a, out):
        for ch in range(CH):
            for t in range(out.shape[1]):
                out[ch, t] = a[R[k] * ch : R[k] * (ch + 1), 128 * t : 128 * (t + 1)]

    put(1, dot3(p12[0:224, 0:384], v1[...]), g1)
    put(1, p12, m1)
    both = dot3(p12[208:336, 256:512], w2[...])
    put(2, both[8:, 0:256], g2)
    put(2, both[8:, 256:384], m2)
    deeper = ((3, 0, g3, m3), (4, 72, g4, m4), (5, 112, g5, m5))
    for k, at, g, m in deeper:
        both = dot3(p345[at : at + 16 * -(-3 * R[k] // 16)], w345[k - 3])
        skip = BASE[k] - BASE[3] - at
        put(k, both[skip:, 0:128], g)
        put(k, both[skip:, 128:256], m)

    def add(k, a, out, tiles, first_tile=0):
        for ch in range(CH):
            for i, t in enumerate(tiles):
                lanes = 128 * (first_tile + i)
                out[ch, t] += a[R[k] * ch : R[k] * (ch + 1), lanes : lanes + 128]

    for m in (6, 7):
        pl.when(there(-messages[m][2], -messages[m][3]))(copies[m].wait_recv)
    sub = lax.broadcasted_iota(jnp.int32, (8, 512), 0)
    terms = [a.astype(F32) for a in split3(jnp.where(sub < 3, cbm[...], cbp[...]))]
    came = jnp.concatenate(
        [of_level(k, a) for k in range(1, LEVELS + 1) for a in terms] + [jnp.zeros((8, 512), F32)], axis=0
    )
    came = jnp.transpose(came)

    def arrived(k, at, rows, lanes, count):
        return jnp.dot(
            came[at : at + rows].astype(BF16), arrive[:, lanes : lanes + count], preferred_element_type=F32
        )[BASE[k] - at :]

    more = arrived(1, 0, 224, 0, 512)
    add(1, more, g1, (0, 3))
    add(1, more, m1, (0, 1), 2)
    more = arrived(2, 208, 128, 512, 384)
    add(2, more, g2, (0, 1))
    add(2, more, m2, (0,), 2)
    for k, at, g, m in deeper:
        more = arrived(k, BASE[3] + at, 16 * -(-3 * R[k] // 16), 896 + 256 * (k - 3), 256)
        add(k, more, g, (0,))
        add(k, more, m, (0,), 1)

    side = jnp.bitwise_and(lax.broadcasted_iota(jnp.int32, (1, 128), 1), 7) < 3

    def add_rows(strip, minus, plus, count, row_of):
        for ch in range(CH):
            ri[count * ch : count * (ch + 1), :] = strip[ch, 0:count, :]
            ci[count * ch : count * (ch + 1), :] = jnp.where(side, minus[ch, 0:count, :], plus[ch, 0:count, :])
        strips = ri[...]
        cells = strips[:, 256:384] + pltpu.roll(ci[...], 64, 1)
        wide = dot3(jnp.concatenate([strips[:, 0:256], cells], axis=1), v1[...])
        level = strips[:, 0:256] + dot3(cells, s1[...])
        both = [dot3(jnp.concatenate([cells, strips[:, 384:512]], axis=1), w2[...])]
        tail = jnp.concatenate([cells, strips[:, 512:640]], axis=1)
        both += [dot3(tail, w345[k - 3]) for k in (3, 4, 5)]
        pairs = [(1, wide, g1), (1, level, m1), (2, both[0][:, 0:256], g2), (2, both[0][:, 256:384], m2)]
        for (k, _, g, m), a in zip(deeper, both[1:]):
            pairs += [(k, a[:, 0:128], g), (k, a[:, 128:256], m)]
        for k, a, out in pairs:
            at = row_of(k) + 1
            for ch in range(CH):
                for t in range(out.shape[1]):
                    out[ch, t, at : at + count, :] += a[count * ch : count * (ch + 1), 128 * t : 128 * (t + 1)]

    def details(counts):
        for g, level, at, out, count in zip((g1, g2, g3, g4, g5), (xs, m1, m2, m3, m4), (8, 1, 1, 1, 1), (d0, d1, d2, d3w, d4w), counts):
            detail(g, level, at, out, count)
        d3[...] = d3w[:, 0, :, 0:64]
        d4[...] = d4w[:, 0, :, 0:32]
        d5[...] = m5[:, 0, 1:5, 0:16]

    for m in (3, 4, 5):
        pl.when(there(-messages[m][2], -messages[m][3]))(copies[m].wait_recv)
    add_rows(rl_in, clm, clp, 2, lambda k: H[k] - 1)
    for k, g in enumerate((g1, g2, g3, g4, g5), 1):
        g[:, :, H[k] + 1 : H[k] + 2, :] = g[:, :, pl.ds(jnp.where(last, H[k], H[k] + 1), 1), :]
    details(H[1:6])
    for m in range(3):
        pl.when(there(-messages[m][2], -messages[m][3]))(copies[m].wait_recv)
    ri[...] = jnp.zeros_like(ri)
    add_rows(rh_in, chm, chp, 3, lambda k: -1)
    details((4,) * 5)
    for copy, (_, _, dr, dc) in zip(copies, messages):
        pl.when(there(dr, dc))(copy.wait_send)


def result_kernel(d0, d1, d2, d3, d4, d5, o0, o1, o2, o3, o4, o5, sem):
    pairs = [(d0.at[:, t], o0.at[:, :, pl.ds(128 * t, 128)]) for t in range(4)]
    pairs += [(d1.at[:, t], o1.at[:, :, pl.ds(128 * t, 128)]) for t in range(2)]
    pairs += [(d2.at[:, 0], o2), (d3, o3), (d4, o4), (d5, o5)]
    copies = [pltpu.make_async_copy(src, dst, sem.at[i]) for i, (src, dst) in enumerate(pairs)]
    for copy in copies:
        copy.start()
    for copy in copies:
        copy.wait()


def body(orthophoto):
    def vmem(*shape, dtype=F32):
        return pltpu.VMEM(shape, dtype)

    held = [(CH, 4, H[0], 128), (CH, 2, H[1], 128), (CH, 1, H[2], 128)]
    held += [(CH, H[3], W[3]), (CH, H[4], W[4]), (CH, H[5], W[5])]
    scratch = [vmem(CH, 4, H[k] + 32, 128) for k in range(6)]
    scratch += [vmem(512, 1024, dtype=BF16), vmem(384, 512, dtype=BF16), vmem(128, 256, dtype=BF16)]
    scratch += [vmem(256, 384, dtype=BF16), vmem(3, 256, 256, dtype=BF16), vmem(128, 1664, dtype=BF16)]
    scratch += [vmem(4, 80, 128), vmem(16, 640), vmem(16, 128)]
    scratch += [vmem(CH, 4, 640), vmem(CH, 2, 640), vmem(8, 512)]
    scratch += [vmem(CH, 4, 640), vmem(CH, 2, 640), vmem(8, 512), vmem(8, 512)]
    scratch += [vmem(CH, 4, 128), vmem(CH, 4, 128), vmem(CH, 2, 128), vmem(CH, 2, 128)]
    scratch += [vmem(CH, t, R[k], 128) for k, t in ((1, 4), (2, 2), (3, 1), (4, 1), (5, 1))]
    scratch += [vmem(CH, t, R[k], 128) for k, t in ((1, 2), (2, 1), (3, 1), (4, 1), (5, 1))]
    scratch += [vmem(CH, 1, H[3], 128), vmem(CH, 1, H[4], 128)]
    scratch += [pltpu.SemaphoreType.DMA((n,)) for n in (12, 8, 8)]
    far = pl.BlockSpec(memory_space=pltpu.HBM)
    inside = pl.BlockSpec(memory_space=pltpu.VMEM)
    inputs = [pltpu.with_memory_space_constraint(jnp.asarray(a), pltpu.HBM) for a in (orthophoto, *tables())]
    arrays = pl.pallas_call(
        exchange_kernel,
        out_shape=[jax.ShapeDtypeStruct(shape, F32) for shape in held],
        in_specs=[far] * len(inputs),
        out_specs=[inside] * len(held),
        scratch_shapes=scratch,
        compiler_params=pltpu.CompilerParams(collective_id=0, has_side_effects=True, vmem_limit_bytes=24 << 20),
    )(*inputs)
    results = pl.pallas_call(
        result_kernel,
        out_shape=[jax.ShapeDtypeStruct((CH, H[k], W[k]), F32) for k in range(6)],
        in_specs=[inside] * len(held),
        out_specs=[far] * 6,
        scratch_shapes=[pltpu.SemaphoreType.DMA((10,))],
        compiler_params=pltpu.CompilerParams(vmem_limit_bytes=8 << 20),
    )(*arrays)
    return tuple(results)


def solution(mesh):
    placed = P(None, "rows", "cols")
    return jax.shard_map(body, mesh=mesh, in_specs=(placed,), out_specs=(placed,) * 6, check_vma=False)
```

```python
import functools

import jax
import jax.numpy as jnp
import numpy as np
from jax import lax
from jax.experimental import pallas as pl
from jax.experimental.pallas import tpu as pltpu
from jax.sharding import PartitionSpec as P

CH = 3
ROWS = 128
COLS = 512
LEVELS = 5
H = [ROWS >> k for k in range(6)]
W = [COLS >> k for k in range(6)]
R = [0, 72, 40, 24, 16, 8]
BASE = [0, 0, 216, 336, 408, 456]
POS = [0, 0, 0, 0, 64, 96]
F32 = jnp.float32
BF16 = jnp.bfloat16
MESH = pl.DeviceIdType.MESH
TAPS = (1.0, 4.0, 6.0, 4.0, 1.0)


def column_reductions(low, high):
    result = [None]
    total = None
    for k in range(1, LEVELS + 1):
        n = W[k - 1]
        step = np.zeros((n + 3, W[k] + 3))
        for j in range(0 if low else -1, W[k] if high else W[k] + 2):
            for tap in range(5):
                cell = 2 * j - 2 + tap
                if low and cell < 0:
                    cell = -cell
                if high and cell > n - 1:
                    cell = 2 * (n - 1) - cell
                if -1 <= cell <= n + 1:
                    step[cell + 1, j + 1] += TAPS[tap] / 16
        total = step[1 : n + 1] if k == 1 else total @ step
        result.append(total / 16.0**k)
    return result


def reduction_table(low, high):
    t = column_reductions(low, high)

    def edge(k):
        cells = (W[k] - 1, W[k] - 1 if high else W[k], W[k] + 1, 1 if low else -1, 0)
        return t[k][:, [c + 1 for c in cells]]

    first = np.zeros((COLS, 512))
    first[:, 0:256] = t[1][:, 1:257]
    first[:, 384:512] = t[2][:, 1:129]
    last = np.zeros((COLS, 256))
    for k in (3, 4, 5):
        last[:, 8 * (k - 1) : 8 * (k - 1) + 5] = edge(k)
        last[:, 128 + POS[k] : 128 + POS[k] + W[k]] = t[k][:, 1 : W[k] + 1]
    for k in (1, 2):
        first[:, 256 + 8 * (k - 1) : 256 + 8 * (k - 1) + 5] = edge(k)
    top = np.asarray(last.astype(jnp.bfloat16), np.float64)
    rest = np.asarray((last - top).astype(jnp.bfloat16), np.float64)
    assert np.array_equal(top + rest, last)
    first[:, 272:296] = top[:, 16:40]
    assert np.array_equal(np.asarray(first.astype(jnp.bfloat16), np.float64), first)
    return np.concatenate([first, top, rest], axis=1)


def expansion_row(k, cell):
    row = np.zeros(2 * W[k])
    for i in range(W[k]):
        row[2 * i] += {i - 1: 0.125, i: 0.75, i + 1: 0.125}.get(cell, 0.0)
        row[2 * i + 1] += {i: 0.5, i + 1: 0.5}.get(cell, 0.0)
    return row


def expansion_table(k, main_at, edge_at, lanes):
    spread = np.zeros((lanes, 2 * W[k]))
    keep = np.zeros((lanes, W[k]))
    for c in range(W[k]):
        spread[main_at + c] = expansion_row(k, c)
        keep[main_at + c, c] = 1
    own = edge_at + 8 * (k - 1)
    came = own + 64
    spread[own + 1] = expansion_row(k, W[k])
    spread[own + 3] = expansion_row(k, -1)
    for s, cell in enumerate((-1, 0, 1, W[k] - 1, W[k])):
        spread[came + s] = expansion_row(k, cell)
        if 0 <= cell < W[k]:
            keep[came + s, cell] = 1
    return spread, keep


def arrival_table(k):
    spread = np.zeros((128, 2 * W[k]))
    keep = np.zeros((128, W[k]))
    for part in range(3):
        for s, cell in enumerate((-1, 0, 1, W[k] - 1, W[k])):
            lane = 24 * (k - 1) + 8 * part + s
            spread[lane] = expansion_row(k, cell)
            if 0 <= cell < W[k]:
                keep[lane, cell] = 1
    return spread, keep


def padded(a, cols):
    return np.pad(a, ((0, 0), (0, cols - a.shape[1])))


def tables():
    plain, low, high = (reduction_table(*e) for e in ((False, False), (True, False), (False, True)))
    assert np.array_equal(plain[128:], low[128:]) and np.array_equal(plain[:384], high[:384])
    t_low = np.stack([plain[:128], low[:128]])
    t_high = np.stack([plain[384:], high[384:]])
    v1, s1 = expansion_table(1, 0, 256, 384)
    w2 = np.concatenate(expansion_table(2, 128, 0, 256), axis=1)
    deep = []
    for k in (3, 4, 5):
        spread, keep = expansion_table(k, 128 + POS[k], 0, 256)
        deep.append(np.concatenate([padded(spread, 128), padded(keep, 128)], axis=1))
    spread, keep = arrival_table(1)
    assert not spread[:, 128:384].any()
    arrive = [spread[:, :128], spread[:, 384:], keep]
    arrive += arrival_table(2)
    for k in (3, 4, 5):
        arrive += [padded(a, 128) for a in arrival_table(k)]
    parts = (t_low, plain[128:384], t_high, v1, s1[256:], w2, np.stack(deep), np.concatenate(arrive, axis=1))
    return [a.astype(jnp.bfloat16) for a in parts]


def split3(a):
    top = a.astype(BF16)
    rest = a - top.astype(F32)
    mid = rest.astype(BF16)
    return top, mid, (rest - mid.astype(F32)).astype(BF16)


def dot3(a, table):
    m = a.shape[0]
    p = jnp.dot(jnp.concatenate(split3(a), axis=0), table, preferred_element_type=F32)
    return p[0:m] + p[m : 2 * m] + p[2 * m : 3 * m]


def reduce_rows(k, t, src, dst, first, last):
    h = H[k]
    count = R[k]

    def tap(ch, at, o):
        return src[ch, t, pl.ds(6 + 2 * at + o, 8, stride=2), :]

    for ch in range(CH):
        for at in range(0, count, 8):
            dst[ch, t, 7 + at : 15 + at, :] = (
                (tap(ch, at, -2) + tap(ch, at, 2)) + (tap(ch, at, -1) + tap(ch, at, 1)) * 4.0 + tap(ch, at, 0) * 6.0
            )
    mirror(dst, t, h, first, last, k < LEVELS)


def mirror(a, t, h, first, last, outer):
    a[:, t, 7:8, :] = a[:, t, pl.ds(jnp.where(first, 9, 7), 1), :]
    if outer:
        a[:, t, 6:7, :] = a[:, t, pl.ds(jnp.where(first, 10, 6), 1), :]
        a[:, t, 8 + h : 9 + h, :] = a[:, t, pl.ds(jnp.where(last, 6 + h, 8 + h), 1), :]


def rows_of(k, y, tiles):
    return jnp.concatenate(
        [jnp.concatenate([y[c, t, 7 : 7 + R[k], :] for t in tiles], axis=1) for c in range(CH)], axis=0
    )


def detail(g, level, at, out, count):
    lo, mid, hi = (g[:, :, i : i + count, :] for i in range(3))
    even, odd = pl.ds(at, count, stride=2), pl.ds(at + 1, count, stride=2)
    out[:, :, pl.ds(0, count, stride=2), :] = level[:, :, even, :] - ((lo + hi) * 0.125 + mid * 0.75)
    out[:, :, pl.ds(1, count, stride=2), :] = level[:, :, odd, :] - (mid + hi) * 0.5


def exchange_kernel(
    x_hbm, tlow_hbm, tmid_hbm, thigh_hbm, v1_hbm, s1_hbm, w2_hbm, w345_hbm, arrive_hbm,
    d0, d1, d2, d3, d4, d5,
    xs, y1, y2, y3, y4, y5, tv, v1, s1, w2, w345, arrive, srs, ri, ci,
    rh, rl, cb, rh_in, rl_in, cbm, cbp, chm, chp, clm, clp,
    g1, g2, g3, g4, g5, m1, m2, m3, m4, m5, d3w, d4w,
    load_sem, send_sem, recv_sem,
):
    r, c = lax.axis_index("rows"), lax.axis_index("cols")
    nr, nc = lax.axis_size("rows"), lax.axis_size("cols")
    first, last = r == 0, r == nr - 1
    left, right = c == 0, c == nc - 1
    up, down = jnp.logical_not(first), jnp.logical_not(last)
    west, east = jnp.logical_not(left), jnp.logical_not(right)

    loads = [
        pltpu.make_async_copy(x_hbm.at[:, :, pl.ds(128 * t, 128)], xs.at[:, t, pl.ds(8, ROWS), :], load_sem.at[t])
        for t in range(4)
    ]
    loads += [
        pltpu.make_async_copy(tlow_hbm.at[left.astype(jnp.int32)], tv.at[pl.ds(0, 128)], load_sem.at[4]),
        pltpu.make_async_copy(tmid_hbm, tv.at[pl.ds(128, 256)], load_sem.at[5]),
        pltpu.make_async_copy(thigh_hbm.at[right.astype(jnp.int32)], tv.at[pl.ds(384, 128)], load_sem.at[6]),
        pltpu.make_async_copy(v1_hbm, v1, load_sem.at[7]),
        pltpu.make_async_copy(s1_hbm, s1, load_sem.at[8]),
        pltpu.make_async_copy(w2_hbm, w2, load_sem.at[9]),
        pltpu.make_async_copy(w345_hbm, w345, load_sem.at[10]),
        pltpu.make_async_copy(arrive_hbm, arrive, load_sem.at[11]),
    ]
    for copy in loads[:7]:
        copy.start()

    def there(dr, dc):
        ok = jnp.bool_(True)
        if dr:
            ok = jnp.logical_and(ok, up if dr < 0 else down)
        if dc:
            ok = jnp.logical_and(ok, west if dc < 0 else east)
        return ok

    edge = pl.ds(256, 128)
    messages = [
        (rh, rh_in, 1, 0),
        (rh.at[:, :, edge], chm, 1, 1),
        (rh.at[:, :, edge], chp, 1, -1),
        (rl, rl_in, -1, 0),
        (rl.at[:, :, edge], clm, -1, 1),
        (rl.at[:, :, edge], clp, -1, -1),
        (cb, cbm, 0, 1),
        (cb, cbp, 0, -1),
    ]
    barrier = pltpu.get_barrier_semaphore()
    for _, dst, dr, dc in messages:

        @pl.when(there(dr, dc))
        def _(dr=dr, dc=dc):
            pl.semaphore_signal(barrier, inc=1, device_id=(r + dr, c + dc), device_id_type=MESH)

        @pl.when(jnp.logical_not(there(-dr, -dc)))
        def _(dst=dst):
            dst[...] = jnp.zeros_like(dst)

    ys = (xs, y1, y2, y3, y4, y5)
    for k in range(LEVELS):
        ys[k][:, :, 0:8, :] = jnp.zeros((CH, 4, 8, 128), F32)
        ys[k][:, :, 8 + H[k] : 32 + H[k], :] = jnp.zeros((CH, 4, 24, 128), F32)
    srs[...] = jnp.zeros_like(srs)
    ri[...] = jnp.zeros_like(ri)
    ci[...] = jnp.zeros_like(ci)
    rh[...] = jnp.zeros_like(rh)

    for copy in loads[:7]:
        copy.wait()
    for t in range(4):
        mirror(xs, t, ROWS, first, last, True)
    for k in range(1, LEVELS + 1):
        for t in range(4):
            reduce_rows(k, t, ys[k - 1], ys[k], first, last)

    for k in range(1, LEVELS + 1):
        for ch in range(CH):
            at = 16 * (k - 1) + 3 * ch
            srs[:, at : at + 3, :] = ys[k][ch, :, 7 + H[k] : 10 + H[k], :]
            at = 16 * (k - 1) + 9 + 2 * ch
            srs[:, at : at + 2, :] = ys[k][ch, :, 7:9, :]
    strips = jnp.concatenate([srs[t] for t in range(4)], axis=1)
    near = dot3(strips[0:32], tv[:, 0:512])
    deep = dot3(strips[32:80], tv[:, 512:1024])
    deep = deep[:, 0:256] + deep[:, 256:512]
    lane = lax.broadcasted_iota(jnp.int32, (16, 128), 1)
    cells = jnp.where(lane < 32, deep[16:32, 0:128], deep[32:48, 0:128])
    cells = jnp.where(lane < 24, deep[0:16, 0:128], cells)
    cells = jnp.where(lane < 8, near[0:16, 256:384], jnp.where(lane < 16, near[16:32, 256:384], cells))
    small = jnp.where(lane < 64, deep[0:16, 128:256], jnp.where(lane < 96, deep[16:32, 128:256], deep[32:48, 128:256]))
    strips = jnp.concatenate([near[0:16, 0:256], cells, near[16:32, 384:512], small], axis=1)
    for ch in range(CH):
        rh[ch, 0:3, :] = strips[3 * ch : 3 * ch + 3]
        rl[ch, :, :] = strips[9 + 2 * ch : 11 + 2 * ch]

    neighbours = (up.astype(jnp.int32) + down.astype(jnp.int32) + 1) * (
        west.astype(jnp.int32) + east.astype(jnp.int32) + 1
    ) - 1
    pl.semaphore_wait(barrier, neighbours)
    copies = []
    for m, (src, dst, dr, dc) in enumerate(messages):
        copies.append(
            pltpu.make_async_remote_copy(
                src_ref=src, dst_ref=dst, send_sem=send_sem.at[m], recv_sem=recv_sem.at[m],
                device_id=(r + dr, c + dc), device_id_type=MESH,
            )
        )
        if m < 6:
            pl.when(there(dr, dc))(copies[m].start)

    for copy in loads[7:]:
        copy.start()

    outer = jnp.concatenate([rows_of(k, ys[k], (0, 3)) for k in range(1, LEVELS + 1)], axis=0)
    table = jnp.concatenate([tv[0:128], tv[384:512]], axis=0)
    turned = dot3(outer, jnp.concatenate([table[:, 256:384], table[:, 768:896]], axis=1))
    turned = jnp.concatenate([turned[:, 0:128] + turned[:, 128:256], jnp.zeros((32, 128), F32)], axis=0)
    turned = jnp.transpose(turned)
    place = lax.broadcasted_iota(jnp.int32, (8, 512), 1)

    def of_level(k, a):
        ok = place < (BASE[k + 1] if k < LEVELS else 480)
        return jnp.where(jnp.logical_and(ok, place >= BASE[k]), a, 0.0)

    cb[...] = sum(of_level(k, turned[8 * (k - 1) : 8 * k]) for k in range(1, LEVELS + 1))
    for m in (6, 7):
        pl.when(there(*messages[m][2:]))(copies[m].start)

    for copy in loads[7:]:
        copy.wait()
    p12 = dot3(jnp.concatenate([rows_of(k, ys[k], range(4)) for k in (1, 2)], axis=0), tv[:, 0:512])
    p345 = dot3(jnp.concatenate([rows_of(k, ys[k], range(4)) for k in (3, 4, 5)], axis=0), tv[:, 512:1024])
    p345 = p345[:, 0:256] + p345[:, 256:512]

    def put(k, a, out):
        for ch in range(CH):
            for t in range(out.shape[1]):
                out[ch, t] = a[R[k] * ch : R[k] * (ch + 1), 128 * t : 128 * (t + 1)]

    put(1, dot3(p12[0:224, 0:384], v1[...]), g1)
    put(1, p12, m1)
    both = dot3(p12[208:336, 256:512], w2[...])
    put(2, both[8:, 0:256], g2)
    put(2, both[8:, 256:384], m2)
    deeper = ((3, 0, g3, m3), (4, 72, g4, m4), (5, 112, g5, m5))
    for k, at, g, m in deeper:
        both = dot3(p345[at : at + 16 * -(-3 * R[k] // 16)], w345[k - 3])
        skip = BASE[k] - BASE[3] - at
        put(k, both[skip:, 0:128], g)
        put(k, both[skip:, 128:256], m)

    def add(k, a, out, tiles, first_tile=0):
        for ch in range(CH):
            for i, t in enumerate(tiles):
                lanes = 128 * (first_tile + i)
                out[ch, t] += a[R[k] * ch : R[k] * (ch + 1), lanes : lanes + 128]

    for m in (6, 7):
        pl.when(there(-messages[m][2], -messages[m][3]))(copies[m].wait_recv)
    sub = lax.broadcasted_iota(jnp.int32, (8, 512), 0)
    terms = [a.astype(F32) for a in split3(jnp.where(sub < 3, cbm[...], cbp[...]))]
    came = jnp.concatenate(
        [of_level(k, a) for k in range(1, LEVELS + 1) for a in terms] + [jnp.zeros((8, 512), F32)], axis=0
    )
    came = jnp.transpose(came)

    def arrived(k, at, rows, lanes, count):
        return jnp.dot(
            came[at : at + rows].astype(BF16), arrive[:, lanes : lanes + count], preferred_element_type=F32
        )[BASE[k] - at :]

    more = arrived(1, 0, 224, 0, 512)
    add(1, more, g1, (0, 3))
    add(1, more, m1, (0, 1), 2)
    more = arrived(2, 208, 128, 512, 384)
    add(2, more, g2, (0, 1))
    add(2, more, m2, (0,), 2)
    for k, at, g, m in deeper:
        more = arrived(k, BASE[3] + at, 16 * -(-3 * R[k] // 16), 896 + 256 * (k - 3), 256)
        add(k, more, g, (0,))
        add(k, more, m, (0,), 1)

    side = jnp.bitwise_and(lax.broadcasted_iota(jnp.int32, (1, 128), 1), 7) < 3

    def add_rows(strip, minus, plus, count, row_of):
        for ch in range(CH):
            ri[count * ch : count * (ch + 1), :] = strip[ch, 0:count, :]
            ci[count * ch : count * (ch + 1), :] = jnp.where(side, minus[ch, 0:count, :], plus[ch, 0:count, :])
        strips = ri[...]
        cells = strips[:, 256:384] + pltpu.roll(ci[...], 64, 1)
        wide = dot3(jnp.concatenate([strips[:, 0:256], cells], axis=1), v1[...])
        level = strips[:, 0:256] + dot3(cells, s1[...])
        both = [dot3(jnp.concatenate([cells, strips[:, 384:512]], axis=1), w2[...])]
        tail = jnp.concatenate([cells, strips[:, 512:640]], axis=1)
        both += [dot3(tail, w345[k - 3]) for k in (3, 4, 5)]
        pairs = [(1, wide, g1), (1, level, m1), (2, both[0][:, 0:256], g2), (2, both[0][:, 256:384], m2)]
        for (k, _, g, m), a in zip(deeper, both[1:]):
            pairs += [(k, a[:, 0:128], g), (k, a[:, 128:256], m)]
        for k, a, out in pairs:
            at = row_of(k) + 1
            for ch in range(CH):
                for t in range(out.shape[1]):
                    out[ch, t, at : at + count, :] += a[count * ch : count * (ch + 1), 128 * t : 128 * (t + 1)]

    def details(counts):
        for g, level, at, out, count in zip((g1, g2, g3, g4, g5), (xs, m1, m2, m3, m4), (8, 1, 1, 1, 1), (d0, d1, d2, d3w, d4w), counts):
            detail(g, level, at, out, count)
        d3[...] = d3w[:, 0, :, 0:64]
        d4[...] = d4w[:, 0, :, 0:32]
        d5[...] = m5[:, 0, 1:5, 0:16]

    for m in (3, 4, 5):
        pl.when(there(-messages[m][2], -messages[m][3]))(copies[m].wait_recv)
    add_rows(rl_in, clm, clp, 2, lambda k: H[k] - 1)
    for k, g in enumerate((g1, g2, g3, g4, g5), 1):
        g[:, :, H[k] + 1 : H[k] + 2, :] = g[:, :, pl.ds(jnp.where(last, H[k], H[k] + 1), 1), :]
    details(H[1:6])
    for m in range(3):
        pl.when(there(-messages[m][2], -messages[m][3]))(copies[m].wait_recv)
    ri[...] = jnp.zeros_like(ri)
    add_rows(rh_in, chm, chp, 3, lambda k: -1)
    details((4,) * 5)
    for copy, (_, _, dr, dc) in zip(copies, messages):
        pl.when(there(dr, dc))(copy.wait_send)


def result_kernel(d0, d1, d2, d3, d4, d5, o0, o1, o2, o3, o4, o5, sem):
    pairs = [(d0.at[:, t], o0.at[:, :, pl.ds(128 * t, 128)]) for t in range(4)]
    pairs += [(d1.at[:, t], o1.at[:, :, pl.ds(128 * t, 128)]) for t in range(2)]
    pairs += [(d2.at[:, 0], o2), (d3, o3), (d4, o4), (d5, o5)]
    copies = [pltpu.make_async_copy(src, dst, sem.at[i]) for i, (src, dst) in enumerate(pairs)]
    for copy in copies:
        copy.start()
    for copy in copies:
        copy.wait()


def body(orthophoto):
    def vmem(*shape, dtype=F32):
        return pltpu.VMEM(shape, dtype)

    held = [(CH, 4, H[0], 128), (CH, 2, H[1], 128), (CH, 1, H[2], 128)]
    held += [(CH, H[3], W[3]), (CH, H[4], W[4]), (CH, H[5], W[5])]
    scratch = [vmem(CH, 4, H[k] + 32, 128) for k in range(6)]
    scratch += [vmem(512, 1024, dtype=BF16), vmem(384, 512, dtype=BF16), vmem(128, 256, dtype=BF16)]
    scratch += [vmem(256, 384, dtype=BF16), vmem(3, 256, 256, dtype=BF16), vmem(128, 1664, dtype=BF16)]
    scratch += [vmem(4, 80, 128), vmem(16, 640), vmem(16, 128)]
    scratch += [vmem(CH, 4, 640), vmem(CH, 2, 640), vmem(8, 512)]
    scratch += [vmem(CH, 4, 640), vmem(CH, 2, 640), vmem(8, 512), vmem(8, 512)]
    scratch += [vmem(CH, 4, 128), vmem(CH, 4, 128), vmem(CH, 2, 128), vmem(CH, 2, 128)]
    scratch += [vmem(CH, t, R[k], 128) for k, t in ((1, 4), (2, 2), (3, 1), (4, 1), (5, 1))]
    scratch += [vmem(CH, t, R[k], 128) for k, t in ((1, 2), (2, 1), (3, 1), (4, 1), (5, 1))]
    scratch += [vmem(CH, 1, H[3], 128), vmem(CH, 1, H[4], 128)]
    scratch += [pltpu.SemaphoreType.DMA((n,)) for n in (12, 8, 8)]
    far = pl.BlockSpec(memory_space=pltpu.HBM)
    inside = pl.BlockSpec(memory_space=pltpu.VMEM)
    inputs = [pltpu.with_memory_space_constraint(jnp.asarray(a), pltpu.HBM) for a in (orthophoto, *tables())]
    arrays = pl.pallas_call(
        exchange_kernel,
        out_shape=[jax.ShapeDtypeStruct(shape, F32) for shape in held],
        in_specs=[far] * len(inputs),
        out_specs=[inside] * len(held),
        scratch_shapes=scratch,
        compiler_params=pltpu.CompilerParams(collective_id=0, has_side_effects=True, vmem_limit_bytes=24 << 20),
    )(*inputs)
    results = pl.pallas_call(
        result_kernel,
        out_shape=[jax.ShapeDtypeStruct((CH, H[k], W[k]), F32) for k in range(6)],
        in_specs=[inside] * len(held),
        out_specs=[far] * 6,
        scratch_shapes=[pltpu.SemaphoreType.DMA((10,))],
        compiler_params=pltpu.CompilerParams(vmem_limit_bytes=8 << 20),
    )(*arrays)
    return tuple(results)


def solution(mesh):
    placed = P(None, "rows", "cols")
    return jax.shard_map(body, mesh=mesh, in_specs=(placed,), out_specs=(placed,) * 6, check_vma=False)
```

```python
import functools

import jax
import jax.numpy as jnp
import numpy as np
from jax import lax
from jax.experimental import pallas as pl
from jax.experimental.pallas import tpu as pltpu
from jax.sharding import PartitionSpec as P

CH = 3
ROWS = 128
COLS = 512
LEVELS = 5
H = [ROWS >> k for k in range(6)]
W = [COLS >> k for k in range(6)]
R = [0, 72, 40, 24, 16, 8]
BASE = [0, 0, 216, 336, 408, 456]
POS = [0, 0, 0, 0, 64, 96]
F32 = jnp.float32
BF16 = jnp.bfloat16
MESH = pl.DeviceIdType.MESH
TAPS = (1.0, 4.0, 6.0, 4.0, 1.0)


def column_reductions(low, high):
    result = [None]
    total = None
    for k in range(1, LEVELS + 1):
        n = W[k - 1]
        step = np.zeros((n + 3, W[k] + 3))
        for j in range(0 if low else -1, W[k] if high else W[k] + 2):
            for tap in range(5):
                cell = 2 * j - 2 + tap
                if low and cell < 0:
                    cell = -cell
                if high and cell > n - 1:
                    cell = 2 * (n - 1) - cell
                if -1 <= cell <= n + 1:
                    step[cell + 1, j + 1] += TAPS[tap] / 16
        total = step[1 : n + 1] if k == 1 else total @ step
        result.append(total / 16.0**k)
    return result


def reduction_table(low, high):
    t = column_reductions(low, high)

    def fill(a, at, k):
        beyond, before = W[k] - 1 if high else W[k], 1 if low else -1
        cells = (W[k] - 1, beyond, W[k] + 1, before, 0)
        a[:, at + 8 * (k - 1) : at + 8 * (k - 1) + 5] = t[k][:, [c + 1 for c in cells]]
        a[:, at + 112 + 2 * (k - 1) : at + 114 + 2 * (k - 1)] = t[k][:, [beyond + 1, before + 1]]

    first = np.zeros((COLS, 512))
    first[:, 0:256] = t[1][:, 1:257]
    first[:, 384:512] = t[2][:, 1:129]
    last = np.zeros((COLS, 256))
    for k in (3, 4, 5):
        fill(last, 0, k)
        last[:, 128 + POS[k] : 128 + POS[k] + W[k]] = t[k][:, 1 : W[k] + 1]
    for k in (1, 2):
        fill(first, 256, k)
    top = np.asarray(last.astype(jnp.bfloat16), np.float64)
    rest = np.asarray((last - top).astype(jnp.bfloat16), np.float64)
    assert np.array_equal(top + rest, last)
    first[:, 272:296] = top[:, 16:40]
    assert np.array_equal(np.asarray(first.astype(jnp.bfloat16), np.float64), first)
    return np.concatenate([first, top, rest], axis=1)


def expansion_row(k, cell):
    row = np.zeros(2 * W[k])
    for i in range(W[k]):
        row[2 * i] += {i - 1: 0.125, i: 0.75, i + 1: 0.125}.get(cell, 0.0)
        row[2 * i + 1] += {i: 0.5, i + 1: 0.5}.get(cell, 0.0)
    return row


def expansion_table(k, main_at, edge_at, lanes):
    spread = np.zeros((lanes, 2 * W[k]))
    keep = np.zeros((lanes, W[k]))
    for c in range(W[k]):
        spread[main_at + c] = expansion_row(k, c)
        keep[main_at + c, c] = 1
    own = edge_at + 112 + 2 * (k - 1)
    came = edge_at + 64 + 8 * (k - 1)
    spread[own] = expansion_row(k, W[k])
    spread[own + 1] = expansion_row(k, -1)
    for s, cell in enumerate((-1, 0, 1, W[k] - 1, W[k])):
        spread[came + s] = expansion_row(k, cell)
        if 0 <= cell < W[k]:
            keep[came + s, cell] = 1
    return spread, keep


def arrival_table(k):
    spread = np.zeros((128, 2 * W[k]))
    keep = np.zeros((128, W[k]))
    for part in range(3):
        for s, cell in enumerate((-1, 0, 1, W[k] - 1, W[k])):
            lane = 24 * (k - 1) + 8 * part + s
            spread[lane] = expansion_row(k, cell)
            if 0 <= cell < W[k]:
                keep[lane, cell] = 1
    return spread, keep


def padded(a, cols):
    return np.pad(a, ((0, 0), (0, cols - a.shape[1])))


def tables():
    plain, low, high = (reduction_table(*e) for e in ((False, False), (True, False), (False, True)))
    assert np.array_equal(plain[128:], low[128:]) and np.array_equal(plain[:384], high[:384])
    t_low = np.stack([plain[:128], low[:128]])
    t_high = np.stack([plain[384:], high[384:]])
    v1, s1 = expansion_table(1, 0, 256, 384)
    w2 = np.concatenate(expansion_table(2, 128, 0, 256), axis=1)
    deep = []
    for k in (3, 4, 5):
        spread, keep = expansion_table(k, 128 + POS[k], 0, 256)
        deep.append(np.concatenate([padded(spread, 128), padded(keep, 128)], axis=1))
    spread, keep = arrival_table(1)
    assert not spread[:, 128:384].any()
    arrive = [spread[:, :128], spread[:, 384:], keep]
    arrive += arrival_table(2)
    for k in (3, 4, 5):
        arrive += [padded(a, 128) for a in arrival_table(k)]
    parts = (t_low, plain[128:384], t_high, v1, s1[256:], w2, np.stack(deep), np.concatenate(arrive, axis=1))
    return [a.astype(jnp.bfloat16) for a in parts]


def split3(a):
    top = a.astype(BF16)
    rest = a - top.astype(F32)
    mid = rest.astype(BF16)
    return top, mid, (rest - mid.astype(F32)).astype(BF16)


def dot3(a, table):
    m = a.shape[0]
    p = jnp.dot(jnp.concatenate(split3(a), axis=0), table, preferred_element_type=F32)
    return p[0:m] + p[m : 2 * m] + p[2 * m : 3 * m]


def reduce_rows(k, t, src, dst, first, last):
    h = H[k]
    count = R[k]

    def tap(ch, at, o):
        return src[ch, t, pl.ds(6 + 2 * at + o, 8, stride=2), :]

    for ch in range(CH):
        for at in range(0, count, 8):
            dst[ch, t, 7 + at : 15 + at, :] = (
                (tap(ch, at, -2) + tap(ch, at, 2)) + (tap(ch, at, -1) + tap(ch, at, 1)) * 4.0 + tap(ch, at, 0) * 6.0
            )
    mirror(dst, t, h, first, last, k < LEVELS)


def mirror(a, t, h, first, last, outer):
    a[:, t, 7:8, :] = a[:, t, pl.ds(jnp.where(first, 9, 7), 1), :]
    if outer:
        a[:, t, 6:7, :] = a[:, t, pl.ds(jnp.where(first, 10, 6), 1), :]
        a[:, t, 8 + h : 9 + h, :] = a[:, t, pl.ds(jnp.where(last, 6 + h, 8 + h), 1), :]


def rows_of(k, y, tiles):
    return jnp.concatenate(
        [jnp.concatenate([y[c, t, 7 : 7 + R[k], :] for t in tiles], axis=1) for c in range(CH)], axis=0
    )


def detail(g, level, at, out, count):
    lo, mid, hi = (g[:, :, i : i + count, :] for i in range(3))
    even, odd = pl.ds(at, count, stride=2), pl.ds(at + 1, count, stride=2)
    out[:, :, pl.ds(0, count, stride=2), :] = level[:, :, even, :] - ((lo + hi) * 0.125 + mid * 0.75)
    out[:, :, pl.ds(1, count, stride=2), :] = level[:, :, odd, :] - (mid + hi) * 0.5


def exchange_kernel(
    x_hbm, tlow_hbm, tmid_hbm, thigh_hbm, v1_hbm, s1_hbm, w2_hbm, w345_hbm, arrive_hbm,
    d0, d1, d2, d3, d4, d5,
    xs, y1, y2, y3, y4, y5, tv, v1, s1, w2, w345, arrive, srs, ci,
    rh, rl, kh, kl, cb, rh_in, rl_in, cbm, cbp, chm, chp, clm, clp,
    g1, g2, g3, g4, g5, m1, m2, m3, m4, m5, d3w, d4w,
    load_sem, send_sem, recv_sem,
):
    r, c = lax.axis_index("rows"), lax.axis_index("cols")
    nr, nc = lax.axis_size("rows"), lax.axis_size("cols")
    first, last = r == 0, r == nr - 1
    left, right = c == 0, c == nc - 1
    up, down = jnp.logical_not(first), jnp.logical_not(last)
    west, east = jnp.logical_not(left), jnp.logical_not(right)

    loads = [
        pltpu.make_async_copy(x_hbm.at[:, :, pl.ds(128 * t, 128)], xs.at[:, t, pl.ds(8, ROWS), :], load_sem.at[t])
        for t in range(4)
    ]
    loads += [
        pltpu.make_async_copy(tlow_hbm.at[left.astype(jnp.int32)], tv.at[pl.ds(0, 128)], load_sem.at[4]),
        pltpu.make_async_copy(tmid_hbm, tv.at[pl.ds(128, 256)], load_sem.at[5]),
        pltpu.make_async_copy(thigh_hbm.at[right.astype(jnp.int32)], tv.at[pl.ds(384, 128)], load_sem.at[6]),
        pltpu.make_async_copy(v1_hbm, v1, load_sem.at[7]),
        pltpu.make_async_copy(s1_hbm, s1, load_sem.at[8]),
        pltpu.make_async_copy(w2_hbm, w2, load_sem.at[9]),
        pltpu.make_async_copy(w345_hbm, w345, load_sem.at[10]),
        pltpu.make_async_copy(arrive_hbm, arrive, load_sem.at[11]),
    ]
    for copy in loads[:7]:
        copy.start()

    def there(dr, dc):
        ok = jnp.bool_(True)
        if dr:
            ok = jnp.logical_and(ok, up if dr < 0 else down)
        if dc:
            ok = jnp.logical_and(ok, west if dc < 0 else east)
        return ok

    messages = [
        (rh, rh_in, 1, 0),
        (kh, chm, 1, 1),
        (kh, chp, 1, -1),
        (rl, rl_in, -1, 0),
        (kl, clm, -1, 1),
        (kl, clp, -1, -1),
        (cb, cbm, 0, 1),
        (cb, cbp, 0, -1),
    ]
    barrier = pltpu.get_barrier_semaphore()
    for _, dst, dr, dc in messages:

        @pl.when(there(dr, dc))
        def _(dr=dr, dc=dc):
            pl.semaphore_signal(barrier, inc=1, device_id=(r + dr, c + dc), device_id_type=MESH)

        @pl.when(jnp.logical_not(there(-dr, -dc)))
        def _(dst=dst):
            dst[...] = jnp.zeros_like(dst)

    ys = (xs, y1, y2, y3, y4, y5)
    for k in range(LEVELS):
        ys[k][:, :, 0:8, :] = jnp.zeros((CH, 4, 8, 128), F32)
        ys[k][:, :, 8 + H[k] : 32 + H[k], :] = jnp.zeros((CH, 4, 24, 128), F32)
    srs[...] = jnp.zeros_like(srs)
    ci[...] = jnp.zeros_like(ci)
    for a in (rh, kh, kl):
        a[...] = jnp.zeros_like(a)

    for copy in loads[:4]:
        copy.wait()
    for t in range(4):
        mirror(xs, t, ROWS, first, last, True)
    for k in range(1, LEVELS + 1):
        for t in range(4):
            reduce_rows(k, t, ys[k - 1], ys[k], first, last)

    for k in range(1, LEVELS + 1):
        for ch in range(CH):
            at = 16 * (k - 1) + 3 * ch
            srs[:, at : at + 3, :] = ys[k][ch, :, 7 + H[k] : 10 + H[k], :]
            at = 16 * (k - 1) + 9 + 2 * ch
            srs[:, at : at + 2, :] = ys[k][ch, :, 7:9, :]
    for copy in loads[4:7]:
        copy.wait()
    strips = jnp.concatenate([srs[t] for t in range(4)], axis=1)
    near = dot3(strips[0:32], tv[:, 0:512])
    deep = dot3(strips[32:80], tv[:, 512:1024])
    deep = deep[:, 0:256] + deep[:, 256:512]
    lane = lax.broadcasted_iota(jnp.int32, (16, 128), 1)
    cells = jnp.where(lane < 32, deep[16:32, 0:128], deep[32:48, 0:128])
    cells = jnp.where(lane < 24, deep[0:16, 0:128], cells)
    cells = jnp.where(lane < 8, near[0:16, 256:384], jnp.where(lane < 16, near[16:32, 256:384], cells))
    beside = jnp.where(lane < 118, deep[0:16, 0:128], jnp.where(lane < 120, deep[16:32, 0:128], deep[32:48, 0:128]))
    beside = jnp.where(lane < 114, near[0:16, 256:384], jnp.where(lane < 116, near[16:32, 256:384], beside))
    small = jnp.where(lane < 64, deep[0:16, 128:256], jnp.where(lane < 96, deep[16:32, 128:256], deep[32:48, 128:256]))
    small = jnp.where(lane < 112, small, beside)
    for t, a in enumerate((near[0:16, 0:128], near[0:16, 128:256], near[16:32, 384:512], small)):
        rh[pl.ds(t, 9, stride=4), :] = a[0:9]
        rl[pl.ds(t, 6, stride=4), :] = a[9:15]
    ci[...] = jnp.where(lane < 40, cells, 0.0)
    kh[0:3, :] = sum(pltpu.roll(ci[pl.ds(i, CH, stride=3), :], 40 * i, 1) for i in range(3))
    kl[0:3, :] = sum(pltpu.roll(ci[pl.ds(9 + i, CH, stride=2), :], 40 * i, 1) for i in range(2))

    neighbours = (up.astype(jnp.int32) + down.astype(jnp.int32) + 1) * (
        west.astype(jnp.int32) + east.astype(jnp.int32) + 1
    ) - 1
    pl.semaphore_wait(barrier, neighbours)
    copies = []
    for m, (src, dst, dr, dc) in enumerate(messages):
        copies.append(
            pltpu.make_async_remote_copy(
                src_ref=src, dst_ref=dst, send_sem=send_sem.at[m], recv_sem=recv_sem.at[m],
                device_id=(r + dr, c + dc), device_id_type=MESH,
            )
        )
        if m < 6:
            pl.when(there(dr, dc))(copies[m].start)

    for copy in loads[7:]:
        copy.start()

    outer = jnp.concatenate([rows_of(k, ys[k], (0, 3)) for k in range(1, LEVELS + 1)], axis=0)
    table = jnp.concatenate([tv[0:128], tv[384:512]], axis=0)
    turned = dot3(outer, jnp.concatenate([table[:, 256:384], table[:, 768:896]], axis=1))
    turned = jnp.concatenate([turned[:, 0:128] + turned[:, 128:256], jnp.zeros((32, 128), F32)], axis=0)
    turned = jnp.transpose(turned)
    place = lax.broadcasted_iota(jnp.int32, (8, 512), 1)

    def of_level(k, a):
        ok = place < (BASE[k + 1] if k < LEVELS else 480)
        return jnp.where(jnp.logical_and(ok, place >= BASE[k]), a, 0.0)

    cb[...] = sum(of_level(k, turned[8 * (k - 1) : 8 * k]) for k in range(1, LEVELS + 1))
    for m in (6, 7):
        pl.when(there(*messages[m][2:]))(copies[m].start)

    for copy in loads[7:]:
        copy.wait()
    p12 = dot3(jnp.concatenate([rows_of(k, ys[k], range(4)) for k in (1, 2)], axis=0), tv[:, 0:512])
    p345 = dot3(jnp.concatenate([rows_of(k, ys[k], range(4)) for k in (3, 4, 5)], axis=0), tv[:, 512:1024])
    p345 = p345[:, 0:256] + p345[:, 256:512]

    def put(k, a, out):
        for ch in range(CH):
            for t in range(out.shape[1]):
                out[ch, t] = a[R[k] * ch : R[k] * (ch + 1), 128 * t : 128 * (t + 1)]

    put(1, dot3(p12[0:224, 0:384], v1[...]), g1)
    put(1, p12, m1)
    both = dot3(p12[208:336, 256:512], w2[...])
    put(2, both[8:, 0:256], g2)
    put(2, both[8:, 256:384], m2)
    deeper = ((3, 0, g3, m3), (4, 72, g4, m4), (5, 112, g5, m5))
    for k, at, g, m in deeper:
        both = dot3(p345[at : at + 16 * -(-3 * R[k] // 16)], w345[k - 3])
        skip = BASE[k] - BASE[3] - at
        put(k, both[skip:, 0:128], g)
        put(k, both[skip:, 128:256], m)

    def add(k, a, out, tiles, first_tile=0):
        for ch in range(CH):
            for i, t in enumerate(tiles):
                lanes = 128 * (first_tile + i)
                out[ch, t] += a[R[k] * ch : R[k] * (ch + 1), lanes : lanes + 128]

    for m in (6, 7):
        pl.when(there(-messages[m][2], -messages[m][3]))(copies[m].wait_recv)
    sub = lax.broadcasted_iota(jnp.int32, (8, 512), 0)
    terms = [a.astype(F32) for a in split3(jnp.where(sub < 3, cbm[...], cbp[...]))]
    came = jnp.concatenate(
        [of_level(k, a) for k in range(1, LEVELS + 1) for a in terms] + [jnp.zeros((8, 512), F32)], axis=0
    )
    came = jnp.transpose(came)

    def arrived(k, at, rows, lanes, count):
        return jnp.dot(
            came[at : at + rows].astype(BF16), arrive[:, lanes : lanes + count], preferred_element_type=F32
        )[BASE[k] - at :]

    more = arrived(1, 0, 224, 0, 512)
    add(1, more, g1, (0, 3))
    add(1, more, m1, (0, 1), 2)
    more = arrived(2, 208, 128, 512, 384)
    add(2, more, g2, (0, 1))
    add(2, more, m2, (0,), 2)
    for k, at, g, m in deeper:
        more = arrived(k, BASE[3] + at, 16 * -(-3 * R[k] // 16), 896 + 256 * (k - 3), 256)
        add(k, more, g, (0,))
        add(k, more, m, (0,), 1)

    side = jnp.bitwise_and(lane, 7) < 3
    middle = jnp.logical_and(lane >= 64, lane < 104)
    ci[...] = jnp.zeros_like(ci)

    def add_rows(strip, minus, plus, count, row_of):
        corner = jnp.where(side[0:4], minus[...], plus[...])
        for i in range(count):
            ci[pl.ds(i, CH, stride=count), :] = pltpu.roll(corner, (64 - 40 * i) % 128, 1)[0:CH]
        rows = CH * count
        fill = jnp.zeros((16 - rows, 128), F32)
        tiles = [jnp.concatenate([strip[pl.ds(t, rows, stride=4), :], fill], axis=0) for t in range(4)]
        cells = jnp.where(lane < 112, jnp.where(middle, ci[...], 0.0), tiles[3])
        wide = dot3(jnp.concatenate([tiles[0], tiles[1], cells], axis=1), v1[...])
        level = jnp.concatenate(tiles[0:2], axis=1) + dot3(cells, s1[...])
        both = [dot3(jnp.concatenate([cells, tiles[2]], axis=1), w2[...])]
        tail = jnp.concatenate([cells, tiles[3]], axis=1)
        both += [dot3(tail, w345[k - 3]) for k in (3, 4, 5)]
        pairs = [(1, wide, g1), (1, level, m1), (2, both[0][:, 0:256], g2), (2, both[0][:, 256:384], m2)]
        for (k, _, g, m), a in zip(deeper, both[1:]):
            pairs += [(k, a[:, 0:128], g), (k, a[:, 128:256], m)]
        for k, a, out in pairs:
            at = row_of(k) + 1
            for ch in range(CH):
                for t in range(out.shape[1]):
                    out[ch, t, at : at + count, :] += a[count * ch : count * (ch + 1), 128 * t : 128 * (t + 1)]

    def details(counts):
        for g, level, at, out, count in zip((g1, g2, g3, g4, g5), (xs, m1, m2, m3, m4), (8, 1, 1, 1, 1), (d0, d1, d2, d3w, d4w), counts):
            detail(g, level, at, out, count)
        d3[...] = d3w[:, 0, :, 0:64]
        d4[...] = d4w[:, 0, :, 0:32]
        d5[...] = m5[:, 0, 1:5, 0:16]

    for m in (3, 4, 5):
        pl.when(there(-messages[m][2], -messages[m][3]))(copies[m].wait_recv)
    add_rows(rl_in, clm, clp, 2, lambda k: H[k] - 1)
    for k, g in enumerate((g1, g2, g3, g4, g5), 1):
        g[:, :, H[k] + 1 : H[k] + 2, :] = g[:, :, pl.ds(jnp.where(last, H[k], H[k] + 1), 1), :]
    details(H[1:6])
    for m in range(3):
        pl.when(there(-messages[m][2], -messages[m][3]))(copies[m].wait_recv)
    add_rows(rh_in, chm, chp, 3, lambda k: -1)
    details((4,) * 5)
    for copy, (_, _, dr, dc) in zip(copies, messages):
        pl.when(there(dr, dc))(copy.wait_send)


def result_kernel(d0, d1, d2, d3, d4, d5, o0, o1, o2, o3, o4, o5, sem):
    pairs = [(d0.at[:, t], o0.at[:, :, pl.ds(128 * t, 128)]) for t in range(4)]
    pairs += [(d1.at[:, t], o1.at[:, :, pl.ds(128 * t, 128)]) for t in range(2)]
    pairs += [(d2.at[:, 0], o2), (d3, o3), (d4, o4), (d5, o5)]
    copies = [pltpu.make_async_copy(src, dst, sem.at[i]) for i, (src, dst) in enumerate(pairs)]
    for copy in copies:
        copy.start()
    for copy in copies:
        copy.wait()


def body(orthophoto):
    def vmem(*shape, dtype=F32):
        return pltpu.VMEM(shape, dtype)

    held = [(CH, 4, H[0], 128), (CH, 2, H[1], 128), (CH, 1, H[2], 128)]
    held += [(CH, H[3], W[3]), (CH, H[4], W[4]), (CH, H[5], W[5])]
    scratch = [vmem(CH, 4, H[k] + 32, 128) for k in range(6)]
    scratch += [vmem(512, 1024, dtype=BF16), vmem(384, 512, dtype=BF16), vmem(128, 256, dtype=BF16)]
    scratch += [vmem(256, 384, dtype=BF16), vmem(3, 256, 256, dtype=BF16), vmem(128, 1664, dtype=BF16)]
    scratch += [vmem(4, 80, 128), vmem(16, 128)]
    scratch += [vmem(40, 128), vmem(24, 128), vmem(4, 128), vmem(4, 128), vmem(8, 512)]
    scratch += [vmem(40, 128), vmem(24, 128), vmem(8, 512), vmem(8, 512)]
    scratch += [vmem(4, 128)] * 4
    scratch += [vmem(CH, t, R[k], 128) for k, t in ((1, 4), (2, 2), (3, 1), (4, 1), (5, 1))]
    scratch += [vmem(CH, t, R[k], 128) for k, t in ((1, 2), (2, 1), (3, 1), (4, 1), (5, 1))]
    scratch += [vmem(CH, 1, H[3], 128), vmem(CH, 1, H[4], 128)]
    scratch += [pltpu.SemaphoreType.DMA((n,)) for n in (12, 8, 8)]
    far = pl.BlockSpec(memory_space=pltpu.HBM)
    inside = pl.BlockSpec(memory_space=pltpu.VMEM)
    inputs = [pltpu.with_memory_space_constraint(jnp.asarray(a), pltpu.HBM) for a in (orthophoto, *tables())]
    arrays = pl.pallas_call(
        exchange_kernel,
        out_shape=[jax.ShapeDtypeStruct(shape, F32) for shape in held],
        in_specs=[far] * len(inputs),
        out_specs=[inside] * len(held),
        scratch_shapes=scratch,
        compiler_params=pltpu.CompilerParams(collective_id=0, has_side_effects=True, vmem_limit_bytes=24 << 20),
    )(*inputs)
    results = pl.pallas_call(
        result_kernel,
        out_shape=[jax.ShapeDtypeStruct((CH, H[k], W[k]), F32) for k in range(6)],
        in_specs=[inside] * len(held),
        out_specs=[far] * 6,
        scratch_shapes=[pltpu.SemaphoreType.DMA((10,))],
        compiler_params=pltpu.CompilerParams(vmem_limit_bytes=8 << 20),
    )(*arrays)
    return tuple(results)


def solution(mesh):
    placed = P(None, "rows", "cols")
    return jax.shard_map(body, mesh=mesh, in_specs=(placed,), out_specs=(placed,) * 6, check_vma=False)
```

```python
import functools

import jax
import jax.numpy as jnp
import numpy as np
from jax import lax
from jax.experimental import pallas as pl
from jax.experimental.pallas import tpu as pltpu
from jax.sharding import PartitionSpec as P

CH = 3
ROWS = 128
COLS = 512
LEVELS = 5
H = [ROWS >> k for k in range(6)]
W = [COLS >> k for k in range(6)]
R = [0, 72, 40, 24, 16, 8]
BASE = [0, 0, 216, 336, 408, 456]
POS = [0, 0, 0, 0, 64, 96]
F32 = jnp.float32
BF16 = jnp.bfloat16
MESH = pl.DeviceIdType.MESH
TAPS = (1.0, 4.0, 6.0, 4.0, 1.0)


def column_reductions(low, high):
    result = [None]
    total = None
    for k in range(1, LEVELS + 1):
        n = W[k - 1]
        step = np.zeros((n + 3, W[k] + 3))
        for j in range(0 if low else -1, W[k] if high else W[k] + 2):
            for tap in range(5):
                cell = 2 * j - 2 + tap
                if low and cell < 0:
                    cell = -cell
                if high and cell > n - 1:
                    cell = 2 * (n - 1) - cell
                if -1 <= cell <= n + 1:
                    step[cell + 1, j + 1] += TAPS[tap] / 16
        total = step[1 : n + 1] if k == 1 else total @ step
        result.append(total / 16.0**k)
    return result


def reduction_table(low, high):
    t = column_reductions(low, high)

    def fill(a, at, k):
        beyond, before = W[k] - 1 if high else W[k], 1 if low else -1
        cells = (W[k] - 1, beyond, W[k] + 1, before, 0)
        a[:, at + 8 * (k - 1) : at + 8 * (k - 1) + 5] = t[k][:, [c + 1 for c in cells]]
        a[:, at + 112 + 2 * (k - 1) : at + 114 + 2 * (k - 1)] = t[k][:, [beyond + 1, before + 1]]

    first = np.zeros((COLS, 512))
    first[:, 0:256] = t[1][:, 1:257]
    first[:, 384:512] = t[2][:, 1:129]
    last = np.zeros((COLS, 256))
    for k in (3, 4, 5):
        fill(last, 0, k)
        last[:, 128 + POS[k] : 128 + POS[k] + W[k]] = t[k][:, 1 : W[k] + 1]
    for k in (1, 2):
        fill(first, 256, k)
    top = np.asarray(last.astype(jnp.bfloat16), np.float64)
    rest = np.asarray((last - top).astype(jnp.bfloat16), np.float64)
    assert np.array_equal(top + rest, last)
    first[:, 272:296] = top[:, 16:40]
    assert np.array_equal(np.asarray(first.astype(jnp.bfloat16), np.float64), first)
    return np.concatenate([first, top, rest], axis=1)


def expansion_row(k, cell):
    row = np.zeros(2 * W[k])
    for i in range(W[k]):
        row[2 * i] += {i - 1: 0.125, i: 0.75, i + 1: 0.125}.get(cell, 0.0)
        row[2 * i + 1] += {i: 0.5, i + 1: 0.5}.get(cell, 0.0)
    return row


def expansion_table(k, main_at, edge_at, lanes):
    spread = np.zeros((lanes, 2 * W[k]))
    keep = np.zeros((lanes, W[k]))
    for c in range(W[k]):
        spread[main_at + c] = expansion_row(k, c)
        keep[main_at + c, c] = 1
    own = edge_at + 112 + 2 * (k - 1)
    came = edge_at + 64 + 8 * (k - 1)
    spread[own] = expansion_row(k, W[k])
    spread[own + 1] = expansion_row(k, -1)
    for s, cell in enumerate((-1, 0, 1, W[k] - 1, W[k])):
        spread[came + s] = expansion_row(k, cell)
        if 0 <= cell < W[k]:
            keep[came + s, cell] = 1
    return spread, keep


def arrival_table(k):
    spread = np.zeros((128, 2 * W[k]))
    keep = np.zeros((128, W[k]))
    for part in range(3):
        for s, cell in enumerate((-1, 0, 1, W[k] - 1, W[k])):
            lane = 24 * (k - 1) + 8 * part + s
            spread[lane] = expansion_row(k, cell)
            if 0 <= cell < W[k]:
                keep[lane, cell] = 1
    return spread, keep


def padded(a, cols):
    return np.pad(a, ((0, 0), (0, cols - a.shape[1])))


def tables():
    plain, low, high = (reduction_table(*e) for e in ((False, False), (True, False), (False, True)))
    assert np.array_equal(plain[128:], low[128:]) and np.array_equal(plain[:384], high[:384])
    t_low = np.stack([plain[:128], low[:128]])
    t_high = np.stack([plain[384:], high[384:]])
    v1, s1 = expansion_table(1, 0, 256, 384)
    w2 = np.concatenate(expansion_table(2, 128, 0, 256), axis=1)
    deep = []
    for k in (3, 4, 5):
        spread, keep = expansion_table(k, 128 + POS[k], 0, 256)
        deep.append(np.concatenate([padded(spread, 128), padded(keep, 128)], axis=1))
    spread, keep = arrival_table(1)
    assert not spread[:, 128:384].any()
    arrive = [spread[:, :128], spread[:, 384:], keep]
    arrive += arrival_table(2)
    for k in (3, 4, 5):
        arrive += [padded(a, 128) for a in arrival_table(k)]
    parts = (t_low, plain[128:384], t_high, v1, s1[256:], w2, np.stack(deep), np.concatenate(arrive, axis=1))
    return [a.astype(jnp.bfloat16) for a in parts]


def split3(a):
    top = a.astype(BF16)
    rest = a - top.astype(F32)
    mid = rest.astype(BF16)
    return top, mid, (rest - mid.astype(F32)).astype(BF16)


def dot3(a, table):
    m = a.shape[0]
    p = jnp.dot(jnp.concatenate(split3(a), axis=0), table, preferred_element_type=F32)
    return p[0:m] + p[m : 2 * m] + p[2 * m : 3 * m]


BELOW = [None, (18, 26, 34, 42, 50, 58), (10, 18, 26), (6, 14), (4,), (3,)]
ABOVE = [None, (-1, 7, 15), (-1, 7), (-1,), (-1,), (-1,)]


def reduce_rows(t, src, dst, starts):
    for ch in range(CH):
        for j in starts:

            def tap(o):
                return src[ch, t, pl.ds(8 + 2 * j + o, 8, stride=2), :]

            dst[ch, t, 8 + j : 16 + j, :] = (tap(-2) + tap(2)) + (tap(-1) + tap(1)) * 4.0 + tap(0) * 6.0


def mirror_start(a, first):
    for t in range(4):
        a[:, t, 7:8, :] = a[:, t, pl.ds(jnp.where(first, 9, 7), 1), :]
        a[:, t, 6:7, :] = a[:, t, pl.ds(jnp.where(first, 10, 6), 1), :]


def mirror_end(a, h, last):
    for t in range(4):
        a[:, t, 8 + h : 9 + h, :] = a[:, t, pl.ds(jnp.where(last, 6 + h, 8 + h), 1), :]


def rows_of(k, y, tiles):
    return jnp.concatenate(
        [jnp.concatenate([y[c, t, 7 : 7 + R[k], :] for t in tiles], axis=1) for c in range(CH)], axis=0
    )


def detail(g, level, at, out, count):
    lo, mid, hi = (g[:, :, i : i + count, :] for i in range(3))
    even, odd = pl.ds(at, count, stride=2), pl.ds(at + 1, count, stride=2)
    out[:, :, pl.ds(0, count, stride=2), :] = level[:, :, even, :] - ((lo + hi) * 0.125 + mid * 0.75)
    out[:, :, pl.ds(1, count, stride=2), :] = level[:, :, odd, :] - (mid + hi) * 0.5


def exchange_kernel(
    x_hbm, tlow_hbm, tmid_hbm, thigh_hbm, v1_hbm, s1_hbm, w2_hbm, w345_hbm, arrive_hbm,
    d0, d1, d2, d3, d4, d5,
    xs, y1, y2, y3, y4, y5, tv, v1, s1, w2, w345, arrive, srs, ci,
    rh, rl, kh, kl, cb, rh_in, rl_in, cbm, cbp, chm, chp, clm, clp,
    g1, g2, g3, g4, g5, m1, m2, m3, m4, m5, d3w, d4w,
    load_sem, send_sem, recv_sem,
):
    r, c = lax.axis_index("rows"), lax.axis_index("cols")
    nr, nc = lax.axis_size("rows"), lax.axis_size("cols")
    first, last = r == 0, r == nr - 1
    left, right = c == 0, c == nc - 1
    up, down = jnp.logical_not(first), jnp.logical_not(last)
    west, east = jnp.logical_not(left), jnp.logical_not(right)

    loads = [
        pltpu.make_async_copy(x_hbm.at[:, :, pl.ds(128 * t, 128)], xs.at[:, t, pl.ds(8, ROWS), :], load_sem.at[t])
        for t in range(4)
    ]
    loads += [
        pltpu.make_async_copy(tlow_hbm.at[left.astype(jnp.int32)], tv.at[pl.ds(0, 128)], load_sem.at[4]),
        pltpu.make_async_copy(tmid_hbm, tv.at[pl.ds(128, 256)], load_sem.at[5]),
        pltpu.make_async_copy(thigh_hbm.at[right.astype(jnp.int32)], tv.at[pl.ds(384, 128)], load_sem.at[6]),
        pltpu.make_async_copy(v1_hbm, v1, load_sem.at[7]),
        pltpu.make_async_copy(s1_hbm, s1, load_sem.at[8]),
        pltpu.make_async_copy(w2_hbm, w2, load_sem.at[9]),
        pltpu.make_async_copy(w345_hbm, w345, load_sem.at[10]),
        pltpu.make_async_copy(arrive_hbm, arrive, load_sem.at[11]),
    ]
    for copy in loads[:7]:
        copy.start()

    def there(dr, dc):
        ok = jnp.bool_(True)
        if dr:
            ok = jnp.logical_and(ok, up if dr < 0 else down)
        if dc:
            ok = jnp.logical_and(ok, west if dc < 0 else east)
        return ok

    messages = [
        (rh, rh_in, 1, 0),
        (kh, chm, 1, 1),
        (kh, chp, 1, -1),
        (rl, rl_in, -1, 0),
        (kl, clm, -1, 1),
        (kl, clp, -1, -1),
        (cb, cbm, 0, 1),
        (cb, cbp, 0, -1),
    ]
    barrier = pltpu.get_barrier_semaphore()
    for _, dst, dr, dc in messages:

        @pl.when(there(dr, dc))
        def _(dr=dr, dc=dc):
            pl.semaphore_signal(barrier, inc=1, device_id=(r + dr, c + dc), device_id_type=MESH)

        @pl.when(jnp.logical_not(there(-dr, -dc)))
        def _(dst=dst):
            dst[...] = jnp.zeros_like(dst)

    ys = (xs, y1, y2, y3, y4, y5)
    for k in range(LEVELS):
        ys[k][:, :, 0:8, :] = jnp.zeros((CH, 4, 8, 128), F32)
        ys[k][:, :, 8 + H[k] : 32 + H[k], :] = jnp.zeros((CH, 4, 24, 128), F32)
    srs[...] = jnp.zeros_like(srs)
    ci[...] = jnp.zeros_like(ci)
    for a in (rh, kh, kl):
        a[...] = jnp.zeros_like(a)

    for copy in loads[:4]:
        copy.wait()
    for k in range(1, LEVELS + 1):
        mirror_end(ys[k - 1], H[k - 1], last)
        for t in range(4):
            reduce_rows(t, ys[k - 1], ys[k], BELOW[k])
        for ch in range(CH):
            at = 16 * (k - 1) + 3 * ch
            srs[:, at : at + 3, :] = ys[k][ch, :, 7 + H[k] : 10 + H[k], :]
    for copy in loads[4:7]:
        copy.wait()
    lane = lax.broadcasted_iota(jnp.int32, (16, 128), 1)

    def form_strips(out, corners, count):
        strips = jnp.concatenate([srs[t] for t in range(4)], axis=1)
        near = dot3(strips[0:32], tv[:, 0:512])
        deep = dot3(strips[32:80], tv[:, 512:1024])
        deep = deep[:, 0:256] + deep[:, 256:512]
        cells = jnp.where(lane < 32, deep[16:32, 0:128], deep[32:48, 0:128])
        cells = jnp.where(lane < 24, deep[0:16, 0:128], cells)
        cells = jnp.where(lane < 8, near[0:16, 256:384], jnp.where(lane < 16, near[16:32, 256:384], cells))
        beside = jnp.where(lane < 118, deep[0:16, 0:128], jnp.where(lane < 120, deep[16:32, 0:128], deep[32:48, 0:128]))
        beside = jnp.where(lane < 114, near[0:16, 256:384], jnp.where(lane < 116, near[16:32, 256:384], beside))
        small = jnp.where(lane < 96, deep[16:32, 128:256], deep[32:48, 128:256])
        small = jnp.where(lane < 64, deep[0:16, 128:256], jnp.where(lane < 112, small, beside))
        for t, a in enumerate((near[0:16, 0:128], near[0:16, 128:256], near[16:32, 384:512], small)):
            out[pl.ds(t, CH * count, stride=4), :] = a[0 : CH * count]
        ci[...] = jnp.where(lane < 40, cells, 0.0)
        corners[0:3, :] = sum(pltpu.roll(ci[pl.ds(i, CH, stride=count), :], 40 * i, 1) for i in range(count))

    form_strips(rh, kh, 3)
    neighbours = (up.astype(jnp.int32) + down.astype(jnp.int32) + 1) * (
        west.astype(jnp.int32) + east.astype(jnp.int32) + 1
    ) - 1
    pl.semaphore_wait(barrier, neighbours)
    copies = []
    for m, (src, dst, dr, dc) in enumerate(messages):
        copies.append(
            pltpu.make_async_remote_copy(
                src_ref=src, dst_ref=dst, send_sem=send_sem.at[m], recv_sem=recv_sem.at[m],
                device_id=(r + dr, c + dc), device_id_type=MESH,
            )
        )
    for m in (1, 2, 0):
        pl.when(there(*messages[m][2:]))(copies[m].start)

    for copy in loads[7:]:
        copy.start()

    for k in range(1, LEVELS + 1):
        mirror_start(ys[k - 1], first)
        for t in range(4):
            reduce_rows(t, ys[k - 1], ys[k], ABOVE[k])
    mirror_start(y5, first)
    for k in range(1, LEVELS + 1):
        for ch in range(CH):
            at = 16 * (k - 1) + 2 * ch
            srs[:, at : at + 2, :] = ys[k][ch, :, 7:9, :]
    form_strips(rl, kl, 2)
    for m in (3, 4, 5):
        pl.when(there(*messages[m][2:]))(copies[m].start)

    outer = jnp.concatenate([rows_of(k, ys[k], (0, 3)) for k in range(1, LEVELS + 1)], axis=0)
    table = jnp.concatenate([tv[0:128], tv[384:512]], axis=0)
    turned = dot3(outer, jnp.concatenate([table[:, 256:384], table[:, 768:896]], axis=1))
    turned = jnp.concatenate([turned[:, 0:128] + turned[:, 128:256], jnp.zeros((32, 128), F32)], axis=0)
    turned = jnp.transpose(turned)
    place = lax.broadcasted_iota(jnp.int32, (8, 512), 1)

    def of_level(k, a):
        ok = place < (BASE[k + 1] if k < LEVELS else 480)
        return jnp.where(jnp.logical_and(ok, place >= BASE[k]), a, 0.0)

    cb[...] = sum(of_level(k, turned[8 * (k - 1) : 8 * k]) for k in range(1, LEVELS + 1))
    for m in (6, 7):
        pl.when(there(*messages[m][2:]))(copies[m].start)

    for copy in loads[7:]:
        copy.wait()
    p12 = dot3(jnp.concatenate([rows_of(k, ys[k], range(4)) for k in (1, 2)], axis=0), tv[:, 0:512])
    p345 = dot3(jnp.concatenate([rows_of(k, ys[k], range(4)) for k in (3, 4, 5)], axis=0), tv[:, 512:1024])
    p345 = p345[:, 0:256] + p345[:, 256:512]

    def put(k, a, out):
        for ch in range(CH):
            for t in range(out.shape[1]):
                out[ch, t] = a[R[k] * ch : R[k] * (ch + 1), 128 * t : 128 * (t + 1)]

    put(1, dot3(p12[0:224, 0:384], v1[...]), g1)
    put(1, p12, m1)
    both = dot3(p12[208:336, 256:512], w2[...])
    put(2, both[8:, 0:256], g2)
    put(2, both[8:, 256:384], m2)
    deeper = ((3, 0, g3, m3), (4, 72, g4, m4), (5, 112, g5, m5))
    for k, at, g, m in deeper:
        both = dot3(p345[at : at + 16 * -(-3 * R[k] // 16)], w345[k - 3])
        skip = BASE[k] - BASE[3] - at
        put(k, both[skip:, 0:128], g)
        put(k, both[skip:, 128:256], m)

    def add(k, a, out, tiles, first_tile=0):
        for ch in range(CH):
            for i, t in enumerate(tiles):
                lanes = 128 * (first_tile + i)
                out[ch, t] += a[R[k] * ch : R[k] * (ch + 1), lanes : lanes + 128]

    for m in (6, 7):
        pl.when(there(-messages[m][2], -messages[m][3]))(copies[m].wait_recv)
    sub = lax.broadcasted_iota(jnp.int32, (8, 512), 0)
    terms = [a.astype(F32) for a in split3(jnp.where(sub < 3, cbm[...], cbp[...]))]
    came = jnp.concatenate(
        [of_level(k, a) for k in range(1, LEVELS + 1) for a in terms] + [jnp.zeros((8, 512), F32)], axis=0
    )
    came = jnp.transpose(came)

    def arrived(k, at, rows, lanes, count):
        return jnp.dot(
            came[at : at + rows].astype(BF16), arrive[:, lanes : lanes + count], preferred_element_type=F32
        )[BASE[k] - at :]

    more = arrived(1, 0, 224, 0, 512)
    add(1, more, g1, (0, 3))
    add(1, more, m1, (0, 1), 2)
    more = arrived(2, 208, 128, 512, 384)
    add(2, more, g2, (0, 1))
    add(2, more, m2, (0,), 2)
    for k, at, g, m in deeper:
        more = arrived(k, BASE[3] + at, 16 * -(-3 * R[k] // 16), 896 + 256 * (k - 3), 256)
        add(k, more, g, (0,))
        add(k, more, m, (0,), 1)

    side = jnp.bitwise_and(lane, 7) < 3
    middle = jnp.logical_and(lane >= 64, lane < 104)
    ci[...] = jnp.zeros_like(ci)

    def add_rows(strip, minus, plus, count, row_of):
        corner = jnp.where(side[0:4], minus[...], plus[...])
        for i in range(count):
            ci[pl.ds(i, CH, stride=count), :] = pltpu.roll(corner, (64 - 40 * i) % 128, 1)[0:CH]
        rows = CH * count
        fill = jnp.zeros((16 - rows, 128), F32)
        tiles = [jnp.concatenate([strip[pl.ds(t, rows, stride=4), :], fill], axis=0) for t in range(4)]
        cells = jnp.where(lane < 112, jnp.where(middle, ci[...], 0.0), tiles[3])
        wide = dot3(jnp.concatenate([tiles[0], tiles[1], cells], axis=1), v1[...])
        level = jnp.concatenate(tiles[0:2], axis=1) + dot3(cells, s1[...])
        both = [dot3(jnp.concatenate([cells, tiles[2]], axis=1), w2[...])]
        tail = jnp.concatenate([cells, tiles[3]], axis=1)
        both += [dot3(tail, w345[k - 3]) for k in (3, 4, 5)]
        pairs = [(1, wide, g1), (1, level, m1), (2, both[0][:, 0:256], g2), (2, both[0][:, 256:384], m2)]
        for (k, _, g, m), a in zip(deeper, both[1:]):
            pairs += [(k, a[:, 0:128], g), (k, a[:, 128:256], m)]
        for k, a, out in pairs:
            at = row_of(k) + 1
            for ch in range(CH):
                for t in range(out.shape[1]):
                    out[ch, t, at : at + count, :] += a[count * ch : count * (ch + 1), 128 * t : 128 * (t + 1)]

    def details(counts):
        for g, level, at, out, count in zip((g1, g2, g3, g4, g5), (xs, m1, m2, m3, m4), (8, 1, 1, 1, 1), (d0, d1, d2, d3w, d4w), counts):
            detail(g, level, at, out, count)
        d3[...] = d3w[:, 0, :, 0:64]
        d4[...] = d4w[:, 0, :, 0:32]
        d5[...] = m5[:, 0, 1:5, 0:16]

    for m in (3, 4, 5):
        pl.when(there(-messages[m][2], -messages[m][3]))(copies[m].wait_recv)
    add_rows(rl_in, clm, clp, 2, lambda k: H[k] - 1)
    for k, g in enumerate((g1, g2, g3, g4, g5), 1):
        g[:, :, H[k] + 1 : H[k] + 2, :] = g[:, :, pl.ds(jnp.where(last, H[k], H[k] + 1), 1), :]
    details(H[1:6])
    for m in range(3):
        pl.when(there(-messages[m][2], -messages[m][3]))(copies[m].wait_recv)
    add_rows(rh_in, chm, chp, 3, lambda k: -1)
    details((4,) * 5)
    for copy, (_, _, dr, dc) in zip(copies, messages):
        pl.when(there(dr, dc))(copy.wait_send)


def result_kernel(d0, d1, d2, d3, d4, d5, o0, o1, o2, o3, o4, o5, sem):
    pairs = [(d0.at[:, t], o0.at[:, :, pl.ds(128 * t, 128)]) for t in range(4)]
    pairs += [(d1.at[:, t], o1.at[:, :, pl.ds(128 * t, 128)]) for t in range(2)]
    pairs += [(d2.at[:, 0], o2), (d3, o3), (d4, o4), (d5, o5)]
    copies = [pltpu.make_async_copy(src, dst, sem.at[i]) for i, (src, dst) in enumerate(pairs)]
    for copy in copies:
        copy.start()
    for copy in copies:
        copy.wait()


def body(orthophoto):
    def vmem(*shape, dtype=F32):
        return pltpu.VMEM(shape, dtype)

    held = [(CH, 4, H[0], 128), (CH, 2, H[1], 128), (CH, 1, H[2], 128)]
    held += [(CH, H[3], W[3]), (CH, H[4], W[4]), (CH, H[5], W[5])]
    scratch = [vmem(CH, 4, H[k] + 32, 128) for k in range(6)]
    scratch += [vmem(512, 1024, dtype=BF16), vmem(384, 512, dtype=BF16), vmem(128, 256, dtype=BF16)]
    scratch += [vmem(256, 384, dtype=BF16), vmem(3, 256, 256, dtype=BF16), vmem(128, 1664, dtype=BF16)]
    scratch += [vmem(4, 80, 128), vmem(16, 128)]
    scratch += [vmem(40, 128), vmem(24, 128), vmem(4, 128), vmem(4, 128), vmem(8, 512)]
    scratch += [vmem(40, 128), vmem(24, 128), vmem(8, 512), vmem(8, 512)]
    scratch += [vmem(4, 128)] * 4
    scratch += [vmem(CH, t, R[k], 128) for k, t in ((1, 4), (2, 2), (3, 1), (4, 1), (5, 1))]
    scratch += [vmem(CH, t, R[k], 128) for k, t in ((1, 2), (2, 1), (3, 1), (4, 1), (5, 1))]
    scratch += [vmem(CH, 1, H[3], 128), vmem(CH, 1, H[4], 128)]
    scratch += [pltpu.SemaphoreType.DMA((n,)) for n in (12, 8, 8)]
    far = pl.BlockSpec(memory_space=pltpu.HBM)
    inside = pl.BlockSpec(memory_space=pltpu.VMEM)
    inputs = [pltpu.with_memory_space_constraint(jnp.asarray(a), pltpu.HBM) for a in (orthophoto, *tables())]
    arrays = pl.pallas_call(
        exchange_kernel,
        out_shape=[jax.ShapeDtypeStruct(shape, F32) for shape in held],
        in_specs=[far] * len(inputs),
        out_specs=[inside] * len(held),
        scratch_shapes=scratch,
        compiler_params=pltpu.CompilerParams(collective_id=0, has_side_effects=True, vmem_limit_bytes=24 << 20),
    )(*inputs)
    results = pl.pallas_call(
        result_kernel,
        out_shape=[jax.ShapeDtypeStruct((CH, H[k], W[k]), F32) for k in range(6)],
        in_specs=[inside] * len(held),
        out_specs=[far] * 6,
        scratch_shapes=[pltpu.SemaphoreType.DMA((10,))],
        compiler_params=pltpu.CompilerParams(vmem_limit_bytes=8 << 20),
    )(*arrays)
    return tuple(results)


def solution(mesh):
    placed = P(None, "rows", "cols")
    return jax.shard_map(body, mesh=mesh, in_specs=(placed,), out_specs=(placed,) * 6, check_vma=False)
```

```python
import functools

import jax
import jax.numpy as jnp
import numpy as np
from jax import lax
from jax.experimental import pallas as pl
from jax.experimental.pallas import tpu as pltpu
from jax.sharding import PartitionSpec as P

CH = 3
ROWS = 128
COLS = 512
LEVELS = 5
H = [ROWS >> k for k in range(6)]
W = [COLS >> k for k in range(6)]
R = [0, 72, 40, 24, 16, 8]
BASE = [0, 0, 216, 336, 408, 456]
POS = [0, 0, 0, 0, 64, 96]
F32 = jnp.float32
BF16 = jnp.bfloat16
MESH = pl.DeviceIdType.MESH
TAPS = (1.0, 4.0, 6.0, 4.0, 1.0)


def column_reductions(low, high):
    result = [None]
    total = None
    for k in range(1, LEVELS + 1):
        n = W[k - 1]
        step = np.zeros((n + 3, W[k] + 3))
        for j in range(0 if low else -1, W[k] if high else W[k] + 2):
            for tap in range(5):
                cell = 2 * j - 2 + tap
                if low and cell < 0:
                    cell = -cell
                if high and cell > n - 1:
                    cell = 2 * (n - 1) - cell
                if -1 <= cell <= n + 1:
                    step[cell + 1, j + 1] += TAPS[tap] / 16
        total = step[1 : n + 1] if k == 1 else total @ step
        result.append(total / 16.0**k)
    return result


def reduction_table(low, high):
    t = column_reductions(low, high)

    def fill(a, at, k):
        beyond, before = W[k] - 1 if high else W[k], 1 if low else -1
        cells = (W[k] - 1, beyond, W[k] + 1, before, 0)
        a[:, at + 8 * (k - 1) : at + 8 * (k - 1) + 5] = t[k][:, [c + 1 for c in cells]]
        a[:, at + 112 + 2 * (k - 1) : at + 114 + 2 * (k - 1)] = t[k][:, [beyond + 1, before + 1]]

    first = np.zeros((COLS, 512))
    first[:, 0:256] = t[1][:, 1:257]
    first[:, 384:512] = t[2][:, 1:129]
    last = np.zeros((COLS, 256))
    for k in (3, 4, 5):
        fill(last, 0, k)
        last[:, 128 + POS[k] : 128 + POS[k] + W[k]] = t[k][:, 1 : W[k] + 1]
    for k in (1, 2):
        fill(first, 256, k)
    top = np.asarray(last.astype(jnp.bfloat16), np.float64)
    rest = np.asarray((last - top).astype(jnp.bfloat16), np.float64)
    assert np.array_equal(top + rest, last)
    first[:, 272:296] = top[:, 16:40]
    assert np.array_equal(np.asarray(first.astype(jnp.bfloat16), np.float64), first)
    return np.concatenate([first, top, rest], axis=1)


def expansion_row(k, cell):
    row = np.zeros(2 * W[k])
    for i in range(W[k]):
        row[2 * i] += {i - 1: 0.125, i: 0.75, i + 1: 0.125}.get(cell, 0.0)
        row[2 * i + 1] += {i: 0.5, i + 1: 0.5}.get(cell, 0.0)
    return row


def expansion_table(k, main_at, edge_at, lanes):
    spread = np.zeros((lanes, 2 * W[k]))
    keep = np.zeros((lanes, W[k]))
    for c in range(W[k]):
        spread[main_at + c] = expansion_row(k, c)
        keep[main_at + c, c] = 1
    own = edge_at + 112 + 2 * (k - 1)
    came = edge_at + 64 + 8 * (k - 1)
    spread[own] = expansion_row(k, W[k])
    spread[own + 1] = expansion_row(k, -1)
    for s, cell in enumerate((-1, 0, 1, W[k] - 1, W[k])):
        spread[came + s] = expansion_row(k, cell)
        if 0 <= cell < W[k]:
            keep[came + s, cell] = 1
    return spread, keep


def arrival_table(k):
    spread = np.zeros((128, 2 * W[k]))
    keep = np.zeros((128, W[k]))
    for part in range(3):
        for s, cell in enumerate((-1, 0, 1, W[k] - 1, W[k])):
            lane = 24 * (k - 1) + 8 * part + s
            spread[lane] = expansion_row(k, cell)
            if 0 <= cell < W[k]:
                keep[lane, cell] = 1
    return spread, keep


def padded(a, cols):
    return np.pad(a, ((0, 0), (0, cols - a.shape[1])))


def tables():
    plain, low, high = (reduction_table(*e) for e in ((False, False), (True, False), (False, True)))
    assert np.array_equal(plain[128:], low[128:]) and np.array_equal(plain[:384], high[:384])
    t_low = np.stack([plain[:128], low[:128]])
    t_high = np.stack([plain[384:], high[384:]])
    v1, s1 = expansion_table(1, 0, 256, 384)
    w2 = np.concatenate(expansion_table(2, 128, 0, 256), axis=1)
    deep = []
    for k in (3, 4, 5):
        spread, keep = expansion_table(k, 128 + POS[k], 0, 256)
        deep.append(np.concatenate([padded(spread, 128), padded(keep, 128)], axis=1))
    spread, keep = arrival_table(1)
    assert not spread[:, 128:384].any()
    arrive = [spread[:, :128], spread[:, 384:], keep]
    arrive += arrival_table(2)
    for k in (3, 4, 5):
        arrive += [padded(a, 128) for a in arrival_table(k)]
    parts = (t_low, plain[128:384], t_high, v1, s1[256:], w2, np.stack(deep), np.concatenate(arrive, axis=1))
    return [a.astype(jnp.bfloat16) for a in parts]


def split3(a):
    top = a.astype(BF16)
    rest = a - top.astype(F32)
    mid = rest.astype(BF16)
    return top, mid, (rest - mid.astype(F32)).astype(BF16)


def dot3(a, table):
    m = a.shape[0]
    p = jnp.dot(jnp.concatenate(split3(a), axis=0), table, preferred_element_type=F32)
    return p[0:m] + p[m : 2 * m] + p[2 * m : 3 * m]


BELOW = [None, (18, 26, 34, 42, 50, 58), (10, 18, 26), (6, 14), (4,), (3,)]
ABOVE = [None, (-1, 7, 15), (-1, 7), (-1,), (-1,), (-1,)]


def reduce_rows(t, src, dst, starts):
    for ch in range(CH):
        for j in starts:

            def tap(o):
                return src[ch, t, pl.ds(8 + 2 * j + o, 8, stride=2), :]

            dst[ch, t, 8 + j : 16 + j, :] = (tap(-2) + tap(2)) + (tap(-1) + tap(1)) * 4.0 + tap(0) * 6.0


def mirror_start(a, first):
    for t in range(4):
        a[:, t, 7:8, :] = a[:, t, pl.ds(jnp.where(first, 9, 7), 1), :]
        a[:, t, 6:7, :] = a[:, t, pl.ds(jnp.where(first, 10, 6), 1), :]


def mirror_end(a, h, last):
    for t in range(4):
        a[:, t, 8 + h : 9 + h, :] = a[:, t, pl.ds(jnp.where(last, 6 + h, 8 + h), 1), :]


def rows_of(k, y, tiles):
    return jnp.concatenate(
        [jnp.concatenate([y[c, t, 7 : 7 + R[k], :] for t in tiles], axis=1) for c in range(CH)], axis=0
    )


def detail(g, level, at, out, count):
    lo, mid, hi = (g[:, :, i : i + count, :] for i in range(3))
    even, odd = pl.ds(at, count, stride=2), pl.ds(at + 1, count, stride=2)
    out[:, :, pl.ds(0, count, stride=2), :] = level[:, :, even, :] - ((lo + hi) * 0.125 + mid * 0.75)
    out[:, :, pl.ds(1, count, stride=2), :] = level[:, :, odd, :] - (mid + hi) * 0.5


def exchange_kernel(
    x_hbm, tlow_hbm, tmid_hbm, thigh_hbm, v1_hbm, s1_hbm, w2_hbm, w345_hbm, arrive_hbm,
    d0, d1, d2, d3, d4, d5,
    xs, y1, y2, y3, y4, y5, tv, v1, s1, w2, w345, arrive, srs, ci,
    rh, rl, kh, kl, cb, rh_in, rl_in, cbm, cbp, chm, chp, clm, clp,
    g1, g2, g3, g4, g5, m1, m2, m3, m4, m5, d3w, d4w,
    load_sem, send_sem, recv_sem,
):
    r, c = lax.axis_index("rows"), lax.axis_index("cols")
    nr, nc = lax.axis_size("rows"), lax.axis_size("cols")
    first, last = r == 0, r == nr - 1
    left, right = c == 0, c == nc - 1
    up, down = jnp.logical_not(first), jnp.logical_not(last)
    west, east = jnp.logical_not(left), jnp.logical_not(right)

    loads = [
        pltpu.make_async_copy(x_hbm.at[:, :, pl.ds(128 * t, 128)], xs.at[:, t, pl.ds(8, ROWS), :], load_sem.at[t])
        for t in range(4)
    ]
    loads += [
        pltpu.make_async_copy(tlow_hbm.at[left.astype(jnp.int32)], tv.at[pl.ds(0, 128)], load_sem.at[4]),
        pltpu.make_async_copy(tmid_hbm, tv.at[pl.ds(128, 256)], load_sem.at[5]),
        pltpu.make_async_copy(thigh_hbm.at[right.astype(jnp.int32)], tv.at[pl.ds(384, 128)], load_sem.at[6]),
        pltpu.make_async_copy(v1_hbm, v1, load_sem.at[7]),
        pltpu.make_async_copy(s1_hbm, s1, load_sem.at[8]),
        pltpu.make_async_copy(w2_hbm, w2, load_sem.at[9]),
        pltpu.make_async_copy(w345_hbm, w345, load_sem.at[10]),
        pltpu.make_async_copy(arrive_hbm, arrive, load_sem.at[11]),
    ]
    for copy in loads[:7]:
        copy.start()

    def there(dr, dc):
        ok = jnp.bool_(True)
        if dr:
            ok = jnp.logical_and(ok, up if dr < 0 else down)
        if dc:
            ok = jnp.logical_and(ok, west if dc < 0 else east)
        return ok

    messages = [
        (rh, rh_in, 1, 0),
        (kh, chm, 1, 1),
        (kh, chp, 1, -1),
        (rl, rl_in, -1, 0),
        (kl, clm, -1, 1),
        (kl, clp, -1, -1),
        (cb, cbm, 0, 1),
        (cb, cbp, 0, -1),
    ]
    barrier = pltpu.get_barrier_semaphore()
    for _, dst, dr, dc in messages:

        @pl.when(there(dr, dc))
        def _(dr=dr, dc=dc):
            pl.semaphore_signal(barrier, inc=1, device_id=(r + dr, c + dc), device_id_type=MESH)

        @pl.when(jnp.logical_not(there(-dr, -dc)))
        def _(dst=dst):
            dst[...] = jnp.zeros_like(dst)

    ys = (xs, y1, y2, y3, y4, y5)
    for k in range(LEVELS):
        ys[k][:, :, 0:8, :] = jnp.zeros((CH, 4, 8, 128), F32)
        ys[k][:, :, 8 + H[k] : 32 + H[k], :] = jnp.zeros((CH, 4, 24, 128), F32)
    srs[...] = jnp.zeros_like(srs)
    ci[...] = jnp.zeros_like(ci)
    for a in (rh, kh, kl):
        a[...] = jnp.zeros_like(a)

    for copy in loads[:4]:
        copy.wait()
    for k in range(1, LEVELS + 1):
        mirror_end(ys[k - 1], H[k - 1], last)
        for t in range(4):
            reduce_rows(t, ys[k - 1], ys[k], BELOW[k])
        for ch in range(CH):
            at = 16 * (k - 1) + 3 * ch
            srs[:, at : at + 3, :] = ys[k][ch, :, 7 + H[k] : 10 + H[k], :]
    for copy in loads[4:7]:
        copy.wait()
    lane = lax.broadcasted_iota(jnp.int32, (16, 128), 1)

    def form_strips(out, corners, count):
        strips = jnp.concatenate([srs[t] for t in range(4)], axis=1)
        near = dot3(strips[0:32], tv[:, 0:512])
        deep = dot3(strips[32:80], tv[:, 512:1024])
        deep = deep[:, 0:256] + deep[:, 256:512]
        cells = jnp.where(lane < 32, deep[16:32, 0:128], deep[32:48, 0:128])
        cells = jnp.where(lane < 24, deep[0:16, 0:128], cells)
        cells = jnp.where(lane < 8, near[0:16, 256:384], jnp.where(lane < 16, near[16:32, 256:384], cells))
        beside = jnp.where(lane < 118, deep[0:16, 0:128], jnp.where(lane < 120, deep[16:32, 0:128], deep[32:48, 0:128]))
        beside = jnp.where(lane < 114, near[0:16, 256:384], jnp.where(lane < 116, near[16:32, 256:384], beside))
        small = jnp.where(lane < 96, deep[16:32, 128:256], deep[32:48, 128:256])
        small = jnp.where(lane < 64, deep[0:16, 128:256], jnp.where(lane < 112, small, beside))
        for t, a in enumerate((near[0:16, 0:128], near[0:16, 128:256], near[16:32, 384:512], small)):
            out[pl.ds(t, CH * count, stride=4), :] = a[0 : CH * count]
        ci[...] = jnp.where(lane < 40, cells, 0.0)
        corners[0:3, :] = sum(pltpu.roll(ci[pl.ds(i, CH, stride=count), :], 40 * i, 1) for i in range(count))

    form_strips(rh, kh, 3)
    place = lax.broadcasted_iota(jnp.int32, (8, 512), 1)

    def of_level(k, a):
        ok = place < (BASE[k + 1] if k < LEVELS else 480)
        return jnp.where(jnp.logical_and(ok, place >= BASE[k]), a, 0.0)

    def put(k, a, out):
        for ch in range(CH):
            for t in range(out.shape[1]):
                out[ch, t] = a[R[k] * ch : R[k] * (ch + 1), 128 * t : 128 * (t + 1)]

    deeper = ((3, 0, g3, m3), (4, 72, g4, m4), (5, 112, g5, m5))

    def reduce_rest():
        for k in range(1, LEVELS + 1):
            mirror_start(ys[k - 1], first)
            for t in range(4):
                reduce_rows(t, ys[k - 1], ys[k], ABOVE[k])
        mirror_start(y5, first)
        for k in range(1, LEVELS + 1):
            for ch in range(CH):
                at = 16 * (k - 1) + 2 * ch
                srs[:, at : at + 2, :] = ys[k][ch, :, 7:9, :]
        form_strips(rl, kl, 2)
        outer = jnp.concatenate([rows_of(k, ys[k], (0, 3)) for k in range(1, LEVELS + 1)], axis=0)
        table = jnp.concatenate([tv[0:128], tv[384:512]], axis=0)
        turned = dot3(outer, jnp.concatenate([table[:, 256:384], table[:, 768:896]], axis=1))
        turned = jnp.concatenate([turned[:, 0:128] + turned[:, 128:256], jnp.zeros((32, 128), F32)], axis=0)
        turned = jnp.transpose(turned)
        cb[...] = sum(of_level(k, turned[8 * (k - 1) : 8 * k]) for k in range(1, LEVELS + 1))

    def expand_own():
        for copy in loads[7:]:
            copy.start()
        p12 = dot3(jnp.concatenate([rows_of(k, ys[k], range(4)) for k in (1, 2)], axis=0), tv[:, 0:512])
        p345 = dot3(jnp.concatenate([rows_of(k, ys[k], range(4)) for k in (3, 4, 5)], axis=0), tv[:, 512:1024])
        p345 = p345[:, 0:256] + p345[:, 256:512]

        for copy in loads[7:]:
            copy.wait()
        put(1, dot3(p12[0:224, 0:384], v1[...]), g1)
        put(1, p12, m1)
        both = dot3(p12[208:336, 256:512], w2[...])
        put(2, both[8:, 0:256], g2)
        put(2, both[8:, 256:384], m2)
        for k, at, g, m in deeper:
            both = dot3(p345[at : at + 16 * -(-3 * R[k] // 16)], w345[k - 3])
            skip = BASE[k] - BASE[3] - at
            put(k, both[skip:, 0:128], g)
            put(k, both[skip:, 128:256], m)

    early = lax.rem(r, 8) == 0

    @pl.when(early)
    def _():
        reduce_rest()
        expand_own()

    neighbours = (up.astype(jnp.int32) + down.astype(jnp.int32) + 1) * (
        west.astype(jnp.int32) + east.astype(jnp.int32) + 1
    ) - 1
    pl.semaphore_wait(barrier, neighbours)
    copies = []
    for m, (src, dst, dr, dc) in enumerate(messages):
        copies.append(
            pltpu.make_async_remote_copy(
                src_ref=src, dst_ref=dst, send_sem=send_sem.at[m], recv_sem=recv_sem.at[m],
                device_id=(r + dr, c + dc), device_id_type=MESH,
            )
        )
    for m in (1, 2, 0):
        pl.when(there(*messages[m][2:]))(copies[m].start)


    @pl.when(jnp.logical_not(early))
    def _():
        reduce_rest()

    for m in range(3, 8):
        pl.when(there(*messages[m][2:]))(copies[m].start)
    pl.when(jnp.logical_not(early))(expand_own)

    def add(k, a, out, tiles, first_tile=0):
        for ch in range(CH):
            for i, t in enumerate(tiles):
                lanes = 128 * (first_tile + i)
                out[ch, t] += a[R[k] * ch : R[k] * (ch + 1), lanes : lanes + 128]

    side = jnp.bitwise_and(lane, 7) < 3
    middle = jnp.logical_and(lane >= 64, lane < 104)
    ci[...] = jnp.zeros_like(ci)

    def add_rows(strip, minus, plus, count, row_of):
        corner = jnp.where(side[0:4], minus[...], plus[...])
        for i in range(count):
            ci[pl.ds(i, CH, stride=count), :] = pltpu.roll(corner, (64 - 40 * i) % 128, 1)[0:CH]
        rows = CH * count
        fill = jnp.zeros((16 - rows, 128), F32)
        tiles = [jnp.concatenate([strip[pl.ds(t, rows, stride=4), :], fill], axis=0) for t in range(4)]
        cells = jnp.where(lane < 112, jnp.where(middle, ci[...], 0.0), tiles[3])
        wide = dot3(jnp.concatenate([tiles[0], tiles[1], cells], axis=1), v1[...])
        level = jnp.concatenate(tiles[0:2], axis=1) + dot3(cells, s1[...])
        both = [dot3(jnp.concatenate([cells, tiles[2]], axis=1), w2[...])]
        tail = jnp.concatenate([cells, tiles[3]], axis=1)
        both += [dot3(tail, w345[k - 3]) for k in (3, 4, 5)]
        pairs = [(1, wide, g1), (1, level, m1), (2, both[0][:, 0:256], g2), (2, both[0][:, 256:384], m2)]
        for (k, _, g, m), a in zip(deeper, both[1:]):
            pairs += [(k, a[:, 0:128], g), (k, a[:, 128:256], m)]
        for k, a, out in pairs:
            at = row_of(k) + 1
            for ch in range(CH):
                for t in range(out.shape[1]):
                    out[ch, t, at : at + count, :] += a[count * ch : count * (ch + 1), 128 * t : 128 * (t + 1)]

    def details(counts):
        for g, level, at, out, count in zip((g1, g2, g3, g4, g5), (xs, m1, m2, m3, m4), (8, 1, 1, 1, 1), (d0, d1, d2, d3w, d4w), counts):
            detail(g, level, at, out, count)
        d3[...] = d3w[:, 0, :, 0:64]
        d4[...] = d4w[:, 0, :, 0:32]
        d5[...] = m5[:, 0, 1:5, 0:16]

    for m in (3, 4, 5):
        pl.when(there(-messages[m][2], -messages[m][3]))(copies[m].wait_recv)
    add_rows(rl_in, clm, clp, 2, lambda k: H[k] - 1)
    for m in (6, 7):
        pl.when(there(-messages[m][2], -messages[m][3]))(copies[m].wait_recv)
    sub = lax.broadcasted_iota(jnp.int32, (8, 512), 0)
    terms = [a.astype(F32) for a in split3(jnp.where(sub < 3, cbm[...], cbp[...]))]
    came = jnp.concatenate(
        [of_level(k, a) for k in range(1, LEVELS + 1) for a in terms] + [jnp.zeros((8, 512), F32)], axis=0
    )
    came = jnp.transpose(came)

    def arrived(k, at, rows, lanes, count):
        return jnp.dot(
            came[at : at + rows].astype(BF16), arrive[:, lanes : lanes + count], preferred_element_type=F32
        )[BASE[k] - at :]

    more = arrived(1, 0, 224, 0, 512)
    add(1, more, g1, (0, 3))
    add(1, more, m1, (0, 1), 2)
    more = arrived(2, 208, 128, 512, 384)
    add(2, more, g2, (0, 1))
    add(2, more, m2, (0,), 2)
    for k, at, g, m in deeper:
        more = arrived(k, BASE[3] + at, 16 * -(-3 * R[k] // 16), 896 + 256 * (k - 3), 256)
        add(k, more, g, (0,))
        add(k, more, m, (0,), 1)

    for k, g in enumerate((g1, g2, g3, g4, g5), 1):
        g[:, :, H[k] + 1 : H[k] + 2, :] = g[:, :, pl.ds(jnp.where(last, H[k], H[k] + 1), 1), :]
    details(H[1:6])
    for m in range(3):
        pl.when(there(-messages[m][2], -messages[m][3]))(copies[m].wait_recv)
    add_rows(rh_in, chm, chp, 3, lambda k: -1)
    details((4,) * 5)
    for copy, (_, _, dr, dc) in zip(copies, messages):
        pl.when(there(dr, dc))(copy.wait_send)


def result_kernel(d0, d1, d2, d3, d4, d5, o0, o1, o2, o3, o4, o5, sem):
    pairs = [(d0.at[:, t], o0.at[:, :, pl.ds(128 * t, 128)]) for t in range(4)]
    pairs += [(d1.at[:, t], o1.at[:, :, pl.ds(128 * t, 128)]) for t in range(2)]
    pairs += [(d2.at[:, 0], o2), (d3, o3), (d4, o4), (d5, o5)]
    copies = [pltpu.make_async_copy(src, dst, sem.at[i]) for i, (src, dst) in enumerate(pairs)]
    for copy in copies:
        copy.start()
    for copy in copies:
        copy.wait()


def body(orthophoto):
    def vmem(*shape, dtype=F32):
        return pltpu.VMEM(shape, dtype)

    held = [(CH, 4, H[0], 128), (CH, 2, H[1], 128), (CH, 1, H[2], 128)]
    held += [(CH, H[3], W[3]), (CH, H[4], W[4]), (CH, H[5], W[5])]
    scratch = [vmem(CH, 4, H[k] + 32, 128) for k in range(6)]
    scratch += [vmem(512, 1024, dtype=BF16), vmem(384, 512, dtype=BF16), vmem(128, 256, dtype=BF16)]
    scratch += [vmem(256, 384, dtype=BF16), vmem(3, 256, 256, dtype=BF16), vmem(128, 1664, dtype=BF16)]
    scratch += [vmem(4, 80, 128), vmem(16, 128)]
    scratch += [vmem(40, 128), vmem(24, 128), vmem(4, 128), vmem(4, 128), vmem(8, 512)]
    scratch += [vmem(40, 128), vmem(24, 128), vmem(8, 512), vmem(8, 512)]
    scratch += [vmem(4, 128)] * 4
    scratch += [vmem(CH, t, R[k], 128) for k, t in ((1, 4), (2, 2), (3, 1), (4, 1), (5, 1))]
    scratch += [vmem(CH, t, R[k], 128) for k, t in ((1, 2), (2, 1), (3, 1), (4, 1), (5, 1))]
    scratch += [vmem(CH, 1, H[3], 128), vmem(CH, 1, H[4], 128)]
    scratch += [pltpu.SemaphoreType.DMA((n,)) for n in (12, 8, 8)]
    far = pl.BlockSpec(memory_space=pltpu.HBM)
    inside = pl.BlockSpec(memory_space=pltpu.VMEM)
    inputs = [pltpu.with_memory_space_constraint(jnp.asarray(a), pltpu.HBM) for a in (orthophoto, *tables())]
    arrays = pl.pallas_call(
        exchange_kernel,
        out_shape=[jax.ShapeDtypeStruct(shape, F32) for shape in held],
        in_specs=[far] * len(inputs),
        out_specs=[inside] * len(held),
        scratch_shapes=scratch,
        compiler_params=pltpu.CompilerParams(collective_id=0, has_side_effects=True, vmem_limit_bytes=24 << 20),
    )(*inputs)
    results = pl.pallas_call(
        result_kernel,
        out_shape=[jax.ShapeDtypeStruct((CH, H[k], W[k]), F32) for k in range(6)],
        in_specs=[inside] * len(held),
        out_specs=[far] * 6,
        scratch_shapes=[pltpu.SemaphoreType.DMA((10,))],
        compiler_params=pltpu.CompilerParams(vmem_limit_bytes=8 << 20),
    )(*arrays)
    return tuple(results)


def solution(mesh):
    placed = P(None, "rows", "cols")
    return jax.shard_map(body, mesh=mesh, in_specs=(placed,), out_specs=(placed,) * 6, check_vma=False)
```

```python
import functools

import jax
import jax.numpy as jnp
import numpy as np
from jax import lax
from jax.experimental import pallas as pl
from jax.experimental.pallas import tpu as pltpu
from jax.sharding import PartitionSpec as P

CH = 3
ROWS = 128
COLS = 512
LEVELS = 5
H = [ROWS >> k for k in range(6)]
W = [COLS >> k for k in range(6)]
R = [0, 72, 40, 24, 16, 8]
BASE = [0, 0, 216, 336, 408, 456]
POS = [0, 0, 0, 0, 64, 96]
F32 = jnp.float32
BF16 = jnp.bfloat16
MESH = pl.DeviceIdType.MESH
TAPS = (1.0, 4.0, 6.0, 4.0, 1.0)


def column_reductions(low, high):
    result = [None]
    total = None
    for k in range(1, LEVELS + 1):
        n = W[k - 1]
        step = np.zeros((n + 3, W[k] + 3))
        for j in range(0 if low else -1, W[k] if high else W[k] + 2):
            for tap in range(5):
                cell = 2 * j - 2 + tap
                if low and cell < 0:
                    cell = -cell
                if high and cell > n - 1:
                    cell = 2 * (n - 1) - cell
                if -1 <= cell <= n + 1:
                    step[cell + 1, j + 1] += TAPS[tap] / 16
        total = step[1 : n + 1] if k == 1 else total @ step
        result.append(total / 16.0**k)
    return result


def reduction_table(low, high):
    t = column_reductions(low, high)

    def fill(a, at, k):
        beyond, before = W[k] - 1 if high else W[k], 1 if low else -1
        cells = (W[k] - 1, beyond, W[k] + 1, before, 0)
        a[:, at + 8 * (k - 1) : at + 8 * (k - 1) + 5] = t[k][:, [c + 1 for c in cells]]
        a[:, at + 112 + 2 * (k - 1) : at + 114 + 2 * (k - 1)] = t[k][:, [beyond + 1, before + 1]]

    first = np.zeros((COLS, 512))
    first[:, 0:256] = t[1][:, 1:257]
    first[:, 384:512] = t[2][:, 1:129]
    last = np.zeros((COLS, 256))
    for k in (3, 4, 5):
        fill(last, 0, k)
        last[:, 128 + POS[k] : 128 + POS[k] + W[k]] = t[k][:, 1 : W[k] + 1]
    for k in (1, 2):
        fill(first, 256, k)
    top = np.asarray(last.astype(jnp.bfloat16), np.float64)
    rest = np.asarray((last - top).astype(jnp.bfloat16), np.float64)
    assert np.array_equal(top + rest, last)
    first[:, 272:296] = top[:, 16:40]
    assert np.array_equal(np.asarray(first.astype(jnp.bfloat16), np.float64), first)
    return np.concatenate([first, top, rest], axis=1)


def expansion_row(k, cell):
    row = np.zeros(2 * W[k])
    for i in range(W[k]):
        row[2 * i] += {i - 1: 0.125, i: 0.75, i + 1: 0.125}.get(cell, 0.0)
        row[2 * i + 1] += {i: 0.5, i + 1: 0.5}.get(cell, 0.0)
    return row


def expansion_table(k, main_at, edge_at, lanes):
    spread = np.zeros((lanes, 2 * W[k]))
    keep = np.zeros((lanes, W[k]))
    for c in range(W[k]):
        spread[main_at + c] = expansion_row(k, c)
        keep[main_at + c, c] = 1
    own = edge_at + 112 + 2 * (k - 1)
    came = edge_at + 64 + 8 * (k - 1)
    spread[own] = expansion_row(k, W[k])
    spread[own + 1] = expansion_row(k, -1)
    for s, cell in enumerate((-1, 0, 1, W[k] - 1, W[k])):
        spread[came + s] = expansion_row(k, cell)
        if 0 <= cell < W[k]:
            keep[came + s, cell] = 1
    return spread, keep


def arrival_table(k):
    spread = np.zeros((128, 2 * W[k]))
    keep = np.zeros((128, W[k]))
    for part in range(3):
        for s, cell in enumerate((-1, 0, 1, W[k] - 1, W[k])):
            lane = 24 * (k - 1) + 8 * part + s
            spread[lane] = expansion_row(k, cell)
            if 0 <= cell < W[k]:
                keep[lane, cell] = 1
    return spread, keep


def padded(a, cols):
    return np.pad(a, ((0, 0), (0, cols - a.shape[1])))


def tables():
    plain, low, high = (reduction_table(*e) for e in ((False, False), (True, False), (False, True)))
    assert np.array_equal(plain[128:], low[128:]) and np.array_equal(plain[:384], high[:384])
    t_low = np.stack([plain[:128], low[:128]])
    t_high = np.stack([plain[384:], high[384:]])
    v1, s1 = expansion_table(1, 0, 256, 384)
    w2 = np.concatenate(expansion_table(2, 128, 0, 256), axis=1)
    deep = []
    for k in (3, 4, 5):
        spread, keep = expansion_table(k, 128 + POS[k], 0, 256)
        deep.append(np.concatenate([padded(spread, 128), padded(keep, 128)], axis=1))
    spread, keep = arrival_table(1)
    assert not spread[:, 128:384].any()
    arrive = [spread[:, :128], spread[:, 384:], keep]
    arrive += arrival_table(2)
    for k in (3, 4, 5):
        arrive += [padded(a, 128) for a in arrival_table(k)]
    parts = (t_low, plain[128:384], t_high, v1, s1[256:], w2, np.stack(deep), np.concatenate(arrive, axis=1))
    return [a.astype(jnp.bfloat16) for a in parts]


def split3(a):
    top = a.astype(BF16)
    rest = a - top.astype(F32)
    mid = rest.astype(BF16)
    return top, mid, (rest - mid.astype(F32)).astype(BF16)


def dot3(a, table):
    m = a.shape[0]
    p = jnp.dot(jnp.concatenate(split3(a), axis=0), table, preferred_element_type=F32)
    return p[0:m] + p[m : 2 * m] + p[2 * m : 3 * m]


BELOW = [None, (18, 26, 34, 42, 50, 58), (10, 18, 26), (6, 14), (4,), (3,)]
ABOVE = [None, (-1, 7, 15), (-1, 7), (-1,), (-1,), (-1,)]


def reduce_rows(t, src, dst, starts):
    for ch in range(CH):
        for j in starts:

            def tap(o):
                return src[ch, t, pl.ds(8 + 2 * j + o, 8, stride=2), :]

            dst[ch, t, 8 + j : 16 + j, :] = (tap(-2) + tap(2)) + (tap(-1) + tap(1)) * 4.0 + tap(0) * 6.0


def mirror_start(a, first):
    for t in range(4):
        a[:, t, 7:8, :] = a[:, t, pl.ds(jnp.where(first, 9, 7), 1), :]
        a[:, t, 6:7, :] = a[:, t, pl.ds(jnp.where(first, 10, 6), 1), :]


def mirror_end(a, h, last):
    for t in range(4):
        a[:, t, 8 + h : 9 + h, :] = a[:, t, pl.ds(jnp.where(last, 6 + h, 8 + h), 1), :]


def rows_of(k, y, tiles):
    return jnp.concatenate(
        [jnp.concatenate([y[c, t, 7 : 7 + R[k], :] for t in tiles], axis=1) for c in range(CH)], axis=0
    )


def detail(g, level, at, out, count):
    lo, mid, hi = (g[:, :, i : i + count, :] for i in range(3))
    even, odd = pl.ds(at, count, stride=2), pl.ds(at + 1, count, stride=2)
    out[:, :, pl.ds(0, count, stride=2), :] = level[:, :, even, :] - ((lo + hi) * 0.125 + mid * 0.75)
    out[:, :, pl.ds(1, count, stride=2), :] = level[:, :, odd, :] - (mid + hi) * 0.5


def exchange_kernel(
    x_hbm, tlow_hbm, tmid_hbm, thigh_hbm, v1_hbm, s1_hbm, w2_hbm, w345_hbm, arrive_hbm,
    d0, d1, d2, d3, d4, d5,
    xs, y1, y2, y3, y4, y5, tv, v1, s1, w2, w345, arrive, srs, ci,
    rh, rl, kh, kl, cb, rh_in, rl_in, cbm, cbp, chm, chp, clm, clp,
    g1, g2, g3, g4, g5, m1, m2, m3, m4, m5, d3w, d4w,
    load_sem, send_sem, recv_sem,
):
    r, c = lax.axis_index("rows"), lax.axis_index("cols")
    nr, nc = lax.axis_size("rows"), lax.axis_size("cols")
    first, last = r == 0, r == nr - 1
    left, right = c == 0, c == nc - 1
    up, down = jnp.logical_not(first), jnp.logical_not(last)
    west, east = jnp.logical_not(left), jnp.logical_not(right)

    def image(at, rows, sem):
        return [
            pltpu.make_async_copy(
                x_hbm.at[:, pl.ds(at, rows), pl.ds(128 * t, 128)], xs.at[:, t, pl.ds(8 + at, rows), :], load_sem.at[sem + t]
            )
            for t in range(4)
        ]

    loads = image(32, ROWS - 32, 0)
    upper = image(0, 32, 12)
    loads += [
        pltpu.make_async_copy(tlow_hbm.at[left.astype(jnp.int32)], tv.at[pl.ds(0, 128)], load_sem.at[4]),
        pltpu.make_async_copy(tmid_hbm, tv.at[pl.ds(128, 256)], load_sem.at[5]),
        pltpu.make_async_copy(thigh_hbm.at[right.astype(jnp.int32)], tv.at[pl.ds(384, 128)], load_sem.at[6]),
        pltpu.make_async_copy(v1_hbm, v1, load_sem.at[7]),
        pltpu.make_async_copy(s1_hbm, s1, load_sem.at[8]),
        pltpu.make_async_copy(w2_hbm, w2, load_sem.at[9]),
        pltpu.make_async_copy(w345_hbm, w345, load_sem.at[10]),
        pltpu.make_async_copy(arrive_hbm, arrive, load_sem.at[11]),
    ]
    for copy in loads[:4]:
        copy.start()

    def there(dr, dc):
        ok = jnp.bool_(True)
        if dr:
            ok = jnp.logical_and(ok, up if dr < 0 else down)
        if dc:
            ok = jnp.logical_and(ok, west if dc < 0 else east)
        return ok

    messages = [
        (rh, rh_in, 1, 0),
        (kh, chm, 1, 1),
        (kh, chp, 1, -1),
        (rl, rl_in, -1, 0),
        (kl, clm, -1, 1),
        (kl, clp, -1, -1),
        (cb, cbm, 0, 1),
        (cb, cbp, 0, -1),
    ]
    barrier = pltpu.get_barrier_semaphore()
    for _, dst, dr, dc in messages:

        @pl.when(there(dr, dc))
        def _(dr=dr, dc=dc):
            pl.semaphore_signal(barrier, inc=1, device_id=(r + dr, c + dc), device_id_type=MESH)

        @pl.when(jnp.logical_not(there(-dr, -dc)))
        def _(dst=dst):
            dst[...] = jnp.zeros_like(dst)

    for copy in loads[4:7] + upper:
        copy.start()

    ys = (xs, y1, y2, y3, y4, y5)
    for k in range(LEVELS):
        ys[k][:, :, 0:8, :] = jnp.zeros((CH, 4, 8, 128), F32)
        ys[k][:, :, 8 + H[k] : 32 + H[k], :] = jnp.zeros((CH, 4, 24, 128), F32)
    srs[...] = jnp.zeros_like(srs)
    ci[...] = jnp.zeros_like(ci)
    for a in (rh, kh, kl):
        a[...] = jnp.zeros_like(a)

    for copy in loads[:4]:
        copy.wait()
    for k in range(1, LEVELS + 1):
        if k == 3:
            for copy in loads[4:7]:
                copy.wait()
        mirror_end(ys[k - 1], H[k - 1], last)
        for t in range(4):
            reduce_rows(t, ys[k - 1], ys[k], BELOW[k])
        for ch in range(CH):
            at = 16 * (k - 1) + 3 * ch
            srs[:, at : at + 3, :] = ys[k][ch, :, 7 + H[k] : 10 + H[k], :]
    lane = lax.broadcasted_iota(jnp.int32, (16, 128), 1)

    def form_strips(out, corners, count):
        strips = jnp.concatenate([srs[t] for t in range(4)], axis=1)
        near = dot3(strips[0:32], tv[:, 0:512])
        deep = dot3(strips[32:80], tv[:, 512:1024])
        deep = deep[:, 0:256] + deep[:, 256:512]
        cells = jnp.where(lane < 32, deep[16:32, 0:128], deep[32:48, 0:128])
        cells = jnp.where(lane < 24, deep[0:16, 0:128], cells)
        cells = jnp.where(lane < 8, near[0:16, 256:384], jnp.where(lane < 16, near[16:32, 256:384], cells))
        beside = jnp.where(lane < 118, deep[0:16, 0:128], jnp.where(lane < 120, deep[16:32, 0:128], deep[32:48, 0:128]))
        beside = jnp.where(lane < 114, near[0:16, 256:384], jnp.where(lane < 116, near[16:32, 256:384], beside))
        small = jnp.where(lane < 96, deep[16:32, 128:256], deep[32:48, 128:256])
        small = jnp.where(lane < 64, deep[0:16, 128:256], jnp.where(lane < 112, small, beside))
        for t, a in enumerate((near[0:16, 0:128], near[0:16, 128:256], near[16:32, 384:512], small)):
            out[pl.ds(t, CH * count, stride=4), :] = a[0 : CH * count]
        ci[...] = jnp.where(lane < 40, cells, 0.0)
        corners[0:3, :] = sum(pltpu.roll(ci[pl.ds(i, CH, stride=count), :], 40 * i, 1) for i in range(count))

    form_strips(rh, kh, 3)
    place = lax.broadcasted_iota(jnp.int32, (8, 512), 1)

    def of_level(k, a):
        ok = place < (BASE[k + 1] if k < LEVELS else 480)
        return jnp.where(jnp.logical_and(ok, place >= BASE[k]), a, 0.0)

    def put(k, a, out):
        for ch in range(CH):
            for t in range(out.shape[1]):
                out[ch, t] = a[R[k] * ch : R[k] * (ch + 1), 128 * t : 128 * (t + 1)]

    deeper = ((3, 0, g3, m3), (4, 72, g4, m4), (5, 112, g5, m5))

    def reduce_rest():
        for copy in upper:
            copy.wait()
        for k in range(1, LEVELS + 1):
            mirror_start(ys[k - 1], first)
            for t in range(4):
                reduce_rows(t, ys[k - 1], ys[k], ABOVE[k])
        mirror_start(y5, first)
        for k in range(1, LEVELS + 1):
            for ch in range(CH):
                at = 16 * (k - 1) + 2 * ch
                srs[:, at : at + 2, :] = ys[k][ch, :, 7:9, :]
        form_strips(rl, kl, 2)
        outer = jnp.concatenate([rows_of(k, ys[k], (0, 3)) for k in range(1, LEVELS + 1)], axis=0)
        table = jnp.concatenate([tv[0:128], tv[384:512]], axis=0)
        turned = dot3(outer, jnp.concatenate([table[:, 256:384], table[:, 768:896]], axis=1))
        turned = jnp.concatenate([turned[:, 0:128] + turned[:, 128:256], jnp.zeros((32, 128), F32)], axis=0)
        turned = jnp.transpose(turned)
        cb[...] = sum(of_level(k, turned[8 * (k - 1) : 8 * k]) for k in range(1, LEVELS + 1))

    def expand_own():
        for copy in loads[7:]:
            copy.start()
        p12 = dot3(jnp.concatenate([rows_of(k, ys[k], range(4)) for k in (1, 2)], axis=0), tv[:, 0:512])
        p345 = dot3(jnp.concatenate([rows_of(k, ys[k], range(4)) for k in (3, 4, 5)], axis=0), tv[:, 512:1024])
        p345 = p345[:, 0:256] + p345[:, 256:512]

        for copy in loads[7:]:
            copy.wait()
        put(1, dot3(p12[0:224, 0:384], v1[...]), g1)
        put(1, p12, m1)
        both = dot3(p12[208:336, 256:512], w2[...])
        put(2, both[8:, 0:256], g2)
        put(2, both[8:, 256:384], m2)
        for k, at, g, m in deeper:
            both = dot3(p345[at : at + 16 * -(-3 * R[k] // 16)], w345[k - 3])
            skip = BASE[k] - BASE[3] - at
            put(k, both[skip:, 0:128], g)
            put(k, both[skip:, 128:256], m)

    early = lax.rem(r, 8) == 0

    @pl.when(early)
    def _():
        reduce_rest()
        expand_own()

    neighbours = (up.astype(jnp.int32) + down.astype(jnp.int32) + 1) * (
        west.astype(jnp.int32) + east.astype(jnp.int32) + 1
    ) - 1
    pl.semaphore_wait(barrier, neighbours)
    copies = []
    for m, (src, dst, dr, dc) in enumerate(messages):
        copies.append(
            pltpu.make_async_remote_copy(
                src_ref=src, dst_ref=dst, send_sem=send_sem.at[m], recv_sem=recv_sem.at[m],
                device_id=(r + dr, c + dc), device_id_type=MESH,
            )
        )
    for m in (1, 2, 0):
        pl.when(there(*messages[m][2:]))(copies[m].start)


    @pl.when(jnp.logical_not(early))
    def _():
        reduce_rest()

    for m in range(3, 8):
        pl.when(there(*messages[m][2:]))(copies[m].start)
    pl.when(jnp.logical_not(early))(expand_own)

    def add(k, a, out, tiles, first_tile=0):
        for ch in range(CH):
            for i, t in enumerate(tiles):
                lanes = 128 * (first_tile + i)
                out[ch, t] += a[R[k] * ch : R[k] * (ch + 1), lanes : lanes + 128]

    side = jnp.bitwise_and(lane, 7) < 3
    middle = jnp.logical_and(lane >= 64, lane < 104)
    ci[...] = jnp.zeros_like(ci)

    def add_rows(strip, minus, plus, count, row_of):
        corner = jnp.where(side[0:4], minus[...], plus[...])
        for i in range(count):
            ci[pl.ds(i, CH, stride=count), :] = pltpu.roll(corner, (64 - 40 * i) % 128, 1)[0:CH]
        rows = CH * count
        fill = jnp.zeros((16 - rows, 128), F32)
        tiles = [jnp.concatenate([strip[pl.ds(t, rows, stride=4), :], fill], axis=0) for t in range(4)]
        cells = jnp.where(lane < 112, jnp.where(middle, ci[...], 0.0), tiles[3])
        wide = dot3(jnp.concatenate([tiles[0], tiles[1], cells], axis=1), v1[...])
        level = jnp.concatenate(tiles[0:2], axis=1) + dot3(cells, s1[...])
        both = [dot3(jnp.concatenate([cells, tiles[2]], axis=1), w2[...])]
        tail = jnp.concatenate([cells, tiles[3]], axis=1)
        both += [dot3(tail, w345[k - 3]) for k in (3, 4, 5)]
        pairs = [(1, wide, g1), (1, level, m1), (2, both[0][:, 0:256], g2), (2, both[0][:, 256:384], m2)]
        for (k, _, g, m), a in zip(deeper, both[1:]):
            pairs += [(k, a[:, 0:128], g), (k, a[:, 128:256], m)]
        for k, a, out in pairs:
            at = row_of(k) + 1
            for ch in range(CH):
                for t in range(out.shape[1]):
                    out[ch, t, at : at + count, :] += a[count * ch : count * (ch + 1), 128 * t : 128 * (t + 1)]

    def details(counts):
        for g, level, at, out, count in zip((g1, g2, g3, g4, g5), (xs, m1, m2, m3, m4), (8, 1, 1, 1, 1), (d0, d1, d2, d3w, d4w), counts):
            detail(g, level, at, out, count)
        d3[...] = d3w[:, 0, :, 0:64]
        d4[...] = d4w[:, 0, :, 0:32]
        d5[...] = m5[:, 0, 1:5, 0:16]

    for m in (3, 4, 5):
        pl.when(there(-messages[m][2], -messages[m][3]))(copies[m].wait_recv)
    add_rows(rl_in, clm, clp, 2, lambda k: H[k] - 1)
    for m in (6, 7):
        pl.when(there(-messages[m][2], -messages[m][3]))(copies[m].wait_recv)
    sub = lax.broadcasted_iota(jnp.int32, (8, 512), 0)
    terms = [a.astype(F32) for a in split3(jnp.where(sub < 3, cbm[...], cbp[...]))]
    came = jnp.concatenate(
        [of_level(k, a) for k in range(1, LEVELS + 1) for a in terms] + [jnp.zeros((8, 512), F32)], axis=0
    )
    came = jnp.transpose(came)

    def arrived(k, at, rows, lanes, count):
        return jnp.dot(
            came[at : at + rows].astype(BF16), arrive[:, lanes : lanes + count], preferred_element_type=F32
        )[BASE[k] - at :]

    more = arrived(1, 0, 224, 0, 512)
    add(1, more, g1, (0, 3))
    add(1, more, m1, (0, 1), 2)
    more = arrived(2, 208, 128, 512, 384)
    add(2, more, g2, (0, 1))
    add(2, more, m2, (0,), 2)
    for k, at, g, m in deeper:
        more = arrived(k, BASE[3] + at, 16 * -(-3 * R[k] // 16), 896 + 256 * (k - 3), 256)
        add(k, more, g, (0,))
        add(k, more, m, (0,), 1)

    for k, g in enumerate((g1, g2, g3, g4, g5), 1):
        g[:, :, H[k] + 1 : H[k] + 2, :] = g[:, :, pl.ds(jnp.where(last, H[k], H[k] + 1), 1), :]
    details(H[1:6])
    for m in range(3):
        pl.when(there(-messages[m][2], -messages[m][3]))(copies[m].wait_recv)
    add_rows(rh_in, chm, chp, 3, lambda k: -1)
    details((4,) * 5)
    for copy, (_, _, dr, dc) in zip(copies, messages):
        pl.when(there(dr, dc))(copy.wait_send)


def result_kernel(d0, d1, d2, d3, d4, d5, o0, o1, o2, o3, o4, o5, sem):
    pairs = [(d0.at[:, t], o0.at[:, :, pl.ds(128 * t, 128)]) for t in range(4)]
    pairs += [(d1.at[:, t], o1.at[:, :, pl.ds(128 * t, 128)]) for t in range(2)]
    pairs += [(d2.at[:, 0], o2), (d3, o3), (d4, o4), (d5, o5)]
    copies = [pltpu.make_async_copy(src, dst, sem.at[i]) for i, (src, dst) in enumerate(pairs)]
    for copy in copies:
        copy.start()
    for copy in copies:
        copy.wait()


def body(orthophoto):
    def vmem(*shape, dtype=F32):
        return pltpu.VMEM(shape, dtype)

    held = [(CH, 4, H[0], 128), (CH, 2, H[1], 128), (CH, 1, H[2], 128)]
    held += [(CH, H[3], W[3]), (CH, H[4], W[4]), (CH, H[5], W[5])]
    scratch = [vmem(CH, 4, H[k] + 32, 128) for k in range(6)]
    scratch += [vmem(512, 1024, dtype=BF16), vmem(384, 512, dtype=BF16), vmem(128, 256, dtype=BF16)]
    scratch += [vmem(256, 384, dtype=BF16), vmem(3, 256, 256, dtype=BF16), vmem(128, 1664, dtype=BF16)]
    scratch += [vmem(4, 80, 128), vmem(16, 128)]
    scratch += [vmem(40, 128), vmem(24, 128), vmem(4, 128), vmem(4, 128), vmem(8, 512)]
    scratch += [vmem(40, 128), vmem(24, 128), vmem(8, 512), vmem(8, 512)]
    scratch += [vmem(4, 128)] * 4
    scratch += [vmem(CH, t, R[k], 128) for k, t in ((1, 4), (2, 2), (3, 1), (4, 1), (5, 1))]
    scratch += [vmem(CH, t, R[k], 128) for k, t in ((1, 2), (2, 1), (3, 1), (4, 1), (5, 1))]
    scratch += [vmem(CH, 1, H[3], 128), vmem(CH, 1, H[4], 128)]
    scratch += [pltpu.SemaphoreType.DMA((n,)) for n in (16, 8, 8)]
    far = pl.BlockSpec(memory_space=pltpu.HBM)
    inside = pl.BlockSpec(memory_space=pltpu.VMEM)
    inputs = [pltpu.with_memory_space_constraint(jnp.asarray(a), pltpu.HBM) for a in (orthophoto, *tables())]
    arrays = pl.pallas_call(
        exchange_kernel,
        out_shape=[jax.ShapeDtypeStruct(shape, F32) for shape in held],
        in_specs=[far] * len(inputs),
        out_specs=[inside] * len(held),
        scratch_shapes=scratch,
        compiler_params=pltpu.CompilerParams(collective_id=0, has_side_effects=True, vmem_limit_bytes=24 << 20),
    )(*inputs)
    results = pl.pallas_call(
        result_kernel,
        out_shape=[jax.ShapeDtypeStruct((CH, H[k], W[k]), F32) for k in range(6)],
        in_specs=[inside] * len(held),
        out_specs=[far] * 6,
        scratch_shapes=[pltpu.SemaphoreType.DMA((10,))],
        compiler_params=pltpu.CompilerParams(vmem_limit_bytes=8 << 20),
    )(*arrays)
    return tuple(results)


def solution(mesh):
    placed = P(None, "rows", "cols")
    return jax.shard_map(body, mesh=mesh, in_specs=(placed,), out_specs=(placed,) * 6, check_vma=False)
```

```python
import functools

import jax
import jax.numpy as jnp
import numpy as np
from jax import lax
from jax.experimental import pallas as pl
from jax.experimental.pallas import tpu as pltpu
from jax.sharding import PartitionSpec as P

CH = 3
ROWS = 128
COLS = 512
LEVELS = 5
H = [ROWS >> k for k in range(6)]
W = [COLS >> k for k in range(6)]
R = [0, 72, 40, 24, 16, 8]
BASE = [0, 0, 216, 336, 408, 456]
POS = [0, 0, 0, 0, 64, 96]
F32 = jnp.float32
BF16 = jnp.bfloat16
MESH = pl.DeviceIdType.MESH
TAPS = (1.0, 4.0, 6.0, 4.0, 1.0)


def column_reductions(low, high):
    result = [None]
    total = None
    for k in range(1, LEVELS + 1):
        n = W[k - 1]
        step = np.zeros((n + 3, W[k] + 3))
        for j in range(0 if low else -1, W[k] if high else W[k] + 2):
            for tap in range(5):
                cell = 2 * j - 2 + tap
                if low and cell < 0:
                    cell = -cell
                if high and cell > n - 1:
                    cell = 2 * (n - 1) - cell
                if -1 <= cell <= n + 1:
                    step[cell + 1, j + 1] += TAPS[tap] / 16
        total = step[1 : n + 1] if k == 1 else total @ step
        result.append(total / 16.0**k)
    return result


def reduction_table(low, high):
    t = column_reductions(low, high)

    def fill(a, at, k):
        beyond, before = W[k] - 1 if high else W[k], 1 if low else -1
        cells = (W[k] - 1, beyond, W[k] + 1, before, 0)
        a[:, at + 8 * (k - 1) : at + 8 * (k - 1) + 5] = t[k][:, [c + 1 for c in cells]]
        a[:, at + 112 + 2 * (k - 1) : at + 114 + 2 * (k - 1)] = t[k][:, [beyond + 1, before + 1]]

    near = np.zeros((COLS, 384))
    near[:, 0:256] = t[1][:, 1:257]
    near[:, 256:384] = t[2][:, 1:129]
    deep, cells = np.zeros((COLS, 128)), np.zeros((COLS, 128))
    for k in range(1, LEVELS + 1):
        fill(cells, 0, k)
        if k > 2:
            deep[:, POS[k] : POS[k] + W[k]] = t[k][:, 1 : W[k] + 1]
    assert not cells[128:384].any()
    return np.concatenate([near, *two_terms(deep)], axis=1), np.concatenate(two_terms(cells), axis=1)


def two_terms(a):
    top = np.asarray(a.astype(jnp.bfloat16), np.float64)
    rest = np.asarray((a - top).astype(jnp.bfloat16), np.float64)
    assert np.array_equal(top + rest, a)
    return top, rest


def expansion_row(k, cell):
    row = np.zeros(2 * W[k])
    for i in range(W[k]):
        row[2 * i] += {i - 1: 0.125, i: 0.75, i + 1: 0.125}.get(cell, 0.0)
        row[2 * i + 1] += {i: 0.5, i + 1: 0.5}.get(cell, 0.0)
    return row


def expansion_table(k, main_at, edge_at, lanes):
    spread = np.zeros((lanes, 2 * W[k]))
    keep = np.zeros((lanes, W[k]))
    for c in range(W[k]):
        spread[main_at + c] = expansion_row(k, c)
        keep[main_at + c, c] = 1
    own = edge_at + 112 + 2 * (k - 1)
    came = edge_at + 64 + 8 * (k - 1)
    spread[own] = expansion_row(k, W[k])
    spread[own + 1] = expansion_row(k, -1)
    for s, cell in enumerate((-1, 0, 1, W[k] - 1, W[k])):
        spread[came + s] = expansion_row(k, cell)
        if 0 <= cell < W[k]:
            keep[came + s, cell] = 1
    return spread, keep


def arrival_table(k):
    spread = np.zeros((128, 2 * W[k]))
    keep = np.zeros((128, W[k]))
    for part in range(3):
        for s, cell in enumerate((-1, 0, 1, W[k] - 1, W[k])):
            lane = 24 * (k - 1) + 8 * part + s
            spread[lane] = expansion_row(k, cell)
            if 0 <= cell < W[k]:
                keep[lane, cell] = 1
    return spread, keep


def padded(a, cols):
    return np.pad(a, ((0, 0), (0, cols - a.shape[1])))


def tables():
    (plain, cells), (low, cells_low), (high, cells_high) = (
        reduction_table(*e) for e in ((False, False), (True, False), (False, True))
    )
    assert np.array_equal(plain[128:], low[128:]) and np.array_equal(plain[:384], high[:384])
    assert np.array_equal(plain[:, 0:384], np.asarray(plain[:, 0:384].astype(jnp.bfloat16), np.float64))
    t_low = np.stack([plain[:128], low[:128]])
    t_high = np.stack([plain[384:], high[384:]])
    c_low = np.stack([cells[:128], cells_low[:128]])
    c_high = np.stack([cells[384:], cells_high[384:]])
    v1, s1 = expansion_table(1, 0, 256, 384)
    w2 = np.concatenate(expansion_table(2, 128, 0, 256), axis=1)
    deep = []
    for k in (3, 4, 5):
        spread, keep = expansion_table(k, 128 + POS[k], 0, 256)
        deep.append(np.concatenate([padded(spread, 128), padded(keep, 128)], axis=1))
    spread, keep = arrival_table(1)
    assert not spread[:, 128:384].any()
    arrive = [spread[:, :128], spread[:, 384:], keep]
    arrive += arrival_table(2)
    for k in (3, 4, 5):
        arrive += [padded(a, 128) for a in arrival_table(k)]
    parts = (c_low, c_high, t_low, plain[128:384], t_high, v1, s1[256:], w2, np.stack(deep), np.concatenate(arrive, axis=1))
    return [a.astype(jnp.bfloat16) for a in parts]


def split3(a):
    top = a.astype(BF16)
    rest = a - top.astype(F32)
    mid = rest.astype(BF16)
    return top, mid, (rest - mid.astype(F32)).astype(BF16)


def dot3(a, table):
    m = a.shape[0]
    p = jnp.dot(jnp.concatenate(split3(a), axis=0), table, preferred_element_type=F32)
    return p[0:m] + p[m : 2 * m] + p[2 * m : 3 * m]


BELOW = [None, (18, 26, 34, 42, 50, 58), (10, 18, 26), (6, 14), (4,), (3,)]
ABOVE = [None, (-1, 7, 15), (-1, 7), (-1,), (-1,), (-1,)]


def reduce_rows(t, src, dst, starts):
    for ch in range(CH):
        for j in starts:

            def tap(o):
                return src[ch, t, pl.ds(8 + 2 * j + o, 8, stride=2), :]

            dst[ch, t, 8 + j : 16 + j, :] = (tap(-2) + tap(2)) + (tap(-1) + tap(1)) * 4.0 + tap(0) * 6.0


def mirror_start(a, first):
    for t in range(4):
        a[:, t, 7:8, :] = a[:, t, pl.ds(jnp.where(first, 9, 7), 1), :]
        a[:, t, 6:7, :] = a[:, t, pl.ds(jnp.where(first, 10, 6), 1), :]


def mirror_end(a, tiles, h, last):
    for t in tiles:
        a[:, t, 8 + h : 9 + h, :] = a[:, t, pl.ds(jnp.where(last, 6 + h, 8 + h), 1), :]


def rows_of(k, y, tiles):
    return jnp.concatenate(
        [jnp.concatenate([y[c, t, 7 : 7 + R[k], :] for t in tiles], axis=1) for c in range(CH)], axis=0
    )


def detail(g, level, at, out, count):
    lo, mid, hi = (g[:, :, i : i + count, :] for i in range(3))
    even, odd = pl.ds(at, count, stride=2), pl.ds(at + 1, count, stride=2)
    out[:, :, pl.ds(0, count, stride=2), :] = level[:, :, even, :] - ((lo + hi) * 0.125 + mid * 0.75)
    out[:, :, pl.ds(1, count, stride=2), :] = level[:, :, odd, :] - (mid + hi) * 0.5


def exchange_kernel(
    x_hbm, clow_hbm, chigh_hbm, tlow_hbm, tmid_hbm, thigh_hbm, v1_hbm, s1_hbm, w2_hbm, w345_hbm, arrive_hbm,
    d0, d1, d2, d3, d4, d5,
    xs, y1, y2, y3, y4, y5, tc, co, tv, v1, s1, w2, w345, arrive, srs, ci, beside,
    rh, rl, kh, kl, cb, rh_in, rl_in, cbm, cbp, chm, chp, clm, clp,
    g1, g2, g3, g4, g5, m1, m2, m3, m4, m5, d3w, d4w,
    load_sem, send_sem, recv_sem,
):
    r, c = lax.axis_index("rows"), lax.axis_index("cols")
    nr, nc = lax.axis_size("rows"), lax.axis_size("cols")
    first, last = r == 0, r == nr - 1
    left, right = c == 0, c == nc - 1
    up, down = jnp.logical_not(first), jnp.logical_not(last)
    west, east = jnp.logical_not(left), jnp.logical_not(right)

    def image(at, rows, sem):
        return [
            pltpu.make_async_copy(
                x_hbm.at[:, pl.ds(at, rows), pl.ds(128 * t, 128)], xs.at[:, t, pl.ds(8 + at, rows), :], load_sem.at[sem + t]
            )
            for t in range(4)
        ]

    lower = image(32, ROWS - 32, 0)
    upper = image(0, 32, 4)
    at_left, at_right = left.astype(jnp.int32), right.astype(jnp.int32)
    cell_tables = [
        pltpu.make_async_copy(clow_hbm.at[at_left], tc.at[pl.ds(0, 128)], load_sem.at[8]),
        pltpu.make_async_copy(chigh_hbm.at[at_right], tc.at[pl.ds(128, 128)], load_sem.at[9]),
    ]
    row_tables = [
        pltpu.make_async_copy(tlow_hbm.at[at_left], tv.at[pl.ds(0, 128)], load_sem.at[10]),
        pltpu.make_async_copy(tmid_hbm, tv.at[pl.ds(128, 256)], load_sem.at[11]),
        pltpu.make_async_copy(thigh_hbm.at[at_right], tv.at[pl.ds(384, 128)], load_sem.at[12]),
    ]
    own_tables = [
        pltpu.make_async_copy(v1_hbm, v1, load_sem.at[13]),
        pltpu.make_async_copy(s1_hbm, s1, load_sem.at[14]),
        pltpu.make_async_copy(w2_hbm, w2, load_sem.at[15]),
        pltpu.make_async_copy(w345_hbm, w345, load_sem.at[16]),
        pltpu.make_async_copy(arrive_hbm, arrive, load_sem.at[17]),
    ]
    for copy in (lower[0], lower[3], *cell_tables, lower[1], lower[2], *row_tables):
        copy.start()

    def there(dr, dc):
        ok = jnp.bool_(True)
        if dr:
            ok = jnp.logical_and(ok, up if dr < 0 else down)
        if dc:
            ok = jnp.logical_and(ok, west if dc < 0 else east)
        return ok

    messages = [
        (rh, rh_in, 1, 0),
        (kh, chm, 1, 1),
        (kh, chp, 1, -1),
        (rl, rl_in, -1, 0),
        (kl, clm, -1, 1),
        (kl, clp, -1, -1),
        (cb, cbm, 0, 1),
        (cb, cbp, 0, -1),
    ]
    barrier = pltpu.get_barrier_semaphore()
    for _, dst, dr, dc in messages:

        @pl.when(there(dr, dc))
        def _(dr=dr, dc=dc):
            pl.semaphore_signal(barrier, inc=1, device_id=(r + dr, c + dc), device_id_type=MESH)

        @pl.when(jnp.logical_not(there(-dr, -dc)))
        def _(dst=dst):
            dst[...] = jnp.zeros_like(dst)

    for copy in upper:
        copy.start()

    ys = (xs, y1, y2, y3, y4, y5)
    for k in range(LEVELS):
        ys[k][:, :, 0:8, :] = jnp.zeros((CH, 4, 8, 128), F32)
        ys[k][:, :, 8 + H[k] : 32 + H[k], :] = jnp.zeros((CH, 4, 24, 128), F32)
    srs[...] = jnp.zeros_like(srs)
    ci[...] = jnp.zeros_like(ci)
    for a in (rh, kh, kl):
        a[...] = jnp.zeros_like(a)

    lane = lax.broadcasted_iota(jnp.int32, (16, 128), 1)

    def reduce_lower(tiles):
        for k in range(1, LEVELS + 1):
            mirror_end(ys[k - 1], tiles, H[k - 1], last)
            for t in tiles:
                reduce_rows(t, ys[k - 1], ys[k], BELOW[k])
            for ch in range(CH):
                at = 16 * (k - 1) + 3 * ch
                for t in tiles:
                    srs[t, at : at + 3, :] = ys[k][ch, t, 7 + H[k] : 10 + H[k], :]

    def form_corners(corners, count):
        both = dot3(jnp.concatenate([srs[0], srs[3]], axis=1), tc[...])
        both = both[:, 0:128] + both[:, 128:256]
        level = [both[16 * k : 16 * k + 16] for k in range(LEVELS)]
        cells, halo = level[4], level[4]
        for k in (3, 2, 1, 0):
            cells = jnp.where(lane < 8 * k + 8, level[k], cells)
            halo = jnp.where(lane < 114 + 2 * k, level[k], halo)
        beside[...] = halo
        ci[...] = jnp.where(lane < 40, cells, 0.0)
        corners[0:3, :] = sum(pltpu.roll(ci[pl.ds(i, CH, stride=count), :], 40 * i, 1) for i in range(count))

    def form_strips(out, count):
        strips = jnp.concatenate([srs[t] for t in range(4)], axis=1)
        near = dot3(strips[0:32], tv[:, 0:384])
        deep = dot3(strips[32:80], tv[:, 384:640])
        deep = deep[:, 0:128] + deep[:, 128:256]
        small = jnp.where(lane < 96, deep[16:32], deep[32:48])
        small = jnp.where(lane < 64, deep[0:16], jnp.where(lane < 112, small, beside[...]))
        for t, a in enumerate((near[0:16, 0:128], near[0:16, 128:256], near[16:32, 256:384], small)):
            out[pl.ds(t, CH * count, stride=4), :] = a[0 : CH * count]

    for copy in (lower[0], lower[3]):
        copy.wait()
    reduce_lower((0, 3))
    for copy in cell_tables:
        copy.wait()
    form_corners(kh, 3)

    place = lax.broadcasted_iota(jnp.int32, (8, 512), 1)

    def of_level(k, a):
        ok = place < (BASE[k + 1] if k < LEVELS else 480)
        return jnp.where(jnp.logical_and(ok, place >= BASE[k]), a, 0.0)

    def put(k, a, out):
        for ch in range(CH):
            for t in range(out.shape[1]):
                out[ch, t] = a[R[k] * ch : R[k] * (ch + 1), 128 * t : 128 * (t + 1)]

    deeper = ((3, 0, g3, m3), (4, 72, g4, m4), (5, 112, g5, m5))

    def reduce_rest():
        for copy in upper:
            copy.wait()
        for k in range(1, LEVELS + 1):
            mirror_start(ys[k - 1], first)
            for t in range(4):
                reduce_rows(t, ys[k - 1], ys[k], ABOVE[k])
        mirror_start(y5, first)
        for k in range(1, LEVELS + 1):
            for ch in range(CH):
                at = 16 * (k - 1) + 2 * ch
                srs[:, at : at + 2, :] = ys[k][ch, :, 7:9, :]
        form_corners(kl, 2)
        form_strips(rl, 2)
        outer = jnp.concatenate([rows_of(k, ys[k], (0, 3)) for k in range(1, LEVELS + 1)], axis=0)
        cells = dot3(outer, tc[...])
        cells = cells[:, 0:128] + cells[:, 128:256]
        co[...] = cells
        turned = jnp.concatenate([cells, jnp.zeros((32, 128), F32)], axis=0)
        turned = jnp.transpose(turned)
        cb[...] = sum(of_level(k, turned[8 * (k - 1) : 8 * k]) for k in range(1, LEVELS + 1))

    def expand_own():
        for copy in own_tables:
            copy.start()
        p12 = dot3(jnp.concatenate([rows_of(k, ys[k], range(4)) for k in (1, 2)], axis=0), tv[:, 0:384])
        p345 = dot3(jnp.concatenate([rows_of(k, ys[k], range(4)) for k in (3, 4, 5)], axis=0), tv[:, 384:640])
        p345 = p345[:, 0:128] + p345[:, 128:256]
        cells = co[...]
        for copy in own_tables:
            copy.wait()
        put(1, dot3(jnp.concatenate([p12[0:224, 0:256], cells[0:224]], axis=1), v1[...]), g1)
        put(1, p12, m1)
        both = dot3(jnp.concatenate([cells[208:336], p12[208:336, 256:384]], axis=1), w2[...])
        put(2, both[8:, 0:256], g2)
        put(2, both[8:, 256:384], m2)
        for k, at, g, m in deeper:
            rows = 16 * -(-3 * R[k] // 16)
            both = dot3(jnp.concatenate([cells[336 + at : 336 + at + rows], p345[at : at + rows]], axis=1), w345[k - 3])
            skip = BASE[k] - BASE[3] - at
            put(k, both[skip:, 0:128], g)
            put(k, both[skip:, 128:256], m)

    early = lax.rem(r, 8) == 0

    def finish_lower():
        for copy in (lower[1], lower[2]):
            copy.wait()
        reduce_lower((1, 2))
        for copy in row_tables:
            copy.wait()
        form_strips(rh, 3)

    @pl.when(early)
    def _():
        finish_lower()
        reduce_rest()
        expand_own()

    neighbours = (up.astype(jnp.int32) + down.astype(jnp.int32) + 1) * (
        west.astype(jnp.int32) + east.astype(jnp.int32) + 1
    ) - 1
    pl.semaphore_wait(barrier, neighbours)
    copies = []
    for m, (src, dst, dr, dc) in enumerate(messages):
        copies.append(
            pltpu.make_async_remote_copy(
                src_ref=src, dst_ref=dst, send_sem=send_sem.at[m], recv_sem=recv_sem.at[m],
                device_id=(r + dr, c + dc), device_id_type=MESH,
            )
        )
    for m in (1, 2):
        pl.when(there(*messages[m][2:]))(copies[m].start)
    pl.when(jnp.logical_not(early))(finish_lower)
    pl.when(there(1, 0))(copies[0].start)


    @pl.when(jnp.logical_not(early))
    def _():
        reduce_rest()

    for m in range(3, 8):
        pl.when(there(*messages[m][2:]))(copies[m].start)
    pl.when(jnp.logical_not(early))(expand_own)

    def add(k, a, out, tiles, first_tile=0):
        for ch in range(CH):
            for i, t in enumerate(tiles):
                lanes = 128 * (first_tile + i)
                out[ch, t] += a[R[k] * ch : R[k] * (ch + 1), lanes : lanes + 128]

    side = jnp.bitwise_and(lane, 7) < 3
    middle = jnp.logical_and(lane >= 64, lane < 104)
    ci[...] = jnp.zeros_like(ci)

    def add_rows(strip, minus, plus, count, row_of):
        corner = jnp.where(side[0:4], minus[...], plus[...])
        for i in range(count):
            ci[pl.ds(i, CH, stride=count), :] = pltpu.roll(corner, (64 - 40 * i) % 128, 1)[0:CH]
        rows = CH * count
        fill = jnp.zeros((16 - rows, 128), F32)
        tiles = [jnp.concatenate([strip[pl.ds(t, rows, stride=4), :], fill], axis=0) for t in range(4)]
        cells = jnp.where(lane < 112, jnp.where(middle, ci[...], 0.0), tiles[3])
        wide = dot3(jnp.concatenate([tiles[0], tiles[1], cells], axis=1), v1[...])
        level = jnp.concatenate(tiles[0:2], axis=1) + dot3(cells, s1[...])
        both = [dot3(jnp.concatenate([cells, tiles[2]], axis=1), w2[...])]
        tail = jnp.concatenate([cells, tiles[3]], axis=1)
        both += [dot3(tail, w345[k - 3]) for k in (3, 4, 5)]
        pairs = [(1, wide, g1), (1, level, m1), (2, both[0][:, 0:256], g2), (2, both[0][:, 256:384], m2)]
        for (k, _, g, m), a in zip(deeper, both[1:]):
            pairs += [(k, a[:, 0:128], g), (k, a[:, 128:256], m)]
        for k, a, out in pairs:
            at = row_of(k) + 1
            for ch in range(CH):
                for t in range(out.shape[1]):
                    out[ch, t, at : at + count, :] += a[count * ch : count * (ch + 1), 128 * t : 128 * (t + 1)]

    def details(counts):
        for g, level, at, out, count in zip((g1, g2, g3, g4, g5), (xs, m1, m2, m3, m4), (8, 1, 1, 1, 1), (d0, d1, d2, d3w, d4w), counts):
            detail(g, level, at, out, count)
        d3[...] = d3w[:, 0, :, 0:64]
        d4[...] = d4w[:, 0, :, 0:32]
        d5[...] = m5[:, 0, 1:5, 0:16]

    for m in (3, 4, 5):
        pl.when(there(-messages[m][2], -messages[m][3]))(copies[m].wait_recv)
    add_rows(rl_in, clm, clp, 2, lambda k: H[k] - 1)
    for m in (6, 7):
        pl.when(there(-messages[m][2], -messages[m][3]))(copies[m].wait_recv)
    sub = lax.broadcasted_iota(jnp.int32, (8, 512), 0)
    terms = [a.astype(F32) for a in split3(jnp.where(sub < 3, cbm[...], cbp[...]))]
    came = jnp.concatenate(
        [of_level(k, a) for k in range(1, LEVELS + 1) for a in terms] + [jnp.zeros((8, 512), F32)], axis=0
    )
    came = jnp.transpose(came)

    def arrived(k, at, rows, lanes, count):
        return jnp.dot(
            came[at : at + rows].astype(BF16), arrive[:, lanes : lanes + count], preferred_element_type=F32
        )[BASE[k] - at :]

    more = arrived(1, 0, 224, 0, 512)
    add(1, more, g1, (0, 3))
    add(1, more, m1, (0, 1), 2)
    more = arrived(2, 208, 128, 512, 384)
    add(2, more, g2, (0, 1))
    add(2, more, m2, (0,), 2)
    for k, at, g, m in deeper:
        more = arrived(k, BASE[3] + at, 16 * -(-3 * R[k] // 16), 896 + 256 * (k - 3), 256)
        add(k, more, g, (0,))
        add(k, more, m, (0,), 1)

    for k, g in enumerate((g1, g2, g3, g4, g5), 1):
        g[:, :, H[k] + 1 : H[k] + 2, :] = g[:, :, pl.ds(jnp.where(last, H[k], H[k] + 1), 1), :]
    details(H[1:6])
    for m in range(3):
        pl.when(there(-messages[m][2], -messages[m][3]))(copies[m].wait_recv)
    add_rows(rh_in, chm, chp, 3, lambda k: -1)
    details((4,) * 5)
    for copy, (_, _, dr, dc) in zip(copies, messages):
        pl.when(there(dr, dc))(copy.wait_send)


def result_kernel(d0, d1, d2, d3, d4, d5, o0, o1, o2, o3, o4, o5, sem):
    pairs = [(d0.at[:, t], o0.at[:, :, pl.ds(128 * t, 128)]) for t in range(4)]
    pairs += [(d1.at[:, t], o1.at[:, :, pl.ds(128 * t, 128)]) for t in range(2)]
    pairs += [(d2.at[:, 0], o2), (d3, o3), (d4, o4), (d5, o5)]
    copies = [pltpu.make_async_copy(src, dst, sem.at[i]) for i, (src, dst) in enumerate(pairs)]
    for copy in copies:
        copy.start()
    for copy in copies:
        copy.wait()


def body(orthophoto):
    def vmem(*shape, dtype=F32):
        return pltpu.VMEM(shape, dtype)

    held = [(CH, 4, H[0], 128), (CH, 2, H[1], 128), (CH, 1, H[2], 128)]
    held += [(CH, H[3], W[3]), (CH, H[4], W[4]), (CH, H[5], W[5])]
    scratch = [vmem(CH, 4, H[k] + 32, 128) for k in range(6)]
    scratch += [vmem(256, 256, dtype=BF16), vmem(480, 128)]
    scratch += [vmem(512, 640, dtype=BF16), vmem(384, 512, dtype=BF16), vmem(128, 256, dtype=BF16)]
    scratch += [vmem(256, 384, dtype=BF16), vmem(3, 256, 256, dtype=BF16), vmem(128, 1664, dtype=BF16)]
    scratch += [vmem(4, 80, 128), vmem(16, 128), vmem(16, 128)]
    scratch += [vmem(40, 128), vmem(24, 128), vmem(4, 128), vmem(4, 128), vmem(8, 512)]
    scratch += [vmem(40, 128), vmem(24, 128), vmem(8, 512), vmem(8, 512)]
    scratch += [vmem(4, 128)] * 4
    scratch += [vmem(CH, t, R[k], 128) for k, t in ((1, 4), (2, 2), (3, 1), (4, 1), (5, 1))]
    scratch += [vmem(CH, t, R[k], 128) for k, t in ((1, 2), (2, 1), (3, 1), (4, 1), (5, 1))]
    scratch += [vmem(CH, 1, H[3], 128), vmem(CH, 1, H[4], 128)]
    scratch += [pltpu.SemaphoreType.DMA((n,)) for n in (18, 8, 8)]
    far = pl.BlockSpec(memory_space=pltpu.HBM)
    inside = pl.BlockSpec(memory_space=pltpu.VMEM)
    inputs = [pltpu.with_memory_space_constraint(jnp.asarray(a), pltpu.HBM) for a in (orthophoto, *tables())]
    arrays = pl.pallas_call(
        exchange_kernel,
        out_shape=[jax.ShapeDtypeStruct(shape, F32) for shape in held],
        in_specs=[far] * len(inputs),
        out_specs=[inside] * len(held),
        scratch_shapes=scratch,
        compiler_params=pltpu.CompilerParams(collective_id=0, has_side_effects=True, vmem_limit_bytes=24 << 20),
    )(*inputs)
    results = pl.pallas_call(
        result_kernel,
        out_shape=[jax.ShapeDtypeStruct((CH, H[k], W[k]), F32) for k in range(6)],
        in_specs=[inside] * len(held),
        out_specs=[far] * 6,
        scratch_shapes=[pltpu.SemaphoreType.DMA((10,))],
        compiler_params=pltpu.CompilerParams(vmem_limit_bytes=8 << 20),
    )(*arrays)
    return tuple(results)


def solution(mesh):
    placed = P(None, "rows", "cols")
    return jax.shard_map(body, mesh=mesh, in_specs=(placed,), out_specs=(placed,) * 6, check_vma=False)
```

```python
import functools

import jax
import jax.numpy as jnp
import numpy as np
from jax import lax
from jax.experimental import pallas as pl
from jax.experimental.pallas import tpu as pltpu
from jax.sharding import PartitionSpec as P

CH = 3
ROWS = 128
COLS = 512
LEVELS = 5
H = [ROWS >> k for k in range(6)]
W = [COLS >> k for k in range(6)]
R = [0, 72, 40, 24, 16, 8]
BASE = [0, 0, 216, 336, 408, 456]
POS = [0, 0, 0, 0, 64, 96]
F32 = jnp.float32
BF16 = jnp.bfloat16
MESH = pl.DeviceIdType.MESH
TAPS = (1.0, 4.0, 6.0, 4.0, 1.0)


def column_reductions(low, high):
    result = [None]
    total = None
    for k in range(1, LEVELS + 1):
        n = W[k - 1]
        step = np.zeros((n + 3, W[k] + 3))
        for j in range(0 if low else -1, W[k] if high else W[k] + 2):
            for tap in range(5):
                cell = 2 * j - 2 + tap
                if low and cell < 0:
                    cell = -cell
                if high and cell > n - 1:
                    cell = 2 * (n - 1) - cell
                if -1 <= cell <= n + 1:
                    step[cell + 1, j + 1] += TAPS[tap] / 16
        total = step[1 : n + 1] if k == 1 else total @ step
        result.append(total / 16.0**k)
    return result


def reduction_table(low, high):
    t = column_reductions(low, high)

    def fill(a, at, k):
        beyond, before = W[k] - 1 if high else W[k], 1 if low else -1
        cells = (W[k] - 1, beyond, W[k] + 1, before, 0)
        a[:, at + 8 * (k - 1) : at + 8 * (k - 1) + 5] = t[k][:, [c + 1 for c in cells]]
        a[:, at + 112 + 2 * (k - 1) : at + 114 + 2 * (k - 1)] = t[k][:, [beyond + 1, before + 1]]

    near = np.zeros((COLS, 384))
    near[:, 0:256] = t[1][:, 1:257]
    near[:, 256:384] = t[2][:, 1:129]
    deep, cells = np.zeros((COLS, 128)), np.zeros((COLS, 128))
    for k in range(1, LEVELS + 1):
        fill(cells, 0, k)
        if k > 2:
            deep[:, POS[k] : POS[k] + W[k]] = t[k][:, 1 : W[k] + 1]
    assert not cells[128:384].any()
    return np.concatenate([near, *two_terms(deep)], axis=1), np.concatenate(two_terms(cells), axis=1)


def two_terms(a):
    top = np.asarray(a.astype(jnp.bfloat16), np.float64)
    rest = np.asarray((a - top).astype(jnp.bfloat16), np.float64)
    assert np.array_equal(top + rest, a)
    return top, rest


def expansion_row(k, cell):
    row = np.zeros(2 * W[k])
    for i in range(W[k]):
        row[2 * i] += {i - 1: 0.125, i: 0.75, i + 1: 0.125}.get(cell, 0.0)
        row[2 * i + 1] += {i: 0.5, i + 1: 0.5}.get(cell, 0.0)
    return row


def expansion_table(k, main_at, edge_at, lanes):
    spread = np.zeros((lanes, 2 * W[k]))
    keep = np.zeros((lanes, W[k]))
    for c in range(W[k]):
        spread[main_at + c] = expansion_row(k, c)
        keep[main_at + c, c] = 1
    own = edge_at + 112 + 2 * (k - 1)
    came = edge_at + 64 + 8 * (k - 1)
    spread[own] = expansion_row(k, W[k])
    spread[own + 1] = expansion_row(k, -1)
    for s, cell in enumerate((-1, 0, 1, W[k] - 1, W[k])):
        spread[came + s] = expansion_row(k, cell)
        if 0 <= cell < W[k]:
            keep[came + s, cell] = 1
    return spread, keep


def arrival_table(k):
    spread = np.zeros((128, 2 * W[k]))
    keep = np.zeros((128, W[k]))
    for part in range(3):
        for s, cell in enumerate((-1, 0, 1, W[k] - 1, W[k])):
            lane = 24 * (k - 1) + 8 * part + s
            spread[lane] = expansion_row(k, cell)
            if 0 <= cell < W[k]:
                keep[lane, cell] = 1
    return spread, keep


def padded(a, cols):
    return np.pad(a, ((0, 0), (0, cols - a.shape[1])))


def tables():
    (plain, cells), (low, cells_low), (high, cells_high) = (
        reduction_table(*e) for e in ((False, False), (True, False), (False, True))
    )
    assert np.array_equal(plain[128:], low[128:]) and np.array_equal(plain[:384], high[:384])
    assert np.array_equal(plain[:, 0:384], np.asarray(plain[:, 0:384].astype(jnp.bfloat16), np.float64))
    t_low = np.stack([plain[:128], low[:128]])
    t_high = np.stack([plain[384:], high[384:]])
    c_low = np.stack([cells[:128], cells_low[:128]])
    c_high = np.stack([cells[384:], cells_high[384:]])
    v1, s1 = expansion_table(1, 0, 256, 384)
    w2 = np.concatenate(expansion_table(2, 128, 0, 256), axis=1)
    deep = []
    for k in (3, 4, 5):
        spread, keep = expansion_table(k, 128 + POS[k], 0, 256)
        deep.append(np.concatenate([padded(spread, 128), padded(keep, 128)], axis=1))
    spread, keep = arrival_table(1)
    assert not spread[:, 128:384].any()
    arrive = [spread[:, :128], spread[:, 384:], keep]
    arrive += arrival_table(2)
    for k in (3, 4, 5):
        arrive += [padded(a, 128) for a in arrival_table(k)]
    parts = (c_low, c_high, t_low, plain[128:384], t_high, v1, s1[256:], w2, np.stack(deep), np.concatenate(arrive, axis=1))
    return [a.astype(jnp.bfloat16) for a in parts]


def split3(a):
    top = a.astype(BF16)
    rest = a - top.astype(F32)
    mid = rest.astype(BF16)
    return top, mid, (rest - mid.astype(F32)).astype(BF16)


def dot3(a, table):
    m = a.shape[0]
    p = jnp.dot(jnp.concatenate(split3(a), axis=0), table, preferred_element_type=F32)
    return p[0:m] + p[m : 2 * m] + p[2 * m : 3 * m]


BELOW = [None, (18, 26, 34, 42, 50, 58), (10, 18, 26), (6, 14), (4,), (3,)]
ABOVE = [None, (-1, 7, 15), (-1, 7), (-1,), (-1,), (-1,)]


def reduce_rows(t, src, dst, starts):
    for ch in range(CH):
        for j in starts:

            def tap(o):
                return src[ch, t, pl.ds(8 + 2 * j + o, 8, stride=2), :]

            dst[ch, t, 8 + j : 16 + j, :] = (tap(-2) + tap(2)) + (tap(-1) + tap(1)) * 4.0 + tap(0) * 6.0


def mirror_start(a, first):
    for t in range(4):
        a[:, t, 7:8, :] = a[:, t, pl.ds(jnp.where(first, 9, 7), 1), :]
        a[:, t, 6:7, :] = a[:, t, pl.ds(jnp.where(first, 10, 6), 1), :]


def mirror_end(a, tiles, h, last):
    for t in tiles:
        a[:, t, 8 + h : 9 + h, :] = a[:, t, pl.ds(jnp.where(last, 6 + h, 8 + h), 1), :]


def rows_of(k, y, tiles):
    return jnp.concatenate(
        [jnp.concatenate([y[c, t, 7 : 7 + R[k], :] for t in tiles], axis=1) for c in range(CH)], axis=0
    )


def detail(g, level, at, out, count):
    lo, mid, hi = (g[:, :, i : i + count, :] for i in range(3))
    even, odd = pl.ds(at, count, stride=2), pl.ds(at + 1, count, stride=2)
    out[:, :, pl.ds(0, count, stride=2), :] = level[:, :, even, :] - ((lo + hi) * 0.125 + mid * 0.75)
    out[:, :, pl.ds(1, count, stride=2), :] = level[:, :, odd, :] - (mid + hi) * 0.5


def exchange_kernel(
    x_hbm, clow_hbm, chigh_hbm, tlow_hbm, tmid_hbm, thigh_hbm, v1_hbm, s1_hbm, w2_hbm, w345_hbm, arrive_hbm,
    d0, d1, d2, d3, d4, d5,
    xs, y1, y2, y3, y4, y5, tc, co, tv, v1, s1, w2, w345, arrive, srs, ci, beside,
    rh, rl, kh, kl, cb, rh_in, rl_in, cbm, cbp, chm, chp, clm, clp,
    g1, g2, g3, g4, g5, m1, m2, m3, m4, m5, d3w, d4w,
    load_sem, send_sem, recv_sem,
):
    r, c = lax.axis_index("rows"), lax.axis_index("cols")
    nr, nc = lax.axis_size("rows"), lax.axis_size("cols")
    first, last = r == 0, r == nr - 1
    left, right = c == 0, c == nc - 1
    up, down = jnp.logical_not(first), jnp.logical_not(last)
    west, east = jnp.logical_not(left), jnp.logical_not(right)

    def image(at, rows, sem):
        return [
            pltpu.make_async_copy(
                x_hbm.at[:, pl.ds(at, rows), pl.ds(128 * t, 128)], xs.at[:, t, pl.ds(8 + at, rows), :], load_sem.at[sem + t]
            )
            for t in range(4)
        ]

    lower = image(32, ROWS - 32, 0)
    upper = image(0, 32, 4)
    at_left, at_right = left.astype(jnp.int32), right.astype(jnp.int32)
    cell_tables = [
        pltpu.make_async_copy(clow_hbm.at[at_left], tc.at[pl.ds(0, 128)], load_sem.at[8]),
        pltpu.make_async_copy(chigh_hbm.at[at_right], tc.at[pl.ds(128, 128)], load_sem.at[9]),
    ]
    row_tables = [
        pltpu.make_async_copy(tlow_hbm.at[at_left], tv.at[pl.ds(0, 128)], load_sem.at[10]),
        pltpu.make_async_copy(tmid_hbm, tv.at[pl.ds(128, 256)], load_sem.at[11]),
        pltpu.make_async_copy(thigh_hbm.at[at_right], tv.at[pl.ds(384, 128)], load_sem.at[12]),
    ]
    own_tables = [
        pltpu.make_async_copy(v1_hbm, v1, load_sem.at[13]),
        pltpu.make_async_copy(s1_hbm, s1, load_sem.at[14]),
        pltpu.make_async_copy(w2_hbm, w2, load_sem.at[15]),
        pltpu.make_async_copy(w345_hbm, w345, load_sem.at[16]),
        pltpu.make_async_copy(arrive_hbm, arrive, load_sem.at[17]),
    ]
    for copy in (lower[0], lower[3], *cell_tables, lower[1], lower[2], *row_tables):
        copy.start()

    def there(dr, dc):
        ok = jnp.bool_(True)
        if dr:
            ok = jnp.logical_and(ok, up if dr < 0 else down)
        if dc:
            ok = jnp.logical_and(ok, west if dc < 0 else east)
        return ok

    messages = [
        (rh, rh_in, 1, 0),
        (kh, chm, 1, 1),
        (kh, chp, 1, -1),
        (rl, rl_in, -1, 0),
        (kl, clm, -1, 1),
        (kl, clp, -1, -1),
        (cb, cbm, 0, 1),
        (cb, cbp, 0, -1),
    ]
    barrier = pltpu.get_barrier_semaphore()
    for _, dst, dr, dc in messages:

        @pl.when(there(dr, dc))
        def _(dr=dr, dc=dc):
            pl.semaphore_signal(barrier, inc=1, device_id=(r + dr, c + dc), device_id_type=MESH)

        @pl.when(jnp.logical_not(there(-dr, -dc)))
        def _(dst=dst):
            dst[...] = jnp.zeros_like(dst)

    for copy in upper:
        copy.start()

    ys = (xs, y1, y2, y3, y4, y5)
    for k in range(LEVELS):
        ys[k][:, :, 0:8, :] = jnp.zeros((CH, 4, 8, 128), F32)
        ys[k][:, :, 8 + H[k] : 32 + H[k], :] = jnp.zeros((CH, 4, 24, 128), F32)
    srs[...] = jnp.zeros_like(srs)
    ci[...] = jnp.zeros_like(ci)
    for a in (rh, kh, kl):
        a[...] = jnp.zeros_like(a)

    lane = lax.broadcasted_iota(jnp.int32, (16, 128), 1)

    def reduce_lower(tiles):
        for k in range(1, LEVELS + 1):
            mirror_end(ys[k - 1], tiles, H[k - 1], last)
            for t in tiles:
                reduce_rows(t, ys[k - 1], ys[k], BELOW[k])
            for ch in range(CH):
                at = 16 * (k - 1) + 3 * ch
                for t in tiles:
                    srs[t, at : at + 3, :] = ys[k][ch, t, 7 + H[k] : 10 + H[k], :]

    def form_corners(corners, count):
        both = dot3(jnp.concatenate([srs[0], srs[3]], axis=1), tc[...])
        both = both[:, 0:128] + both[:, 128:256]
        level = [both[16 * k : 16 * k + 16] for k in range(LEVELS)]
        cells, halo = level[4], level[4]
        for k in (3, 2, 1, 0):
            cells = jnp.where(lane < 8 * k + 8, level[k], cells)
            halo = jnp.where(lane < 114 + 2 * k, level[k], halo)
        beside[...] = halo
        ci[...] = jnp.where(lane < 40, cells, 0.0)
        corners[0:3, :] = sum(pltpu.roll(ci[pl.ds(i, CH, stride=count), :], 40 * i, 1) for i in range(count))

    def form_strips(out, count):
        strips = jnp.concatenate([srs[t] for t in range(4)], axis=1)
        near = dot3(strips[0:32], tv[:, 0:384])
        deep = dot3(strips[32:80], tv[:, 384:640])
        deep = deep[:, 0:128] + deep[:, 128:256]
        small = jnp.where(lane < 96, deep[16:32], deep[32:48])
        small = jnp.where(lane < 64, deep[0:16], jnp.where(lane < 112, small, beside[...]))
        for t, a in enumerate((near[0:16, 0:128], near[0:16, 128:256], near[16:32, 256:384], small)):
            out[pl.ds(t, CH * count, stride=4), :] = a[0 : CH * count]

    for copy in (lower[0], lower[3]):
        copy.wait()
    reduce_lower((0, 3))
    for copy in cell_tables:
        copy.wait()
    form_corners(kh, 3)

    place = lax.broadcasted_iota(jnp.int32, (8, 512), 1)

    def of_level(k, a):
        ok = place < (BASE[k + 1] if k < LEVELS else 480)
        return jnp.where(jnp.logical_and(ok, place >= BASE[k]), a, 0.0)

    def put(k, a, out):
        for ch in range(CH):
            for t in range(out.shape[1]):
                out[ch, t] = a[R[k] * ch : R[k] * (ch + 1), 128 * t : 128 * (t + 1)]

    deeper = ((3, 0, g3, m3), (4, 72, g4, m4), (5, 112, g5, m5))

    def reduce_rest():
        for copy in upper:
            copy.wait()
        for k in range(1, LEVELS + 1):
            mirror_start(ys[k - 1], first)
            for t in range(4):
                reduce_rows(t, ys[k - 1], ys[k], ABOVE[k])
        mirror_start(y5, first)
        for k in range(1, LEVELS + 1):
            for ch in range(CH):
                at = 16 * (k - 1) + 2 * ch
                srs[:, at : at + 2, :] = ys[k][ch, :, 7:9, :]
        form_corners(kl, 2)
        form_strips(rl, 2)
        outer = jnp.concatenate([rows_of(k, ys[k], (0, 3)) for k in range(1, LEVELS + 1)], axis=0)
        cells = dot3(outer, tc[...])
        cells = cells[:, 0:128] + cells[:, 128:256]
        co[...] = cells
        turned = jnp.concatenate([cells, jnp.zeros((32, 128), F32)], axis=0)
        turned = jnp.transpose(turned)
        cb[...] = sum(of_level(k, turned[8 * (k - 1) : 8 * k]) for k in range(1, LEVELS + 1))

    def expand_own():
        for copy in own_tables:
            copy.start()
        p12 = dot3(jnp.concatenate([rows_of(k, ys[k], range(4)) for k in (1, 2)], axis=0), tv[:, 0:384])
        p345 = dot3(jnp.concatenate([rows_of(k, ys[k], range(4)) for k in (3, 4, 5)], axis=0), tv[:, 384:640])
        p345 = p345[:, 0:128] + p345[:, 128:256]
        cells = co[...]
        for copy in own_tables:
            copy.wait()
        put(1, dot3(jnp.concatenate([p12[0:224, 0:256], cells[0:224]], axis=1), v1[...]), g1)
        put(1, p12, m1)
        both = dot3(jnp.concatenate([cells[208:336], p12[208:336, 256:384]], axis=1), w2[...])
        put(2, both[8:, 0:256], g2)
        put(2, both[8:, 256:384], m2)
        for k, at, g, m in deeper:
            rows = 16 * -(-3 * R[k] // 16)
            both = dot3(jnp.concatenate([cells[336 + at : 336 + at + rows], p345[at : at + rows]], axis=1), w345[k - 3])
            skip = BASE[k] - BASE[3] - at
            put(k, both[skip:, 0:128], g)
            put(k, both[skip:, 128:256], m)

    z = lax.rem(r, 8)
    early, earliest = z < 4, z == 0

    def finish_lower():
        for copy in (lower[1], lower[2]):
            copy.wait()
        reduce_lower((1, 2))
        for copy in row_tables:
            copy.wait()
        form_strips(rh, 3)

    @pl.when(early)
    def _():
        finish_lower()
        reduce_rest()

    pl.when(earliest)(expand_own)

    neighbours = (up.astype(jnp.int32) + down.astype(jnp.int32) + 1) * (
        west.astype(jnp.int32) + east.astype(jnp.int32) + 1
    ) - 1
    pl.semaphore_wait(barrier, neighbours)
    copies = []
    for m, (src, dst, dr, dc) in enumerate(messages):
        copies.append(
            pltpu.make_async_remote_copy(
                src_ref=src, dst_ref=dst, send_sem=send_sem.at[m], recv_sem=recv_sem.at[m],
                device_id=(r + dr, c + dc), device_id_type=MESH,
            )
        )
    for m in (1, 2):
        pl.when(there(*messages[m][2:]))(copies[m].start)
    pl.when(jnp.logical_not(early))(finish_lower)
    pl.when(there(1, 0))(copies[0].start)


    @pl.when(jnp.logical_not(early))
    def _():
        reduce_rest()

    for m in range(3, 8):
        pl.when(there(*messages[m][2:]))(copies[m].start)
    pl.when(jnp.logical_not(earliest))(expand_own)

    def add(k, a, out, tiles, first_tile=0):
        for ch in range(CH):
            for i, t in enumerate(tiles):
                lanes = 128 * (first_tile + i)
                out[ch, t] += a[R[k] * ch : R[k] * (ch + 1), lanes : lanes + 128]

    side = jnp.bitwise_and(lane, 7) < 3
    middle = jnp.logical_and(lane >= 64, lane < 104)
    ci[...] = jnp.zeros_like(ci)

    def add_rows(strip, minus, plus, count, row_of):
        corner = jnp.where(side[0:4], minus[...], plus[...])
        for i in range(count):
            ci[pl.ds(i, CH, stride=count), :] = pltpu.roll(corner, (64 - 40 * i) % 128, 1)[0:CH]
        rows = CH * count
        fill = jnp.zeros((16 - rows, 128), F32)
        tiles = [jnp.concatenate([strip[pl.ds(t, rows, stride=4), :], fill], axis=0) for t in range(4)]
        cells = jnp.where(lane < 112, jnp.where(middle, ci[...], 0.0), tiles[3])
        wide = dot3(jnp.concatenate([tiles[0], tiles[1], cells], axis=1), v1[...])
        level = jnp.concatenate(tiles[0:2], axis=1) + dot3(cells, s1[...])
        both = [dot3(jnp.concatenate([cells, tiles[2]], axis=1), w2[...])]
        tail = jnp.concatenate([cells, tiles[3]], axis=1)
        both += [dot3(tail, w345[k - 3]) for k in (3, 4, 5)]
        pairs = [(1, wide, g1), (1, level, m1), (2, both[0][:, 0:256], g2), (2, both[0][:, 256:384], m2)]
        for (k, _, g, m), a in zip(deeper, both[1:]):
            pairs += [(k, a[:, 0:128], g), (k, a[:, 128:256], m)]
        for k, a, out in pairs:
            at = row_of(k) + 1
            for ch in range(CH):
                for t in range(out.shape[1]):
                    out[ch, t, at : at + count, :] += a[count * ch : count * (ch + 1), 128 * t : 128 * (t + 1)]

    def details(counts):
        for g, level, at, out, count in zip((g1, g2, g3, g4, g5), (xs, m1, m2, m3, m4), (8, 1, 1, 1, 1), (d0, d1, d2, d3w, d4w), counts):
            detail(g, level, at, out, count)
        d3[...] = d3w[:, 0, :, 0:64]
        d4[...] = d4w[:, 0, :, 0:32]
        d5[...] = m5[:, 0, 1:5, 0:16]

    for m in (3, 4, 5):
        pl.when(there(-messages[m][2], -messages[m][3]))(copies[m].wait_recv)
    add_rows(rl_in, clm, clp, 2, lambda k: H[k] - 1)
    for m in (6, 7):
        pl.when(there(-messages[m][2], -messages[m][3]))(copies[m].wait_recv)
    sub = lax.broadcasted_iota(jnp.int32, (8, 512), 0)
    terms = [a.astype(F32) for a in split3(jnp.where(sub < 3, cbm[...], cbp[...]))]
    came = jnp.concatenate(
        [of_level(k, a) for k in range(1, LEVELS + 1) for a in terms] + [jnp.zeros((8, 512), F32)], axis=0
    )
    came = jnp.transpose(came)

    def arrived(k, at, rows, lanes, count):
        return jnp.dot(
            came[at : at + rows].astype(BF16), arrive[:, lanes : lanes + count], preferred_element_type=F32
        )[BASE[k] - at :]

    more = arrived(1, 0, 224, 0, 512)
    add(1, more, g1, (0, 3))
    add(1, more, m1, (0, 1), 2)
    more = arrived(2, 208, 128, 512, 384)
    add(2, more, g2, (0, 1))
    add(2, more, m2, (0,), 2)
    for k, at, g, m in deeper:
        more = arrived(k, BASE[3] + at, 16 * -(-3 * R[k] // 16), 896 + 256 * (k - 3), 256)
        add(k, more, g, (0,))
        add(k, more, m, (0,), 1)

    for k, g in enumerate((g1, g2, g3, g4, g5), 1):
        g[:, :, H[k] + 1 : H[k] + 2, :] = g[:, :, pl.ds(jnp.where(last, H[k], H[k] + 1), 1), :]
    details(H[1:6])
    for m in range(3):
        pl.when(there(-messages[m][2], -messages[m][3]))(copies[m].wait_recv)
    add_rows(rh_in, chm, chp, 3, lambda k: -1)
    details((4,) * 5)
    for copy, (_, _, dr, dc) in zip(copies, messages):
        pl.when(there(dr, dc))(copy.wait_send)


def result_kernel(d0, d1, d2, d3, d4, d5, o0, o1, o2, o3, o4, o5, sem):
    pairs = [(d0.at[:, t], o0.at[:, :, pl.ds(128 * t, 128)]) for t in range(4)]
    pairs += [(d1.at[:, t], o1.at[:, :, pl.ds(128 * t, 128)]) for t in range(2)]
    pairs += [(d2.at[:, 0], o2), (d3, o3), (d4, o4), (d5, o5)]
    copies = [pltpu.make_async_copy(src, dst, sem.at[i]) for i, (src, dst) in enumerate(pairs)]
    for copy in copies:
        copy.start()
    for copy in copies:
        copy.wait()


def body(orthophoto):
    def vmem(*shape, dtype=F32):
        return pltpu.VMEM(shape, dtype)

    held = [(CH, 4, H[0], 128), (CH, 2, H[1], 128), (CH, 1, H[2], 128)]
    held += [(CH, H[3], W[3]), (CH, H[4], W[4]), (CH, H[5], W[5])]
    scratch = [vmem(CH, 4, H[k] + 32, 128) for k in range(6)]
    scratch += [vmem(256, 256, dtype=BF16), vmem(480, 128)]
    scratch += [vmem(512, 640, dtype=BF16), vmem(384, 512, dtype=BF16), vmem(128, 256, dtype=BF16)]
    scratch += [vmem(256, 384, dtype=BF16), vmem(3, 256, 256, dtype=BF16), vmem(128, 1664, dtype=BF16)]
    scratch += [vmem(4, 80, 128), vmem(16, 128), vmem(16, 128)]
    scratch += [vmem(40, 128), vmem(24, 128), vmem(4, 128), vmem(4, 128), vmem(8, 512)]
    scratch += [vmem(40, 128), vmem(24, 128), vmem(8, 512), vmem(8, 512)]
    scratch += [vmem(4, 128)] * 4
    scratch += [vmem(CH, t, R[k], 128) for k, t in ((1, 4), (2, 2), (3, 1), (4, 1), (5, 1))]
    scratch += [vmem(CH, t, R[k], 128) for k, t in ((1, 2), (2, 1), (3, 1), (4, 1), (5, 1))]
    scratch += [vmem(CH, 1, H[3], 128), vmem(CH, 1, H[4], 128)]
    scratch += [pltpu.SemaphoreType.DMA((n,)) for n in (18, 8, 8)]
    far = pl.BlockSpec(memory_space=pltpu.HBM)
    inside = pl.BlockSpec(memory_space=pltpu.VMEM)
    inputs = [pltpu.with_memory_space_constraint(jnp.asarray(a), pltpu.HBM) for a in (orthophoto, *tables())]
    arrays = pl.pallas_call(
        exchange_kernel,
        out_shape=[jax.ShapeDtypeStruct(shape, F32) for shape in held],
        in_specs=[far] * len(inputs),
        out_specs=[inside] * len(held),
        scratch_shapes=scratch,
        compiler_params=pltpu.CompilerParams(collective_id=0, has_side_effects=True, vmem_limit_bytes=24 << 20),
    )(*inputs)
    results = pl.pallas_call(
        result_kernel,
        out_shape=[jax.ShapeDtypeStruct((CH, H[k], W[k]), F32) for k in range(6)],
        in_specs=[inside] * len(held),
        out_specs=[far] * 6,
        scratch_shapes=[pltpu.SemaphoreType.DMA((10,))],
        compiler_params=pltpu.CompilerParams(vmem_limit_bytes=8 << 20),
    )(*arrays)
    return tuple(results)


def solution(mesh):
    placed = P(None, "rows", "cols")
    return jax.shard_map(body, mesh=mesh, in_specs=(placed,), out_specs=(placed,) * 6, check_vma=False)
```

```python
import functools

import jax
import jax.numpy as jnp
import numpy as np
from jax import lax
from jax.experimental import pallas as pl
from jax.experimental.pallas import tpu as pltpu
from jax.sharding import PartitionSpec as P

CH = 3
ROWS = 128
COLS = 512
LEVELS = 5
H = [ROWS >> k for k in range(6)]
W = [COLS >> k for k in range(6)]
R = [0, 72, 40, 24, 16, 8]
BASE = [0, 0, 216, 336, 408, 456]
POS = [0, 0, 0, 0, 64, 96]
F32 = jnp.float32
BF16 = jnp.bfloat16
MESH = pl.DeviceIdType.MESH
TAPS = (1.0, 4.0, 6.0, 4.0, 1.0)


def column_reductions(low, high):
    result = [None]
    total = None
    for k in range(1, LEVELS + 1):
        n = W[k - 1]
        step = np.zeros((n + 3, W[k] + 3))
        for j in range(0 if low else -1, W[k] if high else W[k] + 2):
            for tap in range(5):
                cell = 2 * j - 2 + tap
                if low and cell < 0:
                    cell = -cell
                if high and cell > n - 1:
                    cell = 2 * (n - 1) - cell
                if -1 <= cell <= n + 1:
                    step[cell + 1, j + 1] += TAPS[tap] / 16
        total = step[1 : n + 1] if k == 1 else total @ step
        result.append(total / 16.0**k)
    return result


def reduction_table(low, high):
    t = column_reductions(low, high)

    def fill(a, at, k):
        beyond, before = W[k] - 1 if high else W[k], 1 if low else -1
        cells = (W[k] - 1, beyond, W[k] + 1, before, 0)
        a[:, at + 8 * (k - 1) : at + 8 * (k - 1) + 5] = t[k][:, [c + 1 for c in cells]]
        a[:, at + 112 + 2 * (k - 1) : at + 114 + 2 * (k - 1)] = t[k][:, [beyond + 1, before + 1]]

    near = np.zeros((COLS, 384))
    near[:, 0:256] = t[1][:, 1:257]
    near[:, 256:384] = t[2][:, 1:129]
    deep, cells = np.zeros((COLS, 128)), np.zeros((COLS, 128))
    for k in range(1, LEVELS + 1):
        fill(cells, 0, k)
        if k > 2:
            deep[:, POS[k] : POS[k] + W[k]] = t[k][:, 1 : W[k] + 1]
    assert not cells[128:384].any()
    return np.concatenate([near, *two_terms(deep)], axis=1), np.concatenate(two_terms(cells), axis=1)


def two_terms(a):
    top = np.asarray(a.astype(jnp.bfloat16), np.float64)
    rest = np.asarray((a - top).astype(jnp.bfloat16), np.float64)
    assert np.array_equal(top + rest, a)
    return top, rest


def expansion_row(k, cell):
    row = np.zeros(2 * W[k])
    for i in range(W[k]):
        row[2 * i] += {i - 1: 0.125, i: 0.75, i + 1: 0.125}.get(cell, 0.0)
        row[2 * i + 1] += {i: 0.5, i + 1: 0.5}.get(cell, 0.0)
    return row


def expansion_table(k, main_at, edge_at, lanes):
    spread = np.zeros((lanes, 2 * W[k]))
    keep = np.zeros((lanes, W[k]))
    for c in range(W[k]):
        spread[main_at + c] = expansion_row(k, c)
        keep[main_at + c, c] = 1
    own = edge_at + 112 + 2 * (k - 1)
    came = edge_at + 64 + 8 * (k - 1)
    spread[own] = expansion_row(k, W[k])
    spread[own + 1] = expansion_row(k, -1)
    for s, cell in enumerate((-1, 0, 1, W[k] - 1, W[k])):
        spread[came + s] = expansion_row(k, cell)
        if 0 <= cell < W[k]:
            keep[came + s, cell] = 1
    return spread, keep


def arrival_table(k):
    spread = np.zeros((128, 2 * W[k]))
    keep = np.zeros((128, W[k]))
    for part in range(3):
        for s, cell in enumerate((-1, 0, 1, W[k] - 1, W[k])):
            lane = 24 * (k - 1) + 8 * part + s
            spread[lane] = expansion_row(k, cell)
            if 0 <= cell < W[k]:
                keep[lane, cell] = 1
    return spread, keep


def padded(a, cols):
    return np.pad(a, ((0, 0), (0, cols - a.shape[1])))


def tables():
    (plain, cells), (low, cells_low), (high, cells_high) = (
        reduction_table(*e) for e in ((False, False), (True, False), (False, True))
    )
    assert np.array_equal(plain[128:], low[128:]) and np.array_equal(plain[:384], high[:384])
    assert np.array_equal(plain[:, 0:384], np.asarray(plain[:, 0:384].astype(jnp.bfloat16), np.float64))
    t_low = np.stack([plain[:128], low[:128]])
    t_high = np.stack([plain[384:], high[384:]])
    c_low = np.stack([cells[:128], cells_low[:128]])
    c_high = np.stack([cells[384:], cells_high[384:]])
    v1, s1 = expansion_table(1, 0, 256, 384)
    w2 = np.concatenate(expansion_table(2, 128, 0, 256), axis=1)
    deep = []
    for k in (3, 4, 5):
        spread, keep = expansion_table(k, 128 + POS[k], 0, 256)
        deep.append(np.concatenate([padded(spread, 128), padded(keep, 128)], axis=1))
    spread, keep = arrival_table(1)
    assert not spread[:, 128:384].any()
    arrive = [spread[:, :128], spread[:, 384:], keep]
    arrive += arrival_table(2)
    for k in (3, 4, 5):
        arrive += [padded(a, 128) for a in arrival_table(k)]
    parts = (c_low, c_high, t_low, plain[128:384], t_high, v1, s1[256:], w2, np.stack(deep), np.concatenate(arrive, axis=1))
    return [a.astype(jnp.bfloat16) for a in parts]


def split3(a):
    top = a.astype(BF16)
    rest = a - top.astype(F32)
    mid = rest.astype(BF16)
    return top, mid, (rest - mid.astype(F32)).astype(BF16)


def dot3(a, table):
    m = a.shape[0]
    p = jnp.dot(jnp.concatenate(split3(a), axis=0), table, preferred_element_type=F32)
    return p[0:m] + p[m : 2 * m] + p[2 * m : 3 * m]


BELOW = [None, (18, 26, 34, 42, 50, 58), (10, 18, 26), (6, 14), (4,), (3,)]
ABOVE = [None, (-1, 7, 15), (-1, 7), (-1,), (-1,), (-1,)]


def reduce_rows(t, src, dst, starts):
    for ch in range(CH):
        for j in starts:

            def tap(o):
                return src[ch, t, pl.ds(8 + 2 * j + o, 8, stride=2), :]

            dst[ch, t, 8 + j : 16 + j, :] = (tap(-2) + tap(2)) + (tap(-1) + tap(1)) * 4.0 + tap(0) * 6.0


def mirror_start(a, first):
    for t in range(4):
        a[:, t, 7:8, :] = a[:, t, pl.ds(jnp.where(first, 9, 7), 1), :]
        a[:, t, 6:7, :] = a[:, t, pl.ds(jnp.where(first, 10, 6), 1), :]


def mirror_end(a, tiles, h, last):
    for t in tiles:
        a[:, t, 8 + h : 9 + h, :] = a[:, t, pl.ds(jnp.where(last, 6 + h, 8 + h), 1), :]


def rows_of(k, y, tiles):
    return jnp.concatenate(
        [jnp.concatenate([y[c, t, 7 : 7 + R[k], :] for t in tiles], axis=1) for c in range(CH)], axis=0
    )


def detail(g, level, at, out, count):
    lo, mid, hi = (g[:, :, i : i + count, :] for i in range(3))
    even, odd = pl.ds(at, count, stride=2), pl.ds(at + 1, count, stride=2)
    out[:, :, pl.ds(0, count, stride=2), :] = level[:, :, even, :] - ((lo + hi) * 0.125 + mid * 0.75)
    out[:, :, pl.ds(1, count, stride=2), :] = level[:, :, odd, :] - (mid + hi) * 0.5


def exchange_kernel(
    x_hbm, clow_hbm, chigh_hbm, tlow_hbm, tmid_hbm, thigh_hbm, v1_hbm, s1_hbm, w2_hbm, w345_hbm, arrive_hbm,
    d0, d1, d2, d3, d4, d5,
    xs, y1, y2, y3, y4, y5, tc, co, tv, v1, s1, w2, w345, arrive, srs, ci, beside,
    rh, rl, kh, kl, cb, rh_in, rl_in, cbm, cbp, chm, chp, clm, clp,
    g1, g2, g3, g4, g5, m1, m2, m3, m4, m5, d3w, d4w,
    load_sem, send_sem, recv_sem,
):
    r, c = lax.axis_index("rows"), lax.axis_index("cols")
    nr, nc = lax.axis_size("rows"), lax.axis_size("cols")
    first, last = r == 0, r == nr - 1
    left, right = c == 0, c == nc - 1
    up, down = jnp.logical_not(first), jnp.logical_not(last)
    west, east = jnp.logical_not(left), jnp.logical_not(right)

    def image(at, rows, sem):
        return [
            pltpu.make_async_copy(
                x_hbm.at[:, pl.ds(at, rows), pl.ds(128 * t, 128)], xs.at[:, t, pl.ds(8 + at, rows), :], load_sem.at[sem + t]
            )
            for t in range(4)
        ]

    lower = image(32, ROWS - 32, 0)
    upper = image(0, 32, 4)
    at_left, at_right = left.astype(jnp.int32), right.astype(jnp.int32)
    cell_tables = [
        pltpu.make_async_copy(clow_hbm.at[at_left], tc.at[pl.ds(0, 128)], load_sem.at[8]),
        pltpu.make_async_copy(chigh_hbm.at[at_right], tc.at[pl.ds(128, 128)], load_sem.at[9]),
    ]
    row_tables = [
        pltpu.make_async_copy(tlow_hbm.at[at_left], tv.at[pl.ds(0, 128)], load_sem.at[10]),
        pltpu.make_async_copy(tmid_hbm, tv.at[pl.ds(128, 256)], load_sem.at[11]),
        pltpu.make_async_copy(thigh_hbm.at[at_right], tv.at[pl.ds(384, 128)], load_sem.at[12]),
    ]
    own_tables = [
        pltpu.make_async_copy(v1_hbm, v1, load_sem.at[13]),
        pltpu.make_async_copy(s1_hbm, s1, load_sem.at[14]),
        pltpu.make_async_copy(w2_hbm, w2, load_sem.at[15]),
        pltpu.make_async_copy(w345_hbm, w345, load_sem.at[16]),
        pltpu.make_async_copy(arrive_hbm, arrive, load_sem.at[17]),
    ]
    for copy in (*lower, *cell_tables, *row_tables):
        copy.start()

    def there(dr, dc):
        ok = jnp.bool_(True)
        if dr:
            ok = jnp.logical_and(ok, up if dr < 0 else down)
        if dc:
            ok = jnp.logical_and(ok, west if dc < 0 else east)
        return ok

    messages = [
        (rh, rh_in, 1, 0),
        (kh, chm, 1, 1),
        (kh, chp, 1, -1),
        (rl, rl_in, -1, 0),
        (kl, clm, -1, 1),
        (kl, clp, -1, -1),
        (cb, cbm, 0, 1),
        (cb, cbp, 0, -1),
    ]
    barrier = pltpu.get_barrier_semaphore()
    for _, dst, dr, dc in messages:

        @pl.when(there(dr, dc))
        def _(dr=dr, dc=dc):
            pl.semaphore_signal(barrier, inc=1, device_id=(r + dr, c + dc), device_id_type=MESH)

        @pl.when(jnp.logical_not(there(-dr, -dc)))
        def _(dst=dst):
            dst[...] = jnp.zeros_like(dst)

    for copy in upper:
        copy.start()

    ys = (xs, y1, y2, y3, y4, y5)
    for k in range(LEVELS):
        ys[k][:, :, 0:8, :] = jnp.zeros((CH, 4, 8, 128), F32)
        ys[k][:, :, 8 + H[k] : 32 + H[k], :] = jnp.zeros((CH, 4, 24, 128), F32)
    srs[...] = jnp.zeros_like(srs)
    ci[...] = jnp.zeros_like(ci)
    for a in (rh, kh, kl):
        a[...] = jnp.zeros_like(a)

    lane = lax.broadcasted_iota(jnp.int32, (16, 128), 1)

    def reduce_lower(tiles):
        for k in range(1, LEVELS + 1):
            if k == 3:
                for copy in cell_tables + row_tables:
                    copy.wait()
            mirror_end(ys[k - 1], tiles, H[k - 1], last)
            for t in tiles:
                reduce_rows(t, ys[k - 1], ys[k], BELOW[k])
            for ch in range(CH):
                at = 16 * (k - 1) + 3 * ch
                for t in tiles:
                    srs[t, at : at + 3, :] = ys[k][ch, t, 7 + H[k] : 10 + H[k], :]

    def form_corners(corners, count):
        both = dot3(jnp.concatenate([srs[0], srs[3]], axis=1), tc[...])
        both = both[:, 0:128] + both[:, 128:256]
        level = [both[16 * k : 16 * k + 16] for k in range(LEVELS)]
        cells, halo = level[4], level[4]
        for k in (3, 2, 1, 0):
            cells = jnp.where(lane < 8 * k + 8, level[k], cells)
            halo = jnp.where(lane < 114 + 2 * k, level[k], halo)
        beside[...] = halo
        ci[...] = jnp.where(lane < 40, cells, 0.0)
        corners[0:3, :] = sum(pltpu.roll(ci[pl.ds(i, CH, stride=count), :], 40 * i, 1) for i in range(count))

    def form_strips(out, count):
        strips = jnp.concatenate([srs[t] for t in range(4)], axis=1)
        near = dot3(strips[0:32], tv[:, 0:384])
        deep = dot3(strips[32:80], tv[:, 384:640])
        deep = deep[:, 0:128] + deep[:, 128:256]
        small = jnp.where(lane < 96, deep[16:32], deep[32:48])
        small = jnp.where(lane < 64, deep[0:16], jnp.where(lane < 112, small, beside[...]))
        for t, a in enumerate((near[0:16, 0:128], near[0:16, 128:256], near[16:32, 256:384], small)):
            out[pl.ds(t, CH * count, stride=4), :] = a[0 : CH * count]

    for copy in lower:
        copy.wait()
    reduce_lower(range(4))
    form_corners(kh, 3)
    form_strips(rh, 3)

    place = lax.broadcasted_iota(jnp.int32, (8, 512), 1)

    def of_level(k, a):
        ok = place < (BASE[k + 1] if k < LEVELS else 480)
        return jnp.where(jnp.logical_and(ok, place >= BASE[k]), a, 0.0)

    def put(k, a, out):
        for ch in range(CH):
            for t in range(out.shape[1]):
                out[ch, t] = a[R[k] * ch : R[k] * (ch + 1), 128 * t : 128 * (t + 1)]

    deeper = ((3, 0, g3, m3), (4, 72, g4, m4), (5, 112, g5, m5))

    def reduce_rest():
        for copy in upper:
            copy.wait()
        for k in range(1, LEVELS + 1):
            mirror_start(ys[k - 1], first)
            for t in range(4):
                reduce_rows(t, ys[k - 1], ys[k], ABOVE[k])
        mirror_start(y5, first)
        for k in range(1, LEVELS + 1):
            for ch in range(CH):
                at = 16 * (k - 1) + 2 * ch
                srs[:, at : at + 2, :] = ys[k][ch, :, 7:9, :]
        form_corners(kl, 2)
        form_strips(rl, 2)
        outer = jnp.concatenate([rows_of(k, ys[k], (0, 3)) for k in range(1, LEVELS + 1)], axis=0)
        cells = dot3(outer, tc[...])
        cells = cells[:, 0:128] + cells[:, 128:256]
        co[...] = cells
        turned = jnp.concatenate([cells, jnp.zeros((32, 128), F32)], axis=0)
        turned = jnp.transpose(turned)
        cb[...] = sum(of_level(k, turned[8 * (k - 1) : 8 * k]) for k in range(1, LEVELS + 1))

    def expand_own():
        for copy in own_tables:
            copy.start()
        p12 = dot3(jnp.concatenate([rows_of(k, ys[k], range(4)) for k in (1, 2)], axis=0), tv[:, 0:384])
        p345 = dot3(jnp.concatenate([rows_of(k, ys[k], range(4)) for k in (3, 4, 5)], axis=0), tv[:, 384:640])
        p345 = p345[:, 0:128] + p345[:, 128:256]
        cells = co[...]
        for copy in own_tables:
            copy.wait()
        put(1, dot3(jnp.concatenate([p12[0:224, 0:256], cells[0:224]], axis=1), v1[...]), g1)
        put(1, p12, m1)
        both = dot3(jnp.concatenate([cells[208:336], p12[208:336, 256:384]], axis=1), w2[...])
        put(2, both[8:, 0:256], g2)
        put(2, both[8:, 256:384], m2)
        for k, at, g, m in deeper:
            rows = 16 * -(-3 * R[k] // 16)
            both = dot3(jnp.concatenate([cells[336 + at : 336 + at + rows], p345[at : at + rows]], axis=1), w345[k - 3])
            skip = BASE[k] - BASE[3] - at
            put(k, both[skip:, 0:128], g)
            put(k, both[skip:, 128:256], m)

    z = lax.rem(r, 8)
    early, earliest = z < 4, z == 0

    pl.when(early)(reduce_rest)
    pl.when(earliest)(expand_own)

    neighbours = (up.astype(jnp.int32) + down.astype(jnp.int32) + 1) * (
        west.astype(jnp.int32) + east.astype(jnp.int32) + 1
    ) - 1
    pl.semaphore_wait(barrier, neighbours)
    copies = []
    for m, (src, dst, dr, dc) in enumerate(messages):
        copies.append(
            pltpu.make_async_remote_copy(
                src_ref=src, dst_ref=dst, send_sem=send_sem.at[m], recv_sem=recv_sem.at[m],
                device_id=(r + dr, c + dc), device_id_type=MESH,
            )
        )
    for m in (1, 2, 0):
        pl.when(there(*messages[m][2:]))(copies[m].start)


    @pl.when(jnp.logical_not(early))
    def _():
        reduce_rest()

    for m in range(3, 8):
        pl.when(there(*messages[m][2:]))(copies[m].start)
    pl.when(jnp.logical_not(earliest))(expand_own)

    def add(k, a, out, tiles, first_tile=0):
        for ch in range(CH):
            for i, t in enumerate(tiles):
                lanes = 128 * (first_tile + i)
                out[ch, t] += a[R[k] * ch : R[k] * (ch + 1), lanes : lanes + 128]

    side = jnp.bitwise_and(lane, 7) < 3
    middle = jnp.logical_and(lane >= 64, lane < 104)
    ci[...] = jnp.zeros_like(ci)

    def add_rows(strip, minus, plus, count, row_of):
        corner = jnp.where(side[0:4], minus[...], plus[...])
        for i in range(count):
            ci[pl.ds(i, CH, stride=count), :] = pltpu.roll(corner, (64 - 40 * i) % 128, 1)[0:CH]
        rows = CH * count
        fill = jnp.zeros((16 - rows, 128), F32)
        tiles = [jnp.concatenate([strip[pl.ds(t, rows, stride=4), :], fill], axis=0) for t in range(4)]
        cells = jnp.where(lane < 112, jnp.where(middle, ci[...], 0.0), tiles[3])
        wide = dot3(jnp.concatenate([tiles[0], tiles[1], cells], axis=1), v1[...])
        level = jnp.concatenate(tiles[0:2], axis=1) + dot3(cells, s1[...])
        both = [dot3(jnp.concatenate([cells, tiles[2]], axis=1), w2[...])]
        tail = jnp.concatenate([cells, tiles[3]], axis=1)
        both += [dot3(tail, w345[k - 3]) for k in (3, 4, 5)]
        pairs = [(1, wide, g1), (1, level, m1), (2, both[0][:, 0:256], g2), (2, both[0][:, 256:384], m2)]
        for (k, _, g, m), a in zip(deeper, both[1:]):
            pairs += [(k, a[:, 0:128], g), (k, a[:, 128:256], m)]
        for k, a, out in pairs:
            at = row_of(k) + 1
            for ch in range(CH):
                for t in range(out.shape[1]):
                    out[ch, t, at : at + count, :] += a[count * ch : count * (ch + 1), 128 * t : 128 * (t + 1)]

    def details(counts):
        for g, level, at, out, count in zip((g1, g2, g3, g4, g5), (xs, m1, m2, m3, m4), (8, 1, 1, 1, 1), (d0, d1, d2, d3w, d4w), counts):
            detail(g, level, at, out, count)
        d3[...] = d3w[:, 0, :, 0:64]
        d4[...] = d4w[:, 0, :, 0:32]
        d5[...] = m5[:, 0, 1:5, 0:16]

    for m in (3, 4, 5):
        pl.when(there(-messages[m][2], -messages[m][3]))(copies[m].wait_recv)
    add_rows(rl_in, clm, clp, 2, lambda k: H[k] - 1)
    for m in (6, 7):
        pl.when(there(-messages[m][2], -messages[m][3]))(copies[m].wait_recv)
    sub = lax.broadcasted_iota(jnp.int32, (8, 512), 0)
    terms = [a.astype(F32) for a in split3(jnp.where(sub < 3, cbm[...], cbp[...]))]
    came = jnp.concatenate(
        [of_level(k, a) for k in range(1, LEVELS + 1) for a in terms] + [jnp.zeros((8, 512), F32)], axis=0
    )
    came = jnp.transpose(came)

    def arrived(k, at, rows, lanes, count):
        return jnp.dot(
            came[at : at + rows].astype(BF16), arrive[:, lanes : lanes + count], preferred_element_type=F32
        )[BASE[k] - at :]

    more = arrived(1, 0, 224, 0, 512)
    add(1, more, g1, (0, 3))
    add(1, more, m1, (0, 1), 2)
    more = arrived(2, 208, 128, 512, 384)
    add(2, more, g2, (0, 1))
    add(2, more, m2, (0,), 2)
    for k, at, g, m in deeper:
        more = arrived(k, BASE[3] + at, 16 * -(-3 * R[k] // 16), 896 + 256 * (k - 3), 256)
        add(k, more, g, (0,))
        add(k, more, m, (0,), 1)

    for k, g in enumerate((g1, g2, g3, g4, g5), 1):
        g[:, :, H[k] + 1 : H[k] + 2, :] = g[:, :, pl.ds(jnp.where(last, H[k], H[k] + 1), 1), :]
    details(H[1:6])
    for m in range(3):
        pl.when(there(-messages[m][2], -messages[m][3]))(copies[m].wait_recv)
    add_rows(rh_in, chm, chp, 3, lambda k: -1)
    details((4,) * 5)
    for copy, (_, _, dr, dc) in zip(copies, messages):
        pl.when(there(dr, dc))(copy.wait_send)


def result_kernel(d0, d1, d2, d3, d4, d5, o0, o1, o2, o3, o4, o5, sem):
    pairs = [(d0.at[:, t], o0.at[:, :, pl.ds(128 * t, 128)]) for t in range(4)]
    pairs += [(d1.at[:, t], o1.at[:, :, pl.ds(128 * t, 128)]) for t in range(2)]
    pairs += [(d2.at[:, 0], o2), (d3, o3), (d4, o4), (d5, o5)]
    copies = [pltpu.make_async_copy(src, dst, sem.at[i]) for i, (src, dst) in enumerate(pairs)]
    for copy in copies:
        copy.start()
    for copy in copies:
        copy.wait()


def body(orthophoto):
    def vmem(*shape, dtype=F32):
        return pltpu.VMEM(shape, dtype)

    held = [(CH, 4, H[0], 128), (CH, 2, H[1], 128), (CH, 1, H[2], 128)]
    held += [(CH, H[3], W[3]), (CH, H[4], W[4]), (CH, H[5], W[5])]
    scratch = [vmem(CH, 4, H[k] + 32, 128) for k in range(6)]
    scratch += [vmem(256, 256, dtype=BF16), vmem(480, 128)]
    scratch += [vmem(512, 640, dtype=BF16), vmem(384, 512, dtype=BF16), vmem(128, 256, dtype=BF16)]
    scratch += [vmem(256, 384, dtype=BF16), vmem(3, 256, 256, dtype=BF16), vmem(128, 1664, dtype=BF16)]
    scratch += [vmem(4, 80, 128), vmem(16, 128), vmem(16, 128)]
    scratch += [vmem(40, 128), vmem(24, 128), vmem(4, 128), vmem(4, 128), vmem(8, 512)]
    scratch += [vmem(40, 128), vmem(24, 128), vmem(8, 512), vmem(8, 512)]
    scratch += [vmem(4, 128)] * 4
    scratch += [vmem(CH, t, R[k], 128) for k, t in ((1, 4), (2, 2), (3, 1), (4, 1), (5, 1))]
    scratch += [vmem(CH, t, R[k], 128) for k, t in ((1, 2), (2, 1), (3, 1), (4, 1), (5, 1))]
    scratch += [vmem(CH, 1, H[3], 128), vmem(CH, 1, H[4], 128)]
    scratch += [pltpu.SemaphoreType.DMA((n,)) for n in (18, 8, 8)]
    far = pl.BlockSpec(memory_space=pltpu.HBM)
    inside = pl.BlockSpec(memory_space=pltpu.VMEM)
    inputs = [pltpu.with_memory_space_constraint(jnp.asarray(a), pltpu.HBM) for a in (orthophoto, *tables())]
    arrays = pl.pallas_call(
        exchange_kernel,
        out_shape=[jax.ShapeDtypeStruct(shape, F32) for shape in held],
        in_specs=[far] * len(inputs),
        out_specs=[inside] * len(held),
        scratch_shapes=scratch,
        compiler_params=pltpu.CompilerParams(collective_id=0, has_side_effects=True, vmem_limit_bytes=24 << 20),
    )(*inputs)
    results = pl.pallas_call(
        result_kernel,
        out_shape=[jax.ShapeDtypeStruct((CH, H[k], W[k]), F32) for k in range(6)],
        in_specs=[inside] * len(held),
        out_specs=[far] * 6,
        scratch_shapes=[pltpu.SemaphoreType.DMA((10,))],
        compiler_params=pltpu.CompilerParams(vmem_limit_bytes=8 << 20),
    )(*arrays)
    return tuple(results)


def solution(mesh):
    placed = P(None, "rows", "cols")
    return jax.shard_map(body, mesh=mesh, in_specs=(placed,), out_specs=(placed,) * 6, check_vma=False)
```

```python
import functools

import jax
import jax.numpy as jnp
import numpy as np
from jax import lax
from jax.experimental import pallas as pl
from jax.experimental.pallas import tpu as pltpu
from jax.sharding import PartitionSpec as P

CH = 3
ROWS = 128
COLS = 512
LEVELS = 5
H = [ROWS >> k for k in range(6)]
W = [COLS >> k for k in range(6)]
R = [0, 72, 40, 24, 16, 8]
BASE = [0, 0, 216, 336, 408, 456]
POS = [0, 0, 0, 0, 64, 96]
F32 = jnp.float32
BF16 = jnp.bfloat16
MESH = pl.DeviceIdType.MESH
TAPS = (1.0, 4.0, 6.0, 4.0, 1.0)


def column_reductions(low, high):
    result = [None]
    total = None
    for k in range(1, LEVELS + 1):
        n = W[k - 1]
        step = np.zeros((n + 3, W[k] + 3))
        for j in range(0 if low else -1, W[k] if high else W[k] + 2):
            for tap in range(5):
                cell = 2 * j - 2 + tap
                if low and cell < 0:
                    cell = -cell
                if high and cell > n - 1:
                    cell = 2 * (n - 1) - cell
                if -1 <= cell <= n + 1:
                    step[cell + 1, j + 1] += TAPS[tap] / 16
        total = step[1 : n + 1] if k == 1 else total @ step
        result.append(total / 16.0**k)
    return result


def reduction_table(low, high):
    t = column_reductions(low, high)

    def fill(a, at, k):
        beyond, before = W[k] - 1 if high else W[k], 1 if low else -1
        cells = (W[k] - 1, beyond, W[k] + 1, before, 0)
        a[:, at + 8 * (k - 1) : at + 8 * (k - 1) + 5] = t[k][:, [c + 1 for c in cells]]
        a[:, at + 112 + 2 * (k - 1) : at + 114 + 2 * (k - 1)] = t[k][:, [beyond + 1, before + 1]]

    near = np.zeros((COLS, 384))
    near[:, 0:256] = t[1][:, 1:257]
    near[:, 256:384] = t[2][:, 1:129]
    deep, cells = np.zeros((COLS, 128)), np.zeros((COLS, 128))
    for k in range(1, LEVELS + 1):
        fill(cells, 0, k)
        if k > 2:
            deep[:, POS[k] : POS[k] + W[k]] = t[k][:, 1 : W[k] + 1]
    assert not cells[128:384].any()
    return np.concatenate([near, *two_terms(deep)], axis=1), np.concatenate(two_terms(cells), axis=1)


def two_terms(a):
    top = np.asarray(a.astype(jnp.bfloat16), np.float64)
    rest = np.asarray((a - top).astype(jnp.bfloat16), np.float64)
    assert np.array_equal(top + rest, a)
    return top, rest


def expansion_row(k, cell):
    row = np.zeros(2 * W[k])
    for i in range(W[k]):
        row[2 * i] += {i - 1: 0.125, i: 0.75, i + 1: 0.125}.get(cell, 0.0)
        row[2 * i + 1] += {i: 0.5, i + 1: 0.5}.get(cell, 0.0)
    return row


def expansion_table(k, main_at, edge_at, lanes):
    spread = np.zeros((lanes, 2 * W[k]))
    keep = np.zeros((lanes, W[k]))
    for c in range(W[k]):
        spread[main_at + c] = expansion_row(k, c)
        keep[main_at + c, c] = 1
    own = edge_at + 112 + 2 * (k - 1)
    came = edge_at + 64 + 8 * (k - 1)
    spread[own] = expansion_row(k, W[k])
    spread[own + 1] = expansion_row(k, -1)
    for s, cell in enumerate((-1, 0, 1, W[k] - 1, W[k])):
        spread[came + s] = expansion_row(k, cell)
        if 0 <= cell < W[k]:
            keep[came + s, cell] = 1
    return spread, keep


def arrival_table(k):
    spread = np.zeros((128, 2 * W[k]))
    keep = np.zeros((128, W[k]))
    for part in range(3):
        for s, cell in enumerate((-1, 0, 1, W[k] - 1, W[k])):
            lane = 24 * (k - 1) + 8 * part + s
            spread[lane] = expansion_row(k, cell)
            if 0 <= cell < W[k]:
                keep[lane, cell] = 1
    return spread, keep


def padded(a, cols):
    return np.pad(a, ((0, 0), (0, cols - a.shape[1])))


def tables():
    (plain, cells), (low, cells_low), (high, cells_high) = (
        reduction_table(*e) for e in ((False, False), (True, False), (False, True))
    )
    assert np.array_equal(plain[128:], low[128:]) and np.array_equal(plain[:384], high[:384])
    assert np.array_equal(plain[:, 0:384], np.asarray(plain[:, 0:384].astype(jnp.bfloat16), np.float64))
    t_low = np.stack([plain[:128], low[:128]])
    t_high = np.stack([plain[384:], high[384:]])
    c_low = np.stack([cells[:128], cells_low[:128]])
    c_high = np.stack([cells[384:], cells_high[384:]])
    v1, s1 = expansion_table(1, 0, 256, 384)
    w2 = np.concatenate(expansion_table(2, 128, 0, 256), axis=1)
    deep = []
    for k in (3, 4, 5):
        spread, keep = expansion_table(k, 128 + POS[k], 0, 256)
        deep.append(np.concatenate([padded(spread, 128), padded(keep, 128)], axis=1))
    spread, keep = arrival_table(1)
    assert not spread[:, 128:384].any()
    arrive = [spread[:, :128], spread[:, 384:], keep]
    arrive += arrival_table(2)
    for k in (3, 4, 5):
        arrive += [padded(a, 128) for a in arrival_table(k)]
    parts = (c_low, c_high, t_low, plain[128:384], t_high, v1, s1[256:], w2, np.stack(deep), np.concatenate(arrive, axis=1))
    return [a.astype(jnp.bfloat16) for a in parts]


def split3(a):
    top = a.astype(BF16)
    rest = a - top.astype(F32)
    mid = rest.astype(BF16)
    return top, mid, (rest - mid.astype(F32)).astype(BF16)


def dot3(a, table):
    m = a.shape[0]
    p = jnp.dot(jnp.concatenate(split3(a), axis=0), table, preferred_element_type=F32)
    return p[0:m] + p[m : 2 * m] + p[2 * m : 3 * m]


BELOW = [None, (18, 26, 34, 42, 50, 58), (10, 18, 26), (6, 14), (4,), (3,)]
ABOVE = [None, (-1, 7, 15), (-1, 7), (-1,), (-1,), (-1,)]


def reduce_rows(t, src, dst, starts):
    for ch in range(CH):
        for j in starts:

            def tap(o):
                return src[ch, t, pl.ds(8 + 2 * j + o, 8, stride=2), :]

            dst[ch, t, 8 + j : 16 + j, :] = (tap(-2) + tap(2)) + (tap(-1) + tap(1)) * 4.0 + tap(0) * 6.0


def mirror_start(a, first):
    for t in range(4):
        a[:, t, 7:8, :] = a[:, t, pl.ds(jnp.where(first, 9, 7), 1), :]
        a[:, t, 6:7, :] = a[:, t, pl.ds(jnp.where(first, 10, 6), 1), :]


def mirror_end(a, tiles, h, last):
    for t in tiles:
        a[:, t, 8 + h : 9 + h, :] = a[:, t, pl.ds(jnp.where(last, 6 + h, 8 + h), 1), :]


def rows_of(k, y, tiles):
    return jnp.concatenate(
        [jnp.concatenate([y[c, t, 7 : 7 + R[k], :] for t in tiles], axis=1) for c in range(CH)], axis=0
    )


def detail(g, level, at, out, count):
    lo, mid, hi = (g[:, :, i : i + count, :] for i in range(3))
    even, odd = pl.ds(at, count, stride=2), pl.ds(at + 1, count, stride=2)
    out[:, :, pl.ds(0, count, stride=2), :] = level[:, :, even, :] - ((lo + hi) * 0.125 + mid * 0.75)
    out[:, :, pl.ds(1, count, stride=2), :] = level[:, :, odd, :] - (mid + hi) * 0.5


def exchange_kernel(
    x_hbm, clow_hbm, chigh_hbm, tlow_hbm, tmid_hbm, thigh_hbm, v1_hbm, s1_hbm, w2_hbm, w345_hbm, arrive_hbm,
    d0, d1, d2, d3, d4, d5,
    xs, y1, y2, y3, y4, y5, tc, co, tv, v1, s1, w2, w345, arrive, srs, ci, beside,
    rh, rl, kh, kl, cb, rh_in, rl_in, cbm, cbp, chm, chp, clm, clp,
    g1, g2, g3, g4, g5, m1, m2, m3, m4, m5, d3w, d4w,
    load_sem, send_sem, recv_sem,
):
    r, c = lax.axis_index("rows"), lax.axis_index("cols")
    nr, nc = lax.axis_size("rows"), lax.axis_size("cols")
    first, last = r == 0, r == nr - 1
    left, right = c == 0, c == nc - 1
    up, down = jnp.logical_not(first), jnp.logical_not(last)
    west, east = jnp.logical_not(left), jnp.logical_not(right)

    def image(at, rows, sem):
        return [
            pltpu.make_async_copy(
                x_hbm.at[:, pl.ds(at, rows), pl.ds(128 * t, 128)], xs.at[:, t, pl.ds(8 + at, rows), :], load_sem.at[sem + t]
            )
            for t in range(4)
        ]

    lower = image(32, ROWS - 32, 0)
    upper = image(0, 32, 4)
    at_left, at_right = left.astype(jnp.int32), right.astype(jnp.int32)
    cell_tables = [
        pltpu.make_async_copy(clow_hbm.at[at_left], tc.at[pl.ds(0, 128)], load_sem.at[8]),
        pltpu.make_async_copy(chigh_hbm.at[at_right], tc.at[pl.ds(128, 128)], load_sem.at[9]),
    ]
    row_tables = [
        pltpu.make_async_copy(tlow_hbm.at[at_left], tv.at[pl.ds(0, 128)], load_sem.at[10]),
        pltpu.make_async_copy(tmid_hbm, tv.at[pl.ds(128, 256)], load_sem.at[11]),
        pltpu.make_async_copy(thigh_hbm.at[at_right], tv.at[pl.ds(384, 128)], load_sem.at[12]),
    ]
    own_tables = [
        pltpu.make_async_copy(v1_hbm, v1, load_sem.at[13]),
        pltpu.make_async_copy(s1_hbm, s1, load_sem.at[14]),
        pltpu.make_async_copy(w2_hbm, w2, load_sem.at[15]),
        pltpu.make_async_copy(w345_hbm, w345, load_sem.at[16]),
        pltpu.make_async_copy(arrive_hbm, arrive, load_sem.at[17]),
    ]
    for copy in (lower[0], lower[3], *cell_tables, lower[1], lower[2], *row_tables):
        copy.start()

    def there(dr, dc):
        ok = jnp.bool_(True)
        if dr:
            ok = jnp.logical_and(ok, up if dr < 0 else down)
        if dc:
            ok = jnp.logical_and(ok, west if dc < 0 else east)
        return ok

    messages = [
        (rh.at[pl.ds(0, 40)], rh_in.at[pl.ds(0, 40)], 1, 0),
        (kh, chm, 1, 1),
        (kh, chp, 1, -1),
        (rl.at[pl.ds(0, 24)], rl_in.at[pl.ds(0, 24)], -1, 0),
        (kl, clm, -1, 1),
        (kl, clp, -1, -1),
        (cb, cbm, 0, 1),
        (cb, cbp, 0, -1),
    ]
    barrier = pltpu.get_barrier_semaphore()
    for _, dst, dr, dc in messages:

        @pl.when(there(dr, dc))
        def _(dr=dr, dc=dc):
            pl.semaphore_signal(barrier, inc=1, device_id=(r + dr, c + dc), device_id_type=MESH)

        @pl.when(jnp.logical_not(there(-dr, -dc)))
        def _(dst=dst):
            dst[...] = jnp.zeros_like(dst)

    for copy in upper:
        copy.start()

    ys = (xs, y1, y2, y3, y4, y5)
    for k in range(LEVELS):
        ys[k][:, :, 0:8, :] = jnp.zeros((CH, 4, 8, 128), F32)
        ys[k][:, :, 8 + H[k] : 32 + H[k], :] = jnp.zeros((CH, 4, 24, 128), F32)
    srs[...] = jnp.zeros_like(srs)
    ci[...] = jnp.zeros_like(ci)
    for a in (rh, kh, kl):
        a[...] = jnp.zeros_like(a)

    lane = lax.broadcasted_iota(jnp.int32, (16, 128), 1)

    def reduce_lower(tiles):
        for k in range(1, LEVELS + 1):
            mirror_end(ys[k - 1], tiles, H[k - 1], last)
            for t in tiles:
                reduce_rows(t, ys[k - 1], ys[k], BELOW[k])
            for ch in range(CH):
                at = 16 * (k - 1) + 3 * ch
                for t in tiles:
                    srs[t, at : at + 3, :] = ys[k][ch, t, 7 + H[k] : 10 + H[k], :]

    def form_corners(corners, count):
        both = dot3(jnp.concatenate([srs[0, 0:80], srs[3, 0:80]], axis=1), tc[...])
        both = both[:, 0:128] + both[:, 128:256]
        level = [both[16 * k : 16 * k + 16] for k in range(LEVELS)]
        cells, halo = level[4], level[4]
        for k in (3, 2, 1, 0):
            cells = jnp.where(lane < 8 * k + 8, level[k], cells)
            halo = jnp.where(lane < 114 + 2 * k, level[k], halo)
        beside[...] = halo
        ci[0:16, :] = jnp.where(lane < 40, cells, 0.0)
        corners[0:3, :] = sum(pltpu.roll(ci[pl.ds(i, CH, stride=count), :], 40 * i, 1) for i in range(count))

    def form_strips(out, count):
        strips = jnp.concatenate([srs[t, 0:80] for t in range(4)], axis=1)
        near = dot3(strips[0:32], tv[:, 0:384])
        deep = dot3(strips[32:80], tv[:, 384:640])
        deep = deep[:, 0:128] + deep[:, 128:256]
        small = jnp.where(lane < 96, deep[16:32], deep[32:48])
        small = jnp.where(lane < 64, deep[0:16], jnp.where(lane < 112, small, beside[...]))
        for t, a in enumerate((near[0:16, 0:128], near[0:16, 128:256], near[16:32, 256:384], small)):
            out[pl.ds(t, CH * count, stride=4), :] = a[0 : CH * count]

    for copy in (lower[0], lower[3]):
        copy.wait()
    reduce_lower((0, 3))
    for copy in cell_tables:
        copy.wait()
    form_corners(kh, 3)

    place = lax.broadcasted_iota(jnp.int32, (8, 512), 1)

    def of_level(k, a):
        ok = place < (BASE[k + 1] if k < LEVELS else 480)
        return jnp.where(jnp.logical_and(ok, place >= BASE[k]), a, 0.0)

    def put(k, a, out):
        for ch in range(CH):
            for t in range(out.shape[1]):
                out[ch, t, 0 : R[k], :] = a[R[k] * ch : R[k] * (ch + 1), 128 * t : 128 * (t + 1)]

    deeper = ((3, 0, g3, m3), (4, 72, g4, m4), (5, 112, g5, m5))

    def reduce_rest():
        for copy in upper:
            copy.wait()
        for k in range(1, LEVELS + 1):
            mirror_start(ys[k - 1], first)
            for t in range(4):
                reduce_rows(t, ys[k - 1], ys[k], ABOVE[k])
        mirror_start(y5, first)
        for k in range(1, LEVELS + 1):
            for ch in range(CH):
                at = 16 * (k - 1) + 2 * ch
                srs[:, at : at + 2, :] = ys[k][ch, :, 7:9, :]
        form_corners(kl, 2)
        form_strips(rl, 2)
        outer = jnp.concatenate([rows_of(k, ys[k], (0, 3)) for k in range(1, LEVELS + 1)], axis=0)
        cells = dot3(outer, tc[...])
        cells = cells[:, 0:128] + cells[:, 128:256]
        co[...] = cells
        turned = jnp.concatenate([cells, jnp.zeros((32, 128), F32)], axis=0)
        turned = jnp.transpose(turned)
        cb[...] = sum(of_level(k, turned[8 * (k - 1) : 8 * k]) for k in range(1, LEVELS + 1))

    def expand_own():
        for copy in own_tables:
            copy.start()
        p12 = dot3(jnp.concatenate([rows_of(k, ys[k], range(4)) for k in (1, 2)], axis=0), tv[:, 0:384])
        p345 = dot3(jnp.concatenate([rows_of(k, ys[k], range(4)) for k in (3, 4, 5)], axis=0), tv[:, 384:640])
        p345 = p345[:, 0:128] + p345[:, 128:256]
        cells = co[...]
        for copy in own_tables:
            copy.wait()
        put(1, dot3(jnp.concatenate([p12[0:224, 0:256], cells[0:224]], axis=1), v1[...]), g1)
        put(1, p12, m1)
        both = dot3(jnp.concatenate([cells[208:336], p12[208:336, 256:384]], axis=1), w2[...])
        put(2, both[8:, 0:256], g2)
        put(2, both[8:, 256:384], m2)
        for k, at, g, m in deeper:
            rows = 16 * -(-3 * R[k] // 16)
            both = dot3(jnp.concatenate([cells[336 + at : 336 + at + rows], p345[at : at + rows]], axis=1), w345[k - 3])
            skip = BASE[k] - BASE[3] - at
            put(k, both[skip:, 0:128], g)
            put(k, both[skip:, 128:256], m)

    z = lax.rem(r, 8)
    early, earliest = z < 4, z == 0

    def finish_lower():
        for copy in (lower[1], lower[2]):
            copy.wait()
        reduce_lower((1, 2))
        for copy in row_tables:
            copy.wait()
        form_strips(rh, 3)

    @pl.when(early)
    def _():
        finish_lower()
        reduce_rest()

    pl.when(earliest)(expand_own)

    neighbours = (up.astype(jnp.int32) + down.astype(jnp.int32) + 1) * (
        west.astype(jnp.int32) + east.astype(jnp.int32) + 1
    ) - 1
    pl.semaphore_wait(barrier, neighbours)
    copies = []
    for m, (src, dst, dr, dc) in enumerate(messages):
        copies.append(
            pltpu.make_async_remote_copy(
                src_ref=src, dst_ref=dst, send_sem=send_sem.at[m], recv_sem=recv_sem.at[m],
                device_id=(r + dr, c + dc), device_id_type=MESH,
            )
        )
    for m in (1, 2):
        pl.when(there(*messages[m][2:]))(copies[m].start)
    pl.when(jnp.logical_not(early))(finish_lower)
    pl.when(there(1, 0))(copies[0].start)


    @pl.when(jnp.logical_not(early))
    def _():
        reduce_rest()

    for m in range(3, 8):
        pl.when(there(*messages[m][2:]))(copies[m].start)
    pl.when(jnp.logical_not(earliest))(expand_own)

    def add(k, a, out, tiles, first_tile=0):
        for ch in range(CH):
            for i, t in enumerate(tiles):
                lanes = 128 * (first_tile + i)
                out[ch, t, 0 : R[k], :] += a[R[k] * ch : R[k] * (ch + 1), lanes : lanes + 128]

    side = jnp.bitwise_and(lane, 7) < 3
    middle = jnp.logical_and(lane >= 64, lane < 104)
    ci[...] = jnp.zeros_like(ci)

    def add_rows(strip, minus, plus, count, row_of):
        corner = jnp.where(side[0:8], minus[...], plus[...])
        for i in range(count):
            ci[pl.ds(i, CH, stride=count), :] = pltpu.roll(corner, (64 - 40 * i) % 128, 1)[0:CH]
        rows = CH * count
        fill = jnp.zeros((16 - rows, 128), F32)
        tiles = [jnp.concatenate([strip[pl.ds(t, rows, stride=4), :], fill], axis=0) for t in range(4)]
        cells = jnp.where(lane < 112, jnp.where(middle, ci[0:16, :], 0.0), tiles[3])
        wide = dot3(jnp.concatenate([tiles[0], tiles[1], cells], axis=1), v1[...])
        level = jnp.concatenate(tiles[0:2], axis=1) + dot3(cells, s1[...])
        both = [dot3(jnp.concatenate([cells, tiles[2]], axis=1), w2[...])]
        tail = jnp.concatenate([cells, tiles[3]], axis=1)
        both += [dot3(tail, w345[k - 3]) for k in (3, 4, 5)]
        pairs = [(1, wide, g1), (1, level, m1), (2, both[0][:, 0:256], g2), (2, both[0][:, 256:384], m2)]
        for (k, _, g, m), a in zip(deeper, both[1:]):
            pairs += [(k, a[:, 0:128], g), (k, a[:, 128:256], m)]
        for k, a, out in pairs:
            at = row_of(k) + 1
            for ch in range(CH):
                for t in range(out.shape[1]):
                    out[ch, t, at : at + count, :] += a[count * ch : count * (ch + 1), 128 * t : 128 * (t + 1)]

    def details(counts):
        for g, level, at, out, count in zip((g1, g2, g3, g4, g5), (xs, m1, m2, m3, m4), (8, 1, 1, 1, 1), (d0, d1, d2, d3w, d4w), counts):
            detail(g, level, at, out, count)
        d3[...] = d3w[:, 0, 0 : H[3], 0:64]
        d4[...] = d4w[:, 0, 0 : H[4], 0:32]
        d5[...] = m5[:, 0, 1:5, 0:16]

    for m in (3, 4, 5):
        pl.when(there(-messages[m][2], -messages[m][3]))(copies[m].wait_recv)
    add_rows(rl_in, clm, clp, 2, lambda k: H[k] - 1)
    for m in (6, 7):
        pl.when(there(-messages[m][2], -messages[m][3]))(copies[m].wait_recv)
    sub = lax.broadcasted_iota(jnp.int32, (8, 512), 0)
    terms = [a.astype(F32) for a in split3(jnp.where(sub < 3, cbm[...], cbp[...]))]
    came = jnp.concatenate(
        [of_level(k, a) for k in range(1, LEVELS + 1) for a in terms] + [jnp.zeros((8, 512), F32)], axis=0
    )
    came = jnp.transpose(came)

    def arrived(k, at, rows, lanes, count):
        return jnp.dot(
            came[at : at + rows].astype(BF16), arrive[:, lanes : lanes + count], preferred_element_type=F32
        )[BASE[k] - at :]

    more = arrived(1, 0, 224, 0, 512)
    add(1, more, g1, (0, 3))
    add(1, more, m1, (0, 1), 2)
    more = arrived(2, 208, 128, 512, 384)
    add(2, more, g2, (0, 1))
    add(2, more, m2, (0,), 2)
    for k, at, g, m in deeper:
        more = arrived(k, BASE[3] + at, 16 * -(-3 * R[k] // 16), 896 + 256 * (k - 3), 256)
        add(k, more, g, (0,))
        add(k, more, m, (0,), 1)

    for k, g in enumerate((g1, g2, g3, g4, g5), 1):
        g[:, :, H[k] + 1 : H[k] + 2, :] = g[:, :, pl.ds(jnp.where(last, H[k], H[k] + 1), 1), :]
    details(H[1:6])
    for m in range(3):
        pl.when(there(-messages[m][2], -messages[m][3]))(copies[m].wait_recv)
    add_rows(rh_in, chm, chp, 3, lambda k: -1)
    details((4,) * 5)
    for copy, (_, _, dr, dc) in zip(copies, messages):
        pl.when(there(dr, dc))(copy.wait_send)


def result_kernel(d0, d1, d2, d3, d4, d5, o0, o1, o2, o3, o4, o5, sem):
    pairs = [(d0.at[:, t], o0.at[:, :, pl.ds(128 * t, 128)]) for t in range(4)]
    pairs += [(d1.at[:, t], o1.at[:, :, pl.ds(128 * t, 128)]) for t in range(2)]
    pairs += [(d2.at[:, 0], o2), (d3, o3), (d4, o4), (d5, o5)]
    copies = [pltpu.make_async_copy(src, dst, sem.at[i]) for i, (src, dst) in enumerate(pairs)]
    for copy in copies:
        copy.start()
    for copy in copies:
        copy.wait()


def body(orthophoto):
    def vmem(*shape, dtype=F32):
        return pltpu.VMEM(shape, dtype)

    held = [(CH, 4, H[0], 128), (CH, 2, H[1], 128), (CH, 1, H[2], 128)]
    held += [(CH, H[3], W[3]), (CH, H[4], W[4]), (CH, H[5], W[5])]
    scratch = [vmem(CH, 4, H[k] + 32, 128) for k in range(6)]
    scratch += [vmem(256, 256, dtype=BF16), vmem(480, 128)]
    scratch += [vmem(512, 640, dtype=BF16), vmem(384, 512, dtype=BF16), vmem(128, 256, dtype=BF16)]
    scratch += [vmem(256, 384, dtype=BF16), vmem(3, 256, 256, dtype=BF16), vmem(128, 1664, dtype=BF16)]
    scratch += [vmem(4, 88, 128), vmem(32, 128), vmem(16, 128)]
    scratch += [vmem(72, 128), vmem(40, 128), vmem(8, 128), vmem(8, 128), vmem(8, 512)]
    scratch += [vmem(72, 128), vmem(40, 128), vmem(8, 512), vmem(8, 512)]
    scratch += [vmem(8, 128)] * 4
    scratch += [vmem(CH, t, R[k] + 8, 128) for k, t in ((1, 4), (2, 2), (3, 1), (4, 1), (5, 1))]
    scratch += [vmem(CH, t, R[k] + 8, 128) for k, t in ((1, 2), (2, 1), (3, 1), (4, 1), (5, 1))]
    scratch += [vmem(CH, 1, H[3] + 8, 128), vmem(CH, 1, H[4] + 8, 128)]
    scratch += [pltpu.SemaphoreType.DMA((n,)) for n in (18, 8, 8)]
    far = pl.BlockSpec(memory_space=pltpu.HBM)
    inside = pl.BlockSpec(memory_space=pltpu.VMEM)
    inputs = [pltpu.with_memory_space_constraint(jnp.asarray(a), pltpu.HBM) for a in (orthophoto, *tables())]
    arrays = pl.pallas_call(
        exchange_kernel,
        out_shape=[jax.ShapeDtypeStruct(shape, F32) for shape in held],
        in_specs=[far] * len(inputs),
        out_specs=[inside] * len(held),
        scratch_shapes=scratch,
        compiler_params=pltpu.CompilerParams(collective_id=0, has_side_effects=True, vmem_limit_bytes=24 << 20),
    )(*inputs)
    results = pl.pallas_call(
        result_kernel,
        out_shape=[jax.ShapeDtypeStruct((CH, H[k], W[k]), F32) for k in range(6)],
        in_specs=[inside] * len(held),
        out_specs=[far] * 6,
        scratch_shapes=[pltpu.SemaphoreType.DMA((10,))],
        compiler_params=pltpu.CompilerParams(vmem_limit_bytes=8 << 20),
    )(*arrays)
    return tuple(results)


def solution(mesh):
    placed = P(None, "rows", "cols")
    return jax.shard_map(body, mesh=mesh, in_specs=(placed,), out_specs=(placed,) * 6, check_vma=False)
```

```python
import functools

import jax
import jax.numpy as jnp
import numpy as np
from jax import lax
from jax.experimental import pallas as pl
from jax.experimental.pallas import tpu as pltpu
from jax.sharding import PartitionSpec as P

CH = 3
ROWS = 128
COLS = 512
LEVELS = 5
H = [ROWS >> k for k in range(6)]
W = [COLS >> k for k in range(6)]
R = [0, 72, 40, 24, 16, 8]
BASE = [0, 0, 216, 336, 408, 456]
POS = [0, 0, 0, 0, 64, 96]
F32 = jnp.float32
BF16 = jnp.bfloat16
MESH = pl.DeviceIdType.MESH
TAPS = (1.0, 4.0, 6.0, 4.0, 1.0)


def column_reductions(low, high):
    result = [None]
    total = None
    for k in range(1, LEVELS + 1):
        n = W[k - 1]
        step = np.zeros((n + 3, W[k] + 3))
        for j in range(0 if low else -1, W[k] if high else W[k] + 2):
            for tap in range(5):
                cell = 2 * j - 2 + tap
                if low and cell < 0:
                    cell = -cell
                if high and cell > n - 1:
                    cell = 2 * (n - 1) - cell
                if -1 <= cell <= n + 1:
                    step[cell + 1, j + 1] += TAPS[tap] / 16
        total = step[1 : n + 1] if k == 1 else total @ step
        result.append(total / 16.0**k)
    return result


def reduction_table(low, high):
    t = column_reductions(low, high)

    def fill(a, at, k):
        beyond, before = W[k] - 1 if high else W[k], 1 if low else -1
        cells = (W[k] - 1, beyond, W[k] + 1, before, 0)
        a[:, at + 8 * (k - 1) : at + 8 * (k - 1) + 5] = t[k][:, [c + 1 for c in cells]]
        a[:, at + 112 + 2 * (k - 1) : at + 114 + 2 * (k - 1)] = t[k][:, [beyond + 1, before + 1]]

    near = np.zeros((COLS, 384))
    near[:, 0:256] = t[1][:, 1:257]
    near[:, 256:384] = t[2][:, 1:129]
    deep, cells = np.zeros((COLS, 128)), np.zeros((COLS, 128))
    for k in range(1, LEVELS + 1):
        fill(cells, 0, k)
        if k > 2:
            deep[:, POS[k] : POS[k] + W[k]] = t[k][:, 1 : W[k] + 1]
    assert not cells[128:384].any()
    return np.concatenate([near, *two_terms(deep)], axis=1), np.concatenate(two_terms(cells), axis=1)


def two_terms(a):
    top = np.asarray(a.astype(jnp.bfloat16), np.float64)
    rest = np.asarray((a - top).astype(jnp.bfloat16), np.float64)
    assert np.array_equal(top + rest, a)
    return top, rest


def expansion_row(k, cell):
    row = np.zeros(2 * W[k])
    for i in range(W[k]):
        row[2 * i] += {i - 1: 0.125, i: 0.75, i + 1: 0.125}.get(cell, 0.0)
        row[2 * i + 1] += {i: 0.5, i + 1: 0.5}.get(cell, 0.0)
    return row


def expansion_table(k, main_at, edge_at, lanes):
    spread = np.zeros((lanes, 2 * W[k]))
    keep = np.zeros((lanes, W[k]))
    for c in range(W[k]):
        spread[main_at + c] = expansion_row(k, c)
        keep[main_at + c, c] = 1
    own = edge_at + 112 + 2 * (k - 1)
    came = edge_at + 64 + 8 * (k - 1)
    spread[own] = expansion_row(k, W[k])
    spread[own + 1] = expansion_row(k, -1)
    for s, cell in enumerate((-1, 0, 1, W[k] - 1, W[k])):
        spread[came + s] = expansion_row(k, cell)
        if 0 <= cell < W[k]:
            keep[came + s, cell] = 1
    return spread, keep


def arrival_table(k):
    spread = np.zeros((128, 2 * W[k]))
    keep = np.zeros((128, W[k]))
    for part in range(3):
        for s, cell in enumerate((-1, 0, 1, W[k] - 1, W[k])):
            lane = 24 * (k - 1) + 8 * part + s
            spread[lane] = expansion_row(k, cell)
            if 0 <= cell < W[k]:
                keep[lane, cell] = 1
    return spread, keep


def padded(a, cols):
    return np.pad(a, ((0, 0), (0, cols - a.shape[1])))


def tables():
    (plain, cells), (low, cells_low), (high, cells_high) = (
        reduction_table(*e) for e in ((False, False), (True, False), (False, True))
    )
    assert np.array_equal(plain[128:], low[128:]) and np.array_equal(plain[:384], high[:384])
    assert np.array_equal(plain[:, 0:384], np.asarray(plain[:, 0:384].astype(jnp.bfloat16), np.float64))
    t_low = np.stack([plain[:128], low[:128]])
    t_high = np.stack([plain[384:], high[384:]])
    c_low = np.stack([cells[:128], cells_low[:128]])
    c_high = np.stack([cells[384:], cells_high[384:]])
    v1, s1 = expansion_table(1, 0, 256, 384)
    w2 = np.concatenate(expansion_table(2, 128, 0, 256), axis=1)
    deep = []
    for k in (3, 4, 5):
        spread, keep = expansion_table(k, 128 + POS[k], 0, 256)
        deep.append(np.concatenate([padded(spread, 128), padded(keep, 128)], axis=1))
    spread, keep = arrival_table(1)
    assert not spread[:, 128:384].any()
    arrive = [spread[:, :128], spread[:, 384:], keep]
    arrive += arrival_table(2)
    for k in (3, 4, 5):
        arrive += [padded(a, 128) for a in arrival_table(k)]
    parts = (c_low, c_high, t_low, plain[128:384], t_high, v1, s1[256:], w2, np.stack(deep), np.concatenate(arrive, axis=1))
    return [a.astype(jnp.bfloat16) for a in parts]


def split3(a):
    top = a.astype(BF16)
    rest = a - top.astype(F32)
    mid = rest.astype(BF16)
    return top, mid, (rest - mid.astype(F32)).astype(BF16)


def dot3(a, table):
    m = a.shape[0]
    p = jnp.dot(jnp.concatenate(split3(a), axis=0), table, preferred_element_type=F32)
    return p[0:m] + p[m : 2 * m] + p[2 * m : 3 * m]


BELOW = [None, (18, 26, 34, 42, 50, 58), (10, 18, 26), (6, 14), (4,), (3,)]
ABOVE = [None, (-1, 7, 15), (-1, 7), (-1,), (-1,), (-1,)]


def reduce_rows(t, src, dst, starts):
    for ch in range(CH):
        for j in starts:

            def tap(o):
                return src[ch, t, pl.ds(8 + 2 * j + o, 8, stride=2), :]

            dst[ch, t, 8 + j : 16 + j, :] = (tap(-2) + tap(2)) + (tap(-1) + tap(1)) * 4.0 + tap(0) * 6.0


def mirror_start(a, first):
    for t in range(4):
        a[:, t, 7:8, :] = a[:, t, pl.ds(jnp.where(first, 9, 7), 1), :]
        a[:, t, 6:7, :] = a[:, t, pl.ds(jnp.where(first, 10, 6), 1), :]


def mirror_end(a, tiles, h, last):
    for t in tiles:
        a[:, t, 8 + h : 9 + h, :] = a[:, t, pl.ds(jnp.where(last, 6 + h, 8 + h), 1), :]


def rows_of(k, y, tiles):
    return jnp.concatenate(
        [jnp.concatenate([y[c, t, 7 : 7 + R[k], :] for t in tiles], axis=1) for c in range(CH)], axis=0
    )


def detail(g, level, at, out, count):
    lo, mid, hi = (g[:, :, i : i + count, :] for i in range(3))
    even, odd = pl.ds(at, count, stride=2), pl.ds(at + 1, count, stride=2)
    out[:, :, pl.ds(0, count, stride=2), :] = level[:, :, even, :] - ((lo + hi) * 0.125 + mid * 0.75)
    out[:, :, pl.ds(1, count, stride=2), :] = level[:, :, odd, :] - (mid + hi) * 0.5


def exchange_kernel(
    x_hbm, clow_hbm, chigh_hbm, tlow_hbm, tmid_hbm, thigh_hbm, v1_hbm, s1_hbm, w2_hbm, w345_hbm, arrive_hbm,
    d0, d1, d2, d3, d4, d5,
    xs, y1, y2, y3, y4, y5, tc, co, tv, v1, s1, w2, w345, arrive, srs, ci, beside,
    rh, rl, kh, kl, cb, rh_in, rl_in, cbm, cbp, chm, chp, clm, clp,
    g1, g2, g3, g4, g5, m1, m2, m3, m4, m5, d3w, d4w,
    load_sem, send_sem, recv_sem,
):
    r, c = lax.axis_index("rows"), lax.axis_index("cols")
    nr, nc = lax.axis_size("rows"), lax.axis_size("cols")
    first, last = r == 0, r == nr - 1
    left, right = c == 0, c == nc - 1
    up, down = jnp.logical_not(first), jnp.logical_not(last)
    west, east = jnp.logical_not(left), jnp.logical_not(right)

    def image(at, rows, sem):
        return [
            pltpu.make_async_copy(
                x_hbm.at[:, pl.ds(at, rows), pl.ds(128 * t, 128)], xs.at[:, t, pl.ds(8 + at, rows), :], load_sem.at[sem + t]
            )
            for t in range(4)
        ]

    lower = image(32, ROWS - 32, 0)
    upper = image(0, 32, 4)
    at_left, at_right = left.astype(jnp.int32), right.astype(jnp.int32)
    cell_tables = [
        pltpu.make_async_copy(clow_hbm.at[at_left], tc.at[pl.ds(0, 128)], load_sem.at[8]),
        pltpu.make_async_copy(chigh_hbm.at[at_right], tc.at[pl.ds(128, 128)], load_sem.at[9]),
    ]
    row_tables = [
        pltpu.make_async_copy(tlow_hbm.at[at_left], tv.at[pl.ds(0, 128)], load_sem.at[10]),
        pltpu.make_async_copy(tmid_hbm, tv.at[pl.ds(128, 256)], load_sem.at[11]),
        pltpu.make_async_copy(thigh_hbm.at[at_right], tv.at[pl.ds(384, 128)], load_sem.at[12]),
    ]
    own_tables = [
        pltpu.make_async_copy(v1_hbm, v1, load_sem.at[13]),
        pltpu.make_async_copy(s1_hbm, s1, load_sem.at[14]),
        pltpu.make_async_copy(w2_hbm, w2, load_sem.at[15]),
        pltpu.make_async_copy(w345_hbm, w345, load_sem.at[16]),
        pltpu.make_async_copy(arrive_hbm, arrive, load_sem.at[17]),
    ]
    for copy in (lower[0], lower[3], *cell_tables, lower[1], lower[2], *row_tables):
        copy.start()

    def there(dr, dc):
        ok = jnp.bool_(True)
        if dr:
            ok = jnp.logical_and(ok, up if dr < 0 else down)
        if dc:
            ok = jnp.logical_and(ok, west if dc < 0 else east)
        return ok

    messages = [
        (rh.at[pl.ds(0, 40)], rh_in.at[pl.ds(0, 40)], 1, 0),
        (kh, chm, 1, 1),
        (kh, chp, 1, -1),
        (rl.at[pl.ds(0, 24)], rl_in.at[pl.ds(0, 24)], -1, 0),
        (kl, clm, -1, 1),
        (kl, clp, -1, -1),
        (cb, cbm, 0, 1),
        (cb, cbp, 0, -1),
    ]
    barrier = pltpu.get_barrier_semaphore()
    for _, dst, dr, dc in messages:

        @pl.when(there(dr, dc))
        def _(dr=dr, dc=dc):
            pl.semaphore_signal(barrier, inc=1, device_id=(r + dr, c + dc), device_id_type=MESH)

        @pl.when(jnp.logical_not(there(-dr, -dc)))
        def _(dst=dst):
            dst[...] = jnp.zeros_like(dst)

    for copy in upper:
        copy.start()

    ys = (xs, y1, y2, y3, y4, y5)
    for k in range(LEVELS):
        ys[k][:, :, 0:8, :] = jnp.zeros((CH, 4, 8, 128), F32)
        ys[k][:, :, 8 + H[k] : 32 + H[k], :] = jnp.zeros((CH, 4, 24, 128), F32)
    srs[...] = jnp.zeros_like(srs)
    ci[...] = jnp.zeros_like(ci)
    for a in (rh, kh, kl):
        a[...] = jnp.zeros_like(a)

    lane = lax.broadcasted_iota(jnp.int32, (16, 128), 1)

    def reduce_lower(tiles):
        for k in range(1, LEVELS + 1):
            mirror_end(ys[k - 1], tiles, H[k - 1], last)
            for t in tiles:
                reduce_rows(t, ys[k - 1], ys[k], BELOW[k])
            for ch in range(CH):
                at = 16 * (k - 1) + 3 * ch
                for t in tiles:
                    srs[t, at : at + 3, :] = ys[k][ch, t, 7 + H[k] : 10 + H[k], :]

    def form_corners(corners, count):
        both = dot3(jnp.concatenate([srs[0, 0:80], srs[3, 0:80]], axis=1), tc[...])
        both = both[:, 0:128] + both[:, 128:256]
        level = [both[16 * k : 16 * k + 16] for k in range(LEVELS)]
        cells, halo = level[4], level[4]
        for k in (3, 2, 1, 0):
            cells = jnp.where(lane < 8 * k + 8, level[k], cells)
            halo = jnp.where(lane < 114 + 2 * k, level[k], halo)
        beside[...] = halo
        ci[0:16, :] = jnp.where(lane < 40, cells, 0.0)
        corners[0:3, :] = sum(pltpu.roll(ci[pl.ds(i, CH, stride=count), :], 40 * i, 1) for i in range(count))

    def form_strips(out, count):
        strips = jnp.concatenate([srs[t, 0:80] for t in range(4)], axis=1)
        near = dot3(strips[0:32], tv[:, 0:384])
        deep = dot3(strips[32:80], tv[:, 384:640])
        deep = deep[:, 0:128] + deep[:, 128:256]
        small = jnp.where(lane < 96, deep[16:32], deep[32:48])
        small = jnp.where(lane < 64, deep[0:16], jnp.where(lane < 112, small, beside[...]))
        for t, a in enumerate((near[0:16, 0:128], near[0:16, 128:256], near[16:32, 256:384], small)):
            out[pl.ds(t, CH * count, stride=4), :] = a[0 : CH * count]

    for copy in (lower[0], lower[3]):
        copy.wait()
    reduce_lower((0, 3))
    for copy in (*cell_tables, lower[1], lower[2]):
        copy.wait()
    form_corners(kh, 3)
    reduce_lower((1, 2))

    place = lax.broadcasted_iota(jnp.int32, (8, 512), 1)

    def of_level(k, a):
        ok = place < (BASE[k + 1] if k < LEVELS else 480)
        return jnp.where(jnp.logical_and(ok, place >= BASE[k]), a, 0.0)

    def put(k, a, out):
        for ch in range(CH):
            for t in range(out.shape[1]):
                out[ch, t, 0 : R[k], :] = a[R[k] * ch : R[k] * (ch + 1), 128 * t : 128 * (t + 1)]

    deeper = ((3, 0, g3, m3), (4, 72, g4, m4), (5, 112, g5, m5))

    def reduce_rest():
        for copy in upper:
            copy.wait()
        for k in range(1, LEVELS + 1):
            mirror_start(ys[k - 1], first)
            for t in range(4):
                reduce_rows(t, ys[k - 1], ys[k], ABOVE[k])
        mirror_start(y5, first)
        for k in range(1, LEVELS + 1):
            for ch in range(CH):
                at = 16 * (k - 1) + 2 * ch
                srs[:, at : at + 2, :] = ys[k][ch, :, 7:9, :]
        form_corners(kl, 2)
        form_strips(rl, 2)
        outer = jnp.concatenate([rows_of(k, ys[k], (0, 3)) for k in range(1, LEVELS + 1)], axis=0)
        cells = dot3(outer, tc[...])
        cells = cells[:, 0:128] + cells[:, 128:256]
        co[...] = cells
        turned = jnp.concatenate([cells, jnp.zeros((32, 128), F32)], axis=0)
        turned = jnp.transpose(turned)
        cb[...] = sum(of_level(k, turned[8 * (k - 1) : 8 * k]) for k in range(1, LEVELS + 1))

    def expand_own():
        for copy in own_tables:
            copy.start()
        p12 = dot3(jnp.concatenate([rows_of(k, ys[k], range(4)) for k in (1, 2)], axis=0), tv[:, 0:384])
        p345 = dot3(jnp.concatenate([rows_of(k, ys[k], range(4)) for k in (3, 4, 5)], axis=0), tv[:, 384:640])
        p345 = p345[:, 0:128] + p345[:, 128:256]
        cells = co[...]
        for copy in own_tables:
            copy.wait()
        put(1, dot3(jnp.concatenate([p12[0:224, 0:256], cells[0:224]], axis=1), v1[...]), g1)
        put(1, p12, m1)
        both = dot3(jnp.concatenate([cells[208:336], p12[208:336, 256:384]], axis=1), w2[...])
        put(2, both[8:, 0:256], g2)
        put(2, both[8:, 256:384], m2)
        for k, at, g, m in deeper:
            rows = 16 * -(-3 * R[k] // 16)
            both = dot3(jnp.concatenate([cells[336 + at : 336 + at + rows], p345[at : at + rows]], axis=1), w345[k - 3])
            skip = BASE[k] - BASE[3] - at
            put(k, both[skip:, 0:128], g)
            put(k, both[skip:, 128:256], m)

    z = lax.rem(r, 8)
    early, earliest = z < 4, z == 0

    def finish_lower():
        for copy in row_tables:
            copy.wait()
        form_strips(rh, 3)

    @pl.when(early)
    def _():
        finish_lower()
        reduce_rest()

    pl.when(earliest)(expand_own)

    neighbours = (up.astype(jnp.int32) + down.astype(jnp.int32) + 1) * (
        west.astype(jnp.int32) + east.astype(jnp.int32) + 1
    ) - 1
    pl.semaphore_wait(barrier, neighbours)
    copies = []
    for m, (src, dst, dr, dc) in enumerate(messages):
        copies.append(
            pltpu.make_async_remote_copy(
                src_ref=src, dst_ref=dst, send_sem=send_sem.at[m], recv_sem=recv_sem.at[m],
                device_id=(r + dr, c + dc), device_id_type=MESH,
            )
        )
    for m in (1, 2):
        pl.when(there(*messages[m][2:]))(copies[m].start)
    pl.when(jnp.logical_not(early))(finish_lower)
    pl.when(there(1, 0))(copies[0].start)


    @pl.when(jnp.logical_not(early))
    def _():
        reduce_rest()

    for m in range(3, 8):
        pl.when(there(*messages[m][2:]))(copies[m].start)
    pl.when(jnp.logical_not(earliest))(expand_own)

    def add(k, a, out, tiles, first_tile=0):
        for ch in range(CH):
            for i, t in enumerate(tiles):
                lanes = 128 * (first_tile + i)
                out[ch, t, 0 : R[k], :] += a[R[k] * ch : R[k] * (ch + 1), lanes : lanes + 128]

    side = jnp.bitwise_and(lane, 7) < 3
    middle = jnp.logical_and(lane >= 64, lane < 104)
    ci[...] = jnp.zeros_like(ci)

    def add_rows(strip, minus, plus, count, row_of):
        corner = jnp.where(side[0:8], minus[...], plus[...])
        for i in range(count):
            ci[pl.ds(i, CH, stride=count), :] = pltpu.roll(corner, (64 - 40 * i) % 128, 1)[0:CH]
        rows = CH * count
        fill = jnp.zeros((16 - rows, 128), F32)
        tiles = [jnp.concatenate([strip[pl.ds(t, rows, stride=4), :], fill], axis=0) for t in range(4)]
        cells = jnp.where(lane < 112, jnp.where(middle, ci[0:16, :], 0.0), tiles[3])
        wide = dot3(jnp.concatenate([tiles[0], tiles[1], cells], axis=1), v1[...])
        level = jnp.concatenate(tiles[0:2], axis=1) + dot3(cells, s1[...])
        both = [dot3(jnp.concatenate([cells, tiles[2]], axis=1), w2[...])]
        tail = jnp.concatenate([cells, tiles[3]], axis=1)
        both += [dot3(tail, w345[k - 3]) for k in (3, 4, 5)]
        pairs = [(1, wide, g1), (1, level, m1), (2, both[0][:, 0:256], g2), (2, both[0][:, 256:384], m2)]
        for (k, _, g, m), a in zip(deeper, both[1:]):
            pairs += [(k, a[:, 0:128], g), (k, a[:, 128:256], m)]
        for k, a, out in pairs:
            at = row_of(k) + 1
            for ch in range(CH):
                for t in range(out.shape[1]):
                    out[ch, t, at : at + count, :] += a[count * ch : count * (ch + 1), 128 * t : 128 * (t + 1)]

    def details(counts):
        for g, level, at, out, count in zip((g1, g2, g3, g4, g5), (xs, m1, m2, m3, m4), (8, 1, 1, 1, 1), (d0, d1, d2, d3w, d4w), counts):
            detail(g, level, at, out, count)
        d3[...] = d3w[:, 0, 0 : H[3], 0:64]
        d4[...] = d4w[:, 0, 0 : H[4], 0:32]
        d5[...] = m5[:, 0, 1:5, 0:16]

    for m in (3, 4, 5):
        pl.when(there(-messages[m][2], -messages[m][3]))(copies[m].wait_recv)
    add_rows(rl_in, clm, clp, 2, lambda k: H[k] - 1)
    for m in (6, 7):
        pl.when(there(-messages[m][2], -messages[m][3]))(copies[m].wait_recv)
    sub = lax.broadcasted_iota(jnp.int32, (8, 512), 0)
    terms = [a.astype(F32) for a in split3(jnp.where(sub < 3, cbm[...], cbp[...]))]
    came = jnp.concatenate(
        [of_level(k, a) for k in range(1, LEVELS + 1) for a in terms] + [jnp.zeros((8, 512), F32)], axis=0
    )
    came = jnp.transpose(came)

    def arrived(k, at, rows, lanes, count):
        return jnp.dot(
            came[at : at + rows].astype(BF16), arrive[:, lanes : lanes + count], preferred_element_type=F32
        )[BASE[k] - at :]

    more = arrived(1, 0, 224, 0, 512)
    add(1, more, g1, (0, 3))
    add(1, more, m1, (0, 1), 2)
    more = arrived(2, 208, 128, 512, 384)
    add(2, more, g2, (0, 1))
    add(2, more, m2, (0,), 2)
    for k, at, g, m in deeper:
        more = arrived(k, BASE[3] + at, 16 * -(-3 * R[k] // 16), 896 + 256 * (k - 3), 256)
        add(k, more, g, (0,))
        add(k, more, m, (0,), 1)

    for k, g in enumerate((g1, g2, g3, g4, g5), 1):
        g[:, :, H[k] + 1 : H[k] + 2, :] = g[:, :, pl.ds(jnp.where(last, H[k], H[k] + 1), 1), :]
    details(H[1:6])
    for m in range(3):
        pl.when(there(-messages[m][2], -messages[m][3]))(copies[m].wait_recv)
    add_rows(rh_in, chm, chp, 3, lambda k: -1)
    details((4,) * 5)
    for copy, (_, _, dr, dc) in zip(copies, messages):
        pl.when(there(dr, dc))(copy.wait_send)


def result_kernel(d0, d1, d2, d3, d4, d5, o0, o1, o2, o3, o4, o5, sem):
    pairs = [(d0.at[:, t], o0.at[:, :, pl.ds(128 * t, 128)]) for t in range(4)]
    pairs += [(d1.at[:, t], o1.at[:, :, pl.ds(128 * t, 128)]) for t in range(2)]
    pairs += [(d2.at[:, 0], o2), (d3, o3), (d4, o4), (d5, o5)]
    copies = [pltpu.make_async_copy(src, dst, sem.at[i]) for i, (src, dst) in enumerate(pairs)]
    for copy in copies:
        copy.start()
    for copy in copies:
        copy.wait()


def body(orthophoto):
    def vmem(*shape, dtype=F32):
        return pltpu.VMEM(shape, dtype)

    held = [(CH, 4, H[0], 128), (CH, 2, H[1], 128), (CH, 1, H[2], 128)]
    held += [(CH, H[3], W[3]), (CH, H[4], W[4]), (CH, H[5], W[5])]
    scratch = [vmem(CH, 4, H[k] + 32, 128) for k in range(6)]
    scratch += [vmem(256, 256, dtype=BF16), vmem(480, 128)]
    scratch += [vmem(512, 640, dtype=BF16), vmem(384, 512, dtype=BF16), vmem(128, 256, dtype=BF16)]
    scratch += [vmem(256, 384, dtype=BF16), vmem(3, 256, 256, dtype=BF16), vmem(128, 1664, dtype=BF16)]
    scratch += [vmem(4, 88, 128), vmem(32, 128), vmem(16, 128)]
    scratch += [vmem(72, 128), vmem(40, 128), vmem(8, 128), vmem(8, 128), vmem(8, 512)]
    scratch += [vmem(72, 128), vmem(40, 128), vmem(8, 512), vmem(8, 512)]
    scratch += [vmem(8, 128)] * 4
    scratch += [vmem(CH, t, R[k] + 8, 128) for k, t in ((1, 4), (2, 2), (3, 1), (4, 1), (5, 1))]
    scratch += [vmem(CH, t, R[k] + 8, 128) for k, t in ((1, 2), (2, 1), (3, 1), (4, 1), (5, 1))]
    scratch += [vmem(CH, 1, H[3] + 8, 128), vmem(CH, 1, H[4] + 8, 128)]
    scratch += [pltpu.SemaphoreType.DMA((n,)) for n in (18, 8, 8)]
    far = pl.BlockSpec(memory_space=pltpu.HBM)
    inside = pl.BlockSpec(memory_space=pltpu.VMEM)
    inputs = [pltpu.with_memory_space_constraint(jnp.asarray(a), pltpu.HBM) for a in (orthophoto, *tables())]
    arrays = pl.pallas_call(
        exchange_kernel,
        out_shape=[jax.ShapeDtypeStruct(shape, F32) for shape in held],
        in_specs=[far] * len(inputs),
        out_specs=[inside] * len(held),
        scratch_shapes=scratch,
        compiler_params=pltpu.CompilerParams(collective_id=0, has_side_effects=True, vmem_limit_bytes=24 << 20),
    )(*inputs)
    results = pl.pallas_call(
        result_kernel,
        out_shape=[jax.ShapeDtypeStruct((CH, H[k], W[k]), F32) for k in range(6)],
        in_specs=[inside] * len(held),
        out_specs=[far] * 6,
        scratch_shapes=[pltpu.SemaphoreType.DMA((10,))],
        compiler_params=pltpu.CompilerParams(vmem_limit_bytes=8 << 20),
    )(*arrays)
    return tuple(results)


def solution(mesh):
    placed = P(None, "rows", "cols")
    return jax.shard_map(body, mesh=mesh, in_specs=(placed,), out_specs=(placed,) * 6, check_vma=False)
```
